32 devices in a mesh: dp: 8 (over z, x), tensor: 4 (over y, core).
Axes of the slice: x: 2, y: 2, z: 4, core: 2. Of those that a mesh axis runs over, the one named last changes fastest.
Arguments:
- layer_input: bfloat16 [8192, 2048], P('dp'), may hold values from -6 to 6
- ln1_gain: bfloat16 [2048], replicated, may hold values from 0.099609375 to 1.8984375
- ln1_bias: bfloat16 [2048], replicated, may hold values from -3 to 3
- ln2_gain: bfloat16 [2048], replicated, may hold values from 0.099609375 to 1.8984375
- ln2_bias: bfloat16 [2048], replicated, may hold values from -3 to 3
- qkv_weight: bfloat16 [2048, 6144], P(None, 'tensor'), may hold values from -0.125 to 0.125
- qkv_bias: bfloat16 [6144], P('tensor'), may hold values from -1.75 to 1.75
- dense_weight: bfloat16 [2048, 2048], P(None, 'tensor'), may hold values from -0.75 to 0.75
- dense_bias: bfloat16 [2048], replicated, may hold values from -3 to 3
- fc1_weight: bfloat16 [2048, 8192], P(None, 'tensor'), may hold values from -0.125 to 0.125
- fc1_bias: bfloat16 [8192], P('tensor'), may hold values from -3 to 3
- fc2_weight: bfloat16 [2048, 8192], P(None, 'tensor'), may hold values from -0.0625 to 0.0625
- fc2_bias: bfloat16 [2048], replicated, may hold values from -3 to 3
- cotangent: bfloat16 [8192, 2048], P('dp'), may hold values from -6 to 6
Outputs:
- output: bfloat16 [8192, 2048], P('dp')
- input_grad: bfloat16 [8192, 2048], P('dp')
- grad_ln1_gain: float32 [2048], replicated
- grad_ln1_bias: float32 [2048], replicated
- grad_ln2_gain: float32 [2048], replicated
- grad_ln2_bias: float32 [2048], replicated
- grad_qkv_weight: float32 [2048, 6144], P('dp', 'tensor')
- grad_qkv_bias: float32 [6144], P('tensor')
- grad_dense_weight: float32 [2048, 2048], P('dp', 'tensor')
- grad_dense_bias: float32 [2048], replicated
- grad_fc1_weight: float32 [2048, 8192], P('dp', 'tensor')
- grad_fc1_bias: float32 [8192], P('tensor')
- grad_fc2_weight: float32 [2048, 8192], P('dp', 'tensor')
- grad_fc2_bias: float32 [2048], replicated
The draws below stay inside these ranges and needn't reach their ends.
All inputs are finite; a program needn't handle non-finite values.
Results may differ from the reference program's by a relative error of at most 0.013.
Values may be sent and summed in bfloat16 or wider, within the bound.
A program may use at most 256 MiB of HBM per device.

```python
import math
import jax
import jax.numpy as jnp
from jax import lax

D = 2048
HEADS = 8
FF = 8192
SEQ = 1024
HEAD_DIM = 256
ROT = 64
TOKENS = 8192


def strengthened(values, key, source, target, parts, factor):
    def block_of(position):
        return (jnp.arange(values.shape[position]) // (values.shape[position] // parts)).reshape((-1,) + (1,) * (values.ndim - 1 - position))

    one_side = jax.random.permutation(key, parts)[block_of(target)]
    far = (block_of(target) + parts // 2) % parts
    return jnp.where((block_of(source) == one_side) | (block_of(source) == far), factor * values, values)


def levels(own_key, extent, shards, least, largest):
    gain = 1.0
    for position, parts in shards:
        steps = jax.random.uniform(jax.random.fold_in(jax.random.fold_in(own_key, 6), position), (parts,), jnp.float32, least / len(shards), largest / len(shards))
        gain = gain * jnp.repeat(jnp.exp(steps), extent[position] // parts).reshape((-1,) + (1,) * (len(extent) - 1 - position))
    return gain


def noise(rng, shape, deviation, reach, pieces=(), held_as=jnp.bfloat16):
    level = levels(rng, shape, pieces, -0.22, 0.18) if pieces else 1.0
    values = jax.random.normal(rng, shape, jnp.float32) * deviation * level
    return jnp.minimum(jnp.maximum(values, -reach), reach).astype(held_as)


def bell_draw_with(own_key, extent, width, bound, cuts, heavy, held_as=jnp.bfloat16):
    array = width * jax.random.normal(own_key, extent, jnp.float32)
    if cuts:
        array = array * levels(own_key, extent, cuts, -0.22, 0.18)
    return jnp.clip(strengthened(array, jax.random.fold_in(own_key, 3), *heavy), -bound, bound).astype(held_as)


def setup_inputs(seed: int = 0) -> dict:
    splits = jax.random.split(jax.random.key(seed), 15)
    return {
        "layer_input": bell_draw_with(splits[0], (TOKENS, D), 1.0, 6.0, ((0, 8),), (0, 1, 8, 2.0)),
        "ln1_gain": jnp.clip(1.0 + 0.18 * jax.random.normal(splits[1], (D,), jnp.float32), 0.099609375, 1.8984375).astype(jnp.bfloat16),
        "ln1_bias": noise(splits[2], (D,), 0.5, 3.0),
        "ln2_gain": jnp.clip(1.0 + 0.18 * jax.random.normal(splits[3], (D,), jnp.float32), 0.099609375, 1.8984375).astype(jnp.bfloat16),
        "ln2_bias": noise(splits[4], (D,), 0.5, 3.0),
        "qkv_weight": noise(splits[5], (D, 3 * D), D ** -0.5, 0.125, ((1, 4),)),
        "qkv_bias": noise(splits[6], (3 * D,), 0.3, 1.75, ((0, 4),)),
        "dense_weight": noise(splits[7], (D, D), (D // 32) ** -0.5, 0.75, ((1, 4),)),
        "dense_bias": noise(splits[8], (D,), 0.5, 3.0),
        "fc1_weight": noise(splits[9], (D, FF), D ** -0.5, 0.125, ((1, 4),)),
        "fc1_bias": noise(splits[10], (FF,), 0.5, 3.0, ((0, 4),)),
        "fc2_weight": noise(splits[11], (D, FF), FF ** -0.5, 0.0625, ((1, 4),)),
        "fc2_bias": noise(splits[12], (D,), 0.5, 3.0),
        "cotangent": bell_draw_with(splits[13], (TOKENS, D), 1.0, 6.0, ((0, 8),), (0, 1, 8, 2.0)),
    }


EPSILON = 1e-05
PRECISE = lax.Precision.HIGHEST

@jax.custom_vjp
def low(v):
    return lax.optimization_barrier(v.astype(jnp.bfloat16)).astype(jnp.float32)

@jax.custom_vjp
def low_back(v):
    return v

def low_keep(v):
    return (low(v), None)

def low_pass(kept, grad):
    return (grad,)

def back_keep(v):
    return (v, None)

def back_low(kept, grad):
    return (low(grad),)
low.defvjp(low_keep, low_pass)
low_back.defvjp(back_keep, back_low)

def normalize(x_float, gain_row, shift_row):
    row_mean = lax.optimization_barrier(jnp.mean(x_float, -1, keepdims=True))
    centred = x_float - row_mean
    spread = lax.optimization_barrier(jnp.mean(centred * centred, -1, keepdims=True))
    return centred * lax.rsqrt(spread + EPSILON) * gain_row + shift_row

def rotary_tables():
    half_rot = ROT // 2
    freq_index = jnp.arange(half_rot, dtype=jnp.float32)
    frequency = jnp.exp(freq_index * (-2.0 * math.log(10000.0) / ROT))
    angles = jnp.arange(SEQ, dtype=jnp.float32)[:, None] * frequency[None, :]
    return (jnp.cos(angles), jnp.sin(angles))

def rotate(operand, cos_table, sine_table):
    half_rot = ROT // 2
    first_half = operand[..., :half_rot]
    second_half = operand[..., half_rot:ROT]
    cos_part = cos_table[None, :, None, :]
    sine_part = sine_table[None, :, None, :]
    return jnp.concatenate([first_half * cos_part - second_half * sine_part, second_half * cos_part + first_half * sine_part, operand[..., ROT:]], -1)

def attention_heads(queries, keys_rot, values):
    group_seqs = queries.shape[0]
    score_scale = HEAD_DIM ** (-0.5)
    row_ids = jnp.arange(SEQ)[:, None]
    col_ids = jnp.arange(SEQ)[None, :]
    causal = col_ids <= row_ids

    def fold_heads(tensor_in):
        return jnp.transpose(tensor_in, (0, 2, 1, 3)).reshape(group_seqs * HEADS, SEQ, HEAD_DIM)

    def one_head(triple):
        head_query, head_key, head_value = triple
        scores = low_back(jnp.dot(head_query, head_key.T, precision=PRECISE) * score_scale)
        masked = jnp.where(causal, scores, -1e+30)
        row_peak = lax.optimization_barrier(jnp.max(masked, -1, keepdims=True))
        weights = jnp.exp(masked - row_peak)
        probabilities = low(weights / lax.optimization_barrier(jnp.sum(weights, -1, keepdims=True)))
        return jnp.dot(probabilities, head_value, precision=PRECISE)
    context = lax.map(jax.checkpoint(one_head), (fold_heads(queries), fold_heads(keys_rot), fold_heads(values)))
    context = jnp.transpose(context.reshape(group_seqs, HEADS, SEQ, HEAD_DIM), (0, 2, 1, 3))
    return context.reshape(group_seqs * SEQ, D)

def forward(params, x_float):
    gain_one, shift_one, gain_two, shift_two, w_qkv, b_qkv, w_dense, b_dense, w_first, b_first, w_second, b_second = params
    seq_count = x_float.shape[0] // SEQ
    attn_in = low(normalize(x_float, gain_one, shift_one))
    mlp_in = low(normalize(x_float, gain_two, shift_two))
    qkv_all = low_back(jnp.dot(attn_in, w_qkv, precision=PRECISE) + b_qkv)
    qkv_all = qkv_all.reshape(seq_count, SEQ, HEADS, 3, HEAD_DIM)
    cos_table, sine_table = rotary_tables()
    queries = low_back(low(rotate(qkv_all[..., 0, :], cos_table, sine_table)))
    keys_rot = low_back(low(rotate(qkv_all[..., 1, :], cos_table, sine_table)))
    values = low(qkv_all[..., 2, :])
    context = low_back(low(attention_heads(queries, keys_rot, values)))
    attn_out = jnp.dot(context, w_dense.T, precision=PRECISE) + b_dense
    hidden = low_back(jnp.dot(mlp_in, w_first, precision=PRECISE) + b_first)
    activated = low(jax.nn.gelu(hidden, approximate=False))
    mlp_out = jnp.dot(activated, w_second.T, precision=PRECISE) + b_second
    return x_float + attn_out + mlp_out

def reference(layer_input, ln1_gain, ln1_bias, ln2_gain, ln2_bias, qkv_weight, qkv_bias, dense_weight, dense_bias, fc1_weight, fc1_bias, fc2_weight, fc2_bias, cotangent):
    params = (ln1_gain.astype(jnp.float32), ln1_bias.astype(jnp.float32), ln2_gain.astype(jnp.float32), ln2_bias.astype(jnp.float32), qkv_weight.astype(jnp.float32), qkv_bias.astype(jnp.float32), dense_weight.astype(jnp.float32), dense_bias.astype(jnp.float32), fc1_weight.astype(jnp.float32), fc1_bias.astype(jnp.float32), fc2_weight.astype(jnp.float32), fc2_bias.astype(jnp.float32))
    total_seqs = layer_input.shape[0] // SEQ
    group_seqs = math.gcd(total_seqs, max(1, 4096 // SEQ))
    group_count = total_seqs // group_seqs
    x_groups = layer_input.astype(jnp.float32).reshape(group_count, group_seqs * SEQ, D)
    cot_groups = cotangent.astype(jnp.float32).reshape(group_count, group_seqs * SEQ, D)

    def group_step(running, pair_in):
        x_group, cot_group = pair_in
        result, pullback = jax.vjp(forward, params, x_group)
        param_grads, x_grad = pullback(cot_group)
        running = jax.tree.map(jnp.add, running, param_grads)
        return (running, (result.astype(jnp.bfloat16), x_grad.astype(jnp.bfloat16)))
    initial = tuple((jnp.zeros(p_arr.shape, jnp.float32) for p_arr in params))
    grads, (outputs, in_grads) = lax.scan(group_step, initial, (x_groups, cot_groups))
    return (outputs.reshape(layer_input.shape[0], D), in_grads.reshape(layer_input.shape[0], D), grads[0], grads[1], grads[2], grads[3], grads[4], grads[5], grads[6], grads[7], grads[8], grads[9], grads[10], grads[11])
```

```python
from functools import partial
import math

import jax
import jax.numpy as jnp
from jax import lax
from jax.experimental import pallas as pl
from jax.experimental.pallas import tpu as pltpu
from jax.sharding import PartitionSpec as P

HEADS = 8
SEQ = 1024
HEAD_DIM = 256
ROT = 64
EPSILON = 1e-05
VMEM_LIMIT = 60 * 1024 * 1024

f32 = jnp.float32
bf16 = jnp.bfloat16
NN = (((1,), (0,)), ((), ()))
NT = (((1,), (1,)), ((), ()))
TN = (((0,), (0,)), ((), ()))


def dot(a, b, dims=NN):
    return lax.dot_general(a, b, dims, preferred_element_type=f32)


def cost(flops, nbytes, transcendentals=0):
    return pl.CostEstimate(flops=flops, bytes_accessed=nbytes, transcendentals=transcendentals)


def params(**kw):
    return pltpu.CompilerParams(vmem_limit_bytes=VMEM_LIMIT, **kw)


def whole(shape):
    return pl.BlockSpec(shape, lambda *_: (0,) * len(shape))


def rotary_tables():
    half_rot = ROT // 2
    lane = jnp.arange(128)
    freq_index = (lane % half_rot).astype(f32)
    frequency = jnp.exp(freq_index * (-2.0 * math.log(10000.0) / ROT))
    angles = jnp.arange(SEQ, dtype=f32)[:, None] * frequency[None, :]
    cos_table = jnp.where(lane < ROT, jnp.cos(angles), 1.0)
    sine = jnp.sin(angles)
    sine_table = jnp.where(lane < half_rot, -sine, jnp.where(lane < ROT, sine, 0.0))
    return cos_table, sine_table


def turn(block, cos_table, sine_table):
    half_rot = ROT // 2
    head = block[:, :128]
    lane = lax.broadcasted_iota(jnp.int32, head.shape, 1)
    other = jnp.where(lane < half_rot, pltpu.roll(head, 128 - half_rot, 1), pltpu.roll(head, half_rot, 1))
    return jnp.concatenate([head * cos_table + other * sine_table, block[:, 128:]], 1)


def qkv_kernel(x_ref, w_ref, b_ref, cos_ref, sin_ref, o_ref, *, chunk):
    rows = x_ref.shape[0]
    role = lax.rem(pl.program_id(0), 3)
    w = w_ref[...]
    b = b_ref[...].astype(f32)
    for r in range(0, rows, chunk):
        part = pl.ds(r, chunk)
        seq_part = pl.ds(r % SEQ, chunk)
        acc = dot(x_ref[part, :], w) + b

        @pl.when(role < 2)
        def _():
            o_ref[part, :] = turn(acc, cos_ref[seq_part, :], sin_ref[seq_part, :]).astype(bf16)

        @pl.when(role == 2)
        def _():
            o_ref[part, :] = acc.astype(bf16)


def qkv_call(attn_in, weight, bias, cos_table, sin_table):
    rows, width = attn_in.shape
    columns = weight.shape[1]
    return pl.pallas_call(
        partial(qkv_kernel, chunk=min(rows, 256)),
        grid=(columns // HEAD_DIM,),
        in_specs=[
            whole((rows, width)),
            pl.BlockSpec((width, HEAD_DIM), lambda j: (0, j)),
            pl.BlockSpec((1, HEAD_DIM), lambda j: (0, j)),
            whole((SEQ, 128)),
            whole((SEQ, 128)),
        ],
        out_specs=pl.BlockSpec((rows, HEAD_DIM), lambda j: (0, j)),
        out_shape=jax.ShapeDtypeStruct((rows, columns), bf16),
        compiler_params=params(),
        cost_estimate=cost(2 * rows * width * columns, 2 * (rows * width + width * columns + rows * columns)),
        name="qkv",
    )(attn_in, weight, bias.reshape(1, columns), cos_table, sin_table)


def attention_kernel(q_ref, k_ref, v_ref, g_ref, cos_ref, sin_ref, ctx_ref, grad_ref, bias_ref, dk_ref, dv_ref, *, block):
    scale = HEAD_DIM ** (-0.5)
    for i in reversed(range(SEQ // block)):
        rows = pl.ds(i * block, block)
        key_end = (i + 1) * block
        keys = pl.ds(0, key_end)
        q, g = q_ref[rows, :], g_ref[rows, :]
        k, v = k_ref[keys, :], v_ref[keys, :]
        scores = dot(q, k, NT) * scale
        row_id = i * block + lax.broadcasted_iota(jnp.int32, scores.shape, 0)
        col_id = lax.broadcasted_iota(jnp.int32, scores.shape, 1)
        scores = jnp.where(col_id <= row_id, scores, -1e30)
        weights = jnp.exp(scores - jnp.max(scores, -1, keepdims=True))
        probs = weights / jnp.sum(weights, -1, keepdims=True)
        low = probs.astype(bf16)
        ctx_ref[rows, :] = dot(low, v).astype(bf16)
        prob_grad = dot(g, v, NT)
        delta = jnp.sum(probs * prob_grad, -1, keepdims=True)
        score_grad = (probs * (prob_grad - delta)).astype(bf16)
        dv = dot(low, g, TN)
        dk = dot(score_grad, q, TN)
        if i == SEQ // block - 1:
            dv_ref[...] = dv
            dk_ref[...] = dk
        else:
            dv_ref[keys, :] += dv
            dk_ref[keys, :] += dk
        dq = (dot(score_grad, k) * scale).astype(bf16).astype(f32)
        grad_ref[rows, 0:HEAD_DIM] = turn(dq, cos_ref[rows, :], -sin_ref[rows, :]).astype(bf16)
    dk = (dk_ref[...] * scale).astype(bf16).astype(f32)
    grad_ref[:, HEAD_DIM : 2 * HEAD_DIM] = turn(dk, cos_ref[...], -sin_ref[...]).astype(bf16)
    grad_ref[:, 2 * HEAD_DIM :] = dv_ref[...].astype(bf16)
    sums = jnp.sum(grad_ref[...].astype(f32), 0, keepdims=True)

    @pl.when(pl.program_id(1) == 0)
    def _():
        bias_ref[...] = sums

    @pl.when(pl.program_id(1) > 0)
    def _():
        bias_ref[...] += sums


def attention_call(qkv, context_grad, cos_table, sin_table):
    rows, columns = qkv.shape
    heads = columns // (3 * HEAD_DIM)
    seqs = rows // SEQ
    tile = (SEQ, HEAD_DIM)
    return pl.pallas_call(
        partial(attention_kernel, block=256),
        grid=(heads, seqs),
        in_specs=[
            pl.BlockSpec(tile, lambda h, s: (s, 3 * h)),
            pl.BlockSpec(tile, lambda h, s: (s, 3 * h + 1)),
            pl.BlockSpec(tile, lambda h, s: (s, 3 * h + 2)),
            pl.BlockSpec(tile, lambda h, s: (s, h)),
            whole((SEQ, 128)),
            whole((SEQ, 128)),
        ],
        out_specs=[
            pl.BlockSpec(tile, lambda h, s: (s, h)),
            pl.BlockSpec((SEQ, 3 * HEAD_DIM), lambda h, s: (s, h)),
            pl.BlockSpec((1, 3 * HEAD_DIM), lambda h, s: (0, h)),
        ],
        out_shape=[
            jax.ShapeDtypeStruct((rows, heads * HEAD_DIM), bf16),
            jax.ShapeDtypeStruct((rows, columns), bf16),
            jax.ShapeDtypeStruct((1, columns), f32),
        ],
        scratch_shapes=[pltpu.VMEM((SEQ, HEAD_DIM), f32), pltpu.VMEM((SEQ, HEAD_DIM), f32)],
        compiler_params=params(),
        cost_estimate=cost(8 * SEQ * SEQ * HEAD_DIM * heads * seqs, 2 * rows * (2 * columns + 2 * heads * HEAD_DIM), heads * seqs * SEQ * SEQ),
        name="attention",
    )(qkv, qkv, qkv, context_grad, cos_table, sin_table)


def mlp_kernel(x_ref, c_ref, w1_ref, w2_ref, b_ref, act_ref, grad_ref, bias_ref, *, chunk):
    rows = x_ref.shape[0]
    w1, w2 = w1_ref[...], w2_ref[...]
    b = b_ref[...].astype(f32)
    sums = jnp.zeros(bias_ref.shape, f32)
    for r in range(0, rows, chunk):
        part = pl.ds(r, chunk)
        hidden = dot(x_ref[part, :], w1) + b
        above = dot(c_ref[part, :], w2)
        cdf = 0.5 + 0.5 * lax.erf(hidden * (2.0**-0.5))
        density = jnp.exp(hidden * hidden * -0.5) * ((2.0 * math.pi) ** -0.5)
        act_ref[part, :] = (hidden * cdf).astype(bf16)
        low = (above * (cdf + hidden * density)).astype(bf16)
        grad_ref[part, :] = low
        sums = sums + jnp.sum(low.astype(f32), 0, keepdims=True)
    bias_ref[...] = sums


def mlp_call(mlp_in, cotangent, fc1, fc2, bias, tile=256):
    rows, width = mlp_in.shape
    columns = fc1.shape[1]
    column_tile = pl.BlockSpec((width, tile), lambda j: (0, j))
    row_tile = pl.BlockSpec((1, tile), lambda j: (0, j))
    out_tile = pl.BlockSpec((rows, tile), lambda j: (0, j))
    return pl.pallas_call(
        partial(mlp_kernel, chunk=min(rows, 256)),
        grid=(columns // tile,),
        in_specs=[whole((rows, width)), whole((rows, width)), column_tile, column_tile, row_tile],
        out_specs=[out_tile, out_tile, row_tile],
        out_shape=[
            jax.ShapeDtypeStruct((rows, columns), bf16),
            jax.ShapeDtypeStruct((rows, columns), bf16),
            jax.ShapeDtypeStruct((1, columns), f32),
        ],
        compiler_params=params(),
        cost_estimate=cost(4 * rows * width * columns, 4 * (rows * width + width * columns + rows * columns), 2 * rows * columns),
        name="mlp",
    )(mlp_in, cotangent, fc1, fc2, bias.reshape(1, columns))


def output_kernel(ctx_ref, act_ref, dense_ref, fc2_ref, o_ref, *, chunk):
    for r in range(0, ctx_ref.shape[0], chunk):
        part = pl.ds(r, chunk)
        o_ref[part, :] = (dot(ctx_ref[part, :], dense_ref[...], NT) + dot(act_ref[part, :], fc2_ref[...], NT)).astype(bf16)


def output_call(context, activated, dense, fc2, tile=256):
    rows = context.shape[0]
    width = dense.shape[0]
    a, b = context.shape[1], activated.shape[1]
    return pl.pallas_call(
        partial(output_kernel, chunk=min(rows, 256)),
        grid=(width // tile,),
        in_specs=[
            whole((rows, a)),
            whole((rows, b)),
            pl.BlockSpec((tile, a), lambda j: (j, 0)),
            pl.BlockSpec((tile, b), lambda j: (j, 0)),
        ],
        out_specs=pl.BlockSpec((rows, tile), lambda j: (0, j)),
        out_shape=jax.ShapeDtypeStruct((rows, width), bf16),
        compiler_params=params(),
        cost_estimate=cost(2 * rows * width * (a + b), 2 * (rows + width) * (a + b) + 2 * rows * width),
        name="output",
    )(context, activated, dense, fc2)


def input_kernel(g1_ref, g2_ref, w1_ref, w2_ref, x_ref, mean_ref, rstd_ref, gain1_ref, gain2_ref, o_ref, sum_ref, *, chunk):
    rows = g1_ref.shape[0]
    gain1, gain2 = gain1_ref[...], gain2_ref[...]
    sums = [jnp.zeros((1, o_ref.shape[1]), f32) for _ in range(4)]
    for r in range(0, rows, chunk):
        part = pl.ds(r, chunk)
        first = dot(g1_ref[part, :], w1_ref[...], NT)
        second = dot(g2_ref[part, :], w2_ref[...], NT)
        u = (x_ref[part, :].astype(f32) - mean_ref[part, :]) * rstd_ref[part, :]
        o_ref[part, :] = (first * gain1 + second * gain2).astype(bf16)
        for n, term in enumerate((first * u, first, second * u, second)):
            sums[n] = sums[n] + jnp.sum(term, 0, keepdims=True)
    sum_ref[...] = jnp.concatenate(sums, 0)


def input_call(qkv_grad, hidden_grad, qkv_weight, fc1, x, mean, rstd, gain1, gain2, tile=256):
    rows, width = x.shape
    a, b = qkv_grad.shape[1], hidden_grad.shape[1]
    row_tile = pl.BlockSpec((1, tile), lambda j: (0, j))
    out_tile = pl.BlockSpec((rows, tile), lambda j: (0, j))
    return pl.pallas_call(
        partial(input_kernel, chunk=min(rows, 256)),
        grid=(width // tile,),
        in_specs=[
            whole((rows, a)),
            whole((rows, b)),
            pl.BlockSpec((tile, a), lambda j: (j, 0)),
            pl.BlockSpec((tile, b), lambda j: (j, 0)),
            out_tile,
            whole((rows, 1)),
            whole((rows, 1)),
            row_tile,
            row_tile,
        ],
        out_specs=[out_tile, pl.BlockSpec((4, tile), lambda j: (0, j))],
        out_shape=[jax.ShapeDtypeStruct((rows, width), bf16), jax.ShapeDtypeStruct((4, width), f32)],
        compiler_params=params(),
        cost_estimate=cost(2 * rows * width * (a + b), 2 * (rows + width) * (a + b) + 4 * rows * width),
        name="input_grad",
    )(qkv_grad, hidden_grad, qkv_weight, fc1, x, mean, rstd, gain1.reshape(1, width), gain2.reshape(1, width))


def swap(value, axis, bit):
    n = lax.axis_size(axis)
    return lax.ppermute(value, axis, [(i, i ^ (1 << bit)) for i in range(n)])


def my_bit(axis, bit):
    return lax.rem(lax.div(lax.axis_index(axis), 1 << bit), 2)


def take(value, axis, index):
    return lax.dynamic_index_in_dim(value, index, axis, keepdims=False)


def place(remaining, bit):
    return sorted(remaining, reverse=True).index(bit)


def weight_grad(lhs, rhs, order):
    n = lax.axis_size("dp")
    bits = n.bit_length() - 1
    rows = lhs.shape[1] // n
    tokens, columns = rhs.shape
    left = lhs.reshape((tokens,) + (2,) * bits + (rows,))
    remaining = list(range(bits))

    def product(part):
        return dot(part.reshape(tokens, -1), rhs, TN)

    first, second = order[0], order[1]
    at = 1 + place(remaining, first)
    mine = my_bit("dp", first)
    sent = product(take(left, at, 1 - mine)).astype(bf16)
    left = take(left, at, mine)
    received = swap(sent, "dp", first)
    remaining.remove(first)
    shape = (2,) * (bits - 1) + (rows, columns)
    at = place(remaining, second)
    mine = my_bit("dp", second)
    received = received.reshape(shape)

    def with_received(which):
        part = product(take(left, 1 + at, which))
        return part + take(received, at, which).reshape(part.shape).astype(f32)

    sent = with_received(1 - mine).astype(bf16)
    kept = with_received(mine).astype(bf16)
    remaining.remove(second)
    got = swap(sent, "dp", second)
    for bit in order[2:]:
        shape = (2,) * len(remaining) + (rows, columns)
        at = place(remaining, bit)
        mine = my_bit("dp", bit)
        kept, got = kept.reshape(shape), got.reshape(shape)

        def total(which):
            return take(kept, at, which).astype(f32) + take(got, at, which).astype(f32)

        sent, kept = total(1 - mine).astype(bf16), total(mine).astype(bf16)
        remaining.remove(bit)
        got = swap(sent, "dp", bit)
    return (kept.astype(f32) + got.astype(f32)).reshape(rows, columns)


def tensor_scatter(part):
    bits = lax.axis_size("tensor").bit_length() - 1
    total = part
    for bit in range(bits):
        halves = total.reshape(2 ** (bits - 1 - bit), 2, -1, part.shape[1]) if bit == 0 else total.reshape(
            2 ** (bits - 1 - bit), 2, -1, part.shape[1]
        )
        mine = my_bit("tensor", bit)
        got = swap(take(halves, 1, 1 - mine).astype(bf16), "tensor", bit)
        total = take(halves, 1, mine).astype(f32) + got.astype(f32)
    return total.reshape(-1, part.shape[1])


def tensor_gather(piece):
    n = lax.axis_size("tensor")
    bits = n.bit_length() - 1
    rows, width = piece.shape
    me = lax.axis_index("tensor")
    held = [(me, piece)]
    for bit in reversed(range(bits)):
        held = held + [(lax.bitwise_xor(owner, 1 << bit), swap(value, "tensor", bit)) for owner, value in held]
    whole_array = jnp.zeros((n * rows, width), piece.dtype)
    for owner, value in held:
        whole_array = lax.dynamic_update_slice(whole_array, value, (owner * rows, 0))
    return whole_array


def sum_over(value, axes):
    for axis in axes:
        for bit in range(lax.axis_size(axis).bit_length() - 1):
            value = value + swap(value, axis, bit)
    return value


def on_device(
    layer_input,
    ln1_gain,
    ln1_bias,
    ln2_gain,
    ln2_bias,
    qkv_weight,
    qkv_bias,
    dense_weight,
    dense_bias,
    fc1_weight,
    fc1_bias,
    fc2_weight,
    fc2_bias,
    cotangent,
):
    rows, width = layer_input.shape
    x = layer_input.astype(f32)
    mean = jnp.mean(x, -1, keepdims=True)
    centred = x - mean
    rstd = lax.rsqrt(jnp.mean(centred * centred, -1, keepdims=True) + EPSILON)
    u = centred * rstd
    gain_one, gain_two = ln1_gain.astype(f32), ln2_gain.astype(f32)
    attn_in = (u * gain_one + ln1_bias.astype(f32)).astype(bf16)
    mlp_in = (u * gain_two + ln2_bias.astype(f32)).astype(bf16)
    cos_table, sin_table = rotary_tables()

    bits = list(range(lax.axis_size("dp").bit_length() - 1))
    x_first = bits
    z_first = [bits[1], bits[0]] + bits[2:]

    activated, hidden_grad, fc1_bias_grad = mlp_call(mlp_in, cotangent, fc1_weight, fc2_weight, fc1_bias)
    half = activated.shape[1] // 2
    grad_fc2 = jnp.concatenate(
        [
            weight_grad(cotangent, activated[:, :half], x_first),
            weight_grad(cotangent, activated[:, half:], z_first),
        ],
        1,
    )
    grad_fc1 = weight_grad(mlp_in, hidden_grad, x_first)

    qkv = qkv_call(attn_in, qkv_weight, qkv_bias, cos_table, sin_table)
    context_grad = dot(cotangent, dense_weight).astype(bf16)
    context, qkv_grad, qkv_bias_grad = attention_call(qkv, context_grad, cos_table, sin_table)
    grad_dense = weight_grad(cotangent, context, z_first)
    grad_qkv = weight_grad(attn_in, qkv_grad, x_first)

    partial_in, norm_sums = input_call(
        qkv_grad, hidden_grad, qkv_weight, fc1_weight, layer_input, mean, rstd, gain_one, gain_two
    )
    partial_out = output_call(context, activated, dense_weight, fc2_weight)

    n_tensor = lax.axis_size("tensor")
    own = lax.axis_index("tensor")

    def own_rows(value):
        return lax.dynamic_slice_in_dim(value, own * (rows // n_tensor), rows // n_tensor, 0)

    w = tensor_scatter(partial_in)
    own_u = (own_rows(layer_input).astype(f32) - own_rows(mean)) * own_rows(rstd)
    term = own_rows(rstd) * (w - jnp.mean(w, -1, keepdims=True) - own_u * jnp.mean(w * own_u, -1, keepdims=True))
    input_grad = tensor_gather((own_rows(cotangent).astype(f32) + term).astype(bf16))

    bias_total = dense_bias.astype(f32) + fc2_bias.astype(f32)
    output = tensor_gather((own_rows(layer_input).astype(f32) + tensor_scatter(partial_out) + bias_total).astype(bf16))

    out_bias_grad = jnp.sum(cotangent.astype(f32), 0)
    norm_sums = sum_over(norm_sums.reshape(-1), ("tensor",))
    sizes = [width * 4, qkv_bias_grad.shape[1], fc1_bias_grad.shape[1], width]
    small = sum_over(
        jnp.concatenate([norm_sums, qkv_bias_grad.reshape(-1), fc1_bias_grad.reshape(-1), out_bias_grad]), ("dp",)
    )
    offsets = [sum(sizes[:n]) for n in range(5)]
    norm_sums, qkv_bias_grad, fc1_bias_grad, out_bias_grad = (small[offsets[n] : offsets[n + 1]] for n in range(4))
    gain_grad_one, shift_grad_one, gain_grad_two, shift_grad_two = (
        norm_sums[n * width : (n + 1) * width] for n in range(4)
    )
    return (
        output,
        input_grad,
        gain_grad_one,
        shift_grad_one,
        gain_grad_two,
        shift_grad_two,
        grad_qkv,
        qkv_bias_grad,
        grad_dense,
        out_bias_grad,
        grad_fc1,
        fc1_bias_grad,
        grad_fc2,
        out_bias_grad,
    )


def solution(mesh):
    in_specs = (
        P("dp", None),
        P(),
        P(),
        P(),
        P(),
        P(None, "tensor"),
        P("tensor"),
        P(None, "tensor"),
        P(),
        P(None, "tensor"),
        P("tensor"),
        P(None, "tensor"),
        P(),
        P("dp", None),
    )
    out_specs = (
        P("dp", None),
        P("dp", None),
        P(),
        P(),
        P(),
        P(),
        P("dp", "tensor"),
        P("tensor"),
        P("dp", "tensor"),
        P(),
        P("dp", "tensor"),
        P("tensor"),
        P("dp", "tensor"),
        P(),
    )
    return jax.shard_map(
        on_device, mesh=mesh, in_specs=in_specs, out_specs=out_specs, check_vma=False
    )
```

```python
import itertools
import math
from functools import partial

import jax
import jax.numpy as jnp
from jax import lax
from jax.experimental import pallas as pl
from jax.experimental.pallas import tpu as pltpu
from jax.sharding import PartitionSpec as P

HEADS = 8
SEQ = 1024
HEAD_DIM = 256
ROT = 64
EPSILON = 1e-05
VMEM_LIMIT = 63 * 1024 * 1024

f32 = jnp.float32
bf16 = jnp.bfloat16
NN = (((1,), (0,)), ((), ()))
NT = (((1,), (1,)), ((), ()))
TN = (((0,), (0,)), ((), ()))


def dot(a, b, dims=NN):
    return lax.dot_general(a, b, dims, preferred_element_type=f32)


def turn(block, cos_table, sine_table):
    half_rot = ROT // 2
    head = block[:, :128]
    lane = lax.broadcasted_iota(jnp.int32, head.shape, 1)
    other = jnp.where(lane < half_rot, pltpu.roll(head, 128 - half_rot, 1), pltpu.roll(head, half_rot, 1))
    return jnp.concatenate([head * cos_table + other * sine_table, block[:, 128:]], 1)


def angle_tables():
    half_rot = ROT // 2
    lane = jnp.arange(128)
    frequency = jnp.exp((lane % half_rot).astype(f32) * (-2.0 * math.log(10000.0) / ROT))
    frequency = jnp.where(lane < ROT, frequency, 0.0)
    step = jnp.arange(32, dtype=f32)
    angles = jnp.concatenate([step, 32.0 * step])[:, None] * frequency[None, :]
    cos, sin = jnp.cos(angles), jnp.sin(angles)
    sign = jnp.where(lane < half_rot, -1.0, 1.0)[None, :]
    return jnp.concatenate([cos[:32], sin[:32], cos[32:], sin[32:], jnp.broadcast_to(sign, (8, 128))], 0)


CHUNK = 512
MESH = pl.DeviceIdType.MESH
VEC_ROWS = 8


class Slots:
    def __init__(self, count):
        self.free = [(n, []) for n in range(count)]

    def take(self):
        slot, waits = self.free.pop(0)
        for wait in waits:
            wait()
        return slot

    def give(self, slot, *waits):
        self.free.append((slot, list(waits)))

    def drain(self):
        for _, waits in self.free:
            for wait in waits:
                wait()


def layer_kernel(
    x_hbm, c_hbm, vec_in, table_in, fc1_hbm, fc2_hbm, wqkv_hbm, dense_hbm,
    out_hbm, grad_hbm, keep_hbm, last_hbm, small_out, r1_hbm, r2_hbm, core_hbm, y_hbm,
    attn_in, mlp_in, cot, act, hg, qg, ctx, mean_ref, rstd_ref, cos_ref, sin_ref, vec, w1buf, w2buf,
    s1, s2, s3, k2, ld1, ldm, ld2, piece, xrow, small, small_in,
    load_sem, weight_sem, send_sem, recv_sem, keep_sem,
    *, jobs, orders, heads, block=256,
):
    rows, width = cot.shape
    hidden = act.shape[1]
    nb = width // 8
    quarter = rows // 4
    me, own = lax.axis_index("dp"), lax.axis_index("tensor")
    dp_bits = [lax.rem(lax.div(me, 1 << k), 2) for k in range(3)]
    t_bits = [lax.rem(lax.div(own, 1 << k), 2) for k in range(2)]

    def dp_flip(*bits):
        return me + sum((1 - 2 * dp_bits[k]) * (1 << k) for k in bits)

    def t_flip(*bits):
        return own + sum((1 - 2 * t_bits[k]) * (1 << k) for k in bits)

    def dp_partner(bit):
        return (dp_flip(bit), own)

    def t_partner(bit):
        return (me, t_flip(bit))

    partners = [dp_partner(k) for k in range(3)] + [t_partner(k) for k in range(2)]
    barrier = pltpu.get_barrier_semaphore()
    for partner in partners:
        pl.semaphore_signal(barrier, inc=1, device_id=partner, device_id_type=MESH)

    copies = itertools.count()

    def send_copy(src, dst, partner):
        n = next(copies)
        copy = pltpu.make_async_remote_copy(
            src_ref=src, dst_ref=dst, send_sem=send_sem.at[n], recv_sem=recv_sem.at[n], device_id=partner, device_id_type=MESH
        )
        copy.start()
        return copy

    loads = itertools.count()

    def load(src, dst):
        copy = pltpu.make_async_copy(src, dst, load_sem.at[next(loads)])
        copy.start()
        return copy

    load_x = load(x_hbm, act)
    load_c = load(c_hbm, cot)

    def mlp_weights(j):
        slot = j % 2
        at = pl.ds(j * CHUNK, CHUNK)
        return [load(fc1_hbm.at[:, at], w1buf.at[slot]), load(fc2_hbm.at[:, at], w2buf.at[slot])]

    def head_weights(h):
        slot = h % 2
        base = 3 * h * HEAD_DIM
        return [
            load(wqkv_hbm.at[:, pl.ds(base, 2 * HEAD_DIM)], w1buf.at[slot]),
            load(wqkv_hbm.at[:, pl.ds(base + 2 * HEAD_DIM, HEAD_DIM)], w2buf.at[slot, :, pl.ds(0, HEAD_DIM)]),
            load(dense_hbm.at[:, pl.ds(h * HEAD_DIM, HEAD_DIM)], w2buf.at[slot, :, pl.ds(HEAD_DIM, HEAD_DIM)]),
        ]

    weights = {("mlp", 0): mlp_weights(0), ("mlp", 1): mlp_weights(1)}
    tiles = hidden // CHUNK

    small[...] = jnp.zeros_like(small)
    per_row = width // 128
    for n in range(VEC_ROWS):
        for i in range(per_row):
            vec[n : n + 1, i * 128 : (i + 1) * 128] = vec_in[n * per_row + i : n * per_row + i + 1, :]
    low_cos, low_sin = table_in[0:32, :], table_in[32:64, :]
    sign = table_in[128:129, :]
    for n in range(SEQ // 32):
        high_cos, high_sin = table_in[64 + n : 65 + n, :], table_in[96 + n : 97 + n, :]
        cos_ref[n * 32 : (n + 1) * 32, :] = high_cos * low_cos - high_sin * low_sin
        sin_ref[n * 32 : (n + 1) * 32, :] = sign * (high_sin * low_cos + high_cos * low_sin)

    load_x.wait()

    def norm_rows(i, _):
        part = pl.ds(pl.multiple_of(i * 128, 128), 128)
        x = act[part, :].astype(f32)
        mean = jnp.mean(x, -1, keepdims=True)
        centred = x - mean
        rstd = lax.rsqrt(jnp.mean(centred * centred, -1, keepdims=True) + EPSILON)
        u = centred * rstd
        attn_in[part, :] = (u * vec[0:1, :] + vec[1:2, :]).astype(bf16)
        mlp_in[part, :] = (u * vec[2:3, :] + vec[3:4, :]).astype(bf16)
        mean_ref[part, :] = mean
        rstd_ref[part, :] = rstd
        return 0

    lax.fori_loop(0, rows // 128, norm_rows, 0)
    load_c.wait()
    pl.semaphore_wait(barrier, len(partners))

    s1_slots, s2_slots, s3_slots, k2_slots = Slots(s1.shape[0]), Slots(s2.shape[0]), Slots(s3.shape[0]), Slots(k2.shape[0])
    state = {}

    def operands(c):
        n_fc = hidden // CHUNK
        n_qkv = qg.shape[1] // CHUNK
        if c < n_fc:
            return cot, act, c
        if c < 2 * n_fc:
            return mlp_in, hg, c - n_fc
        if c < 2 * n_fc + n_qkv:
            return attn_in, qg, c - 2 * n_fc
        return cot, ctx, c - 2 * n_fc - n_qkv

    def block_of(lhs, index):
        return lhs[:, pl.ds(pl.multiple_of(index * nb, nb), nb)]

    def w1(c):
        lhs, rhs, j = operands(c)
        one, two, three = orders[c]
        slot = s1_slots.take()
        base = dp_flip(one, two, three)

        def body(n, _):
            second, third = n // 2, lax.rem(n, 2)
            index = base - second * (1 - 2 * dp_bits[two]) * (1 << two) - third * (1 - 2 * dp_bits[three]) * (1 << three)
            s1[slot, n] = dot(block_of(lhs, index), rhs[:, j * CHUNK : (j + 1) * CHUNK], TN).astype(bf16)
            return 0

        lax.fori_loop(0, 4, body, 0)
        copy = send_copy(s1.at[slot], r1_hbm.at[c], dp_partner(one))
        s1_slots.give(slot, copy.wait_send)
        state[c] = copy

    def w2(c):
        lhs, rhs, j = operands(c)
        one, two, three = orders[c]
        state[c].wait_recv()
        loaded = load(r1_hbm.at[c], ld1)
        slot, kept = s2_slots.take(), k2_slots.take()
        loaded.wait()

        def part(base, n, out):
            def body(i, _):
                index = base - i * (1 - 2 * dp_bits[three]) * (1 << three)
                out[i] = (dot(block_of(lhs, index), rhs[:, j * CHUNK : (j + 1) * CHUNK], TN) + ld1[n + i].astype(f32)).astype(bf16)
                return 0

            lax.fori_loop(0, 2, body, 0)

        part(dp_flip(two, three), 0, s2.at[slot])
        copy = send_copy(s2.at[slot], r2_hbm.at[c], dp_partner(two))
        s2_slots.give(slot, copy.wait_send)
        part(dp_flip(three), 2, k2.at[kept])
        state[c] = (copy, kept)

    def a3(c):
        copy, kept = state[c]
        three = orders[c][2]
        copy.wait_recv()
        loaded = load(r2_hbm.at[c], ld2)
        slot = s3_slots.take()
        loaded.wait()
        s3[slot] = (k2[kept, 0].astype(f32) + ld2[0].astype(f32)).astype(bf16)
        columns = pl.ds(c * CHUNK, CHUNK)
        copy = send_copy(s3.at[slot], last_hbm.at[:, columns], dp_partner(three))
        s3_slots.give(slot, copy.wait_send)
        k2[kept, 1] = (k2[kept, 1].astype(f32) + ld2[1].astype(f32)).astype(bf16)
        keep = pltpu.make_async_copy(k2.at[kept, 1], keep_hbm.at[:, columns], keep_sem.at[c])
        keep.start()
        k2_slots.give(kept, keep.wait)
        state[c] = copy

    def mlp(j):
        slot = j % 2
        for copy in weights.pop(("mlp", j)):
            copy.wait()
        at = j * CHUNK
        bias = vec[4:5, at : at + CHUNK]

        def body(i, sums):
            part = pl.ds(pl.multiple_of(i * block, block), block)
            h = dot(mlp_in[part, :], w1buf[slot]) + bias
            above = dot(cot[part, :], w2buf[slot])
            cdf = 0.5 + 0.5 * lax.erf(h * (2.0**-0.5))
            density = jnp.exp(h * h * -0.5) * ((2.0 * math.pi) ** -0.5)
            act[part, at : at + CHUNK] = (h * cdf).astype(bf16)
            low = (above * (cdf + h * density)).astype(bf16)
            hg[part, at : at + CHUNK] = low
            above_sum = jnp.sum(cot[part, at : at + CHUNK].astype(f32), 0, keepdims=True)
            return sums[0] + jnp.sum(low.astype(f32), 0, keepdims=True), sums[1] + above_sum

        zero = jnp.zeros((1, CHUNK), f32)
        bias_sum, above_sum = lax.fori_loop(0, rows // block, body, (zero, zero))
        small[4:5, at : at + CHUNK] = bias_sum
        small[6:7, at : at + CHUNK] = above_sum
        if j + 2 < tiles:
            weights["mlp", j + 2] = mlp_weights(j + 2)
        else:
            h = j + 2 - tiles
            weights["head", h] = head_weights(h)

    def attention(h):
        slot = h % 2
        for copy in weights.pop(("head", h)):
            copy.wait()
        base = 3 * h * HEAD_DIM
        scale = HEAD_DIM ** (-0.5)

        def scoped(qkv_ref, g_ref, dk_ref, dv_ref):
            def project(i, _):
                part = pl.ds(pl.multiple_of(i * block, block), block)
                acc = dot(attn_in[part, :], w1buf[slot]) + vec[7:8, base : base + 2 * HEAD_DIM]
                cos, sin = cos_ref[part, :], sin_ref[part, :]
                for n in range(2):
                    at = n * HEAD_DIM
                    qkv_ref[part, at : at + HEAD_DIM] = turn(acc[:, at : at + HEAD_DIM], cos, sin).astype(bf16)
                acc = dot(attn_in[part, :], w2buf[slot, :, 0:HEAD_DIM]) + vec[7:8, base + 2 * HEAD_DIM : base + 3 * HEAD_DIM]
                qkv_ref[part, 2 * HEAD_DIM :] = acc.astype(bf16)
                g_ref[part, :] = dot(cot[part, :], w2buf[slot, :, HEAD_DIM : 2 * HEAD_DIM]).astype(bf16)
                return 0

            lax.fori_loop(0, rows // block, project, 0)
            for i in reversed(range(SEQ // block)):
                part = pl.ds(i * block, block)
                key_end = (i + 1) * block
                keys = pl.ds(0, key_end)
                q, g = qkv_ref[part, 0:HEAD_DIM], g_ref[part, :]
                k, v = qkv_ref[keys, HEAD_DIM : 2 * HEAD_DIM], qkv_ref[keys, 2 * HEAD_DIM :]
                scores = dot(q, k, NT) * scale
                row_id = i * block + lax.broadcasted_iota(jnp.int32, scores.shape, 0)
                col_id = lax.broadcasted_iota(jnp.int32, scores.shape, 1)
                scores = jnp.where(col_id <= row_id, scores, -1e30)
                e = jnp.exp(scores - jnp.max(scores, -1, keepdims=True))
                probs = e / jnp.sum(e, -1, keepdims=True)
                low = probs.astype(bf16)
                ctx[part, h * HEAD_DIM : (h + 1) * HEAD_DIM] = dot(low, v).astype(bf16)
                prob_grad = dot(g, v, NT)
                delta = jnp.sum(probs * prob_grad, -1, keepdims=True)
                score_grad = (probs * (prob_grad - delta)).astype(bf16)
                dv = dot(low, g, TN)
                dk = dot(score_grad, q, TN)
                if i == SEQ // block - 1:
                    dv_ref[...] = dv
                    dk_ref[...] = dk
                else:
                    dv_ref[keys, :] += dv
                    dk_ref[keys, :] += dk
                dq = (dot(score_grad, k) * scale).astype(bf16).astype(f32)
                qg[part, base : base + HEAD_DIM] = turn(dq, cos_ref[part, :], -sin_ref[part, :]).astype(bf16)
            dk = (dk_ref[...] * scale).astype(bf16).astype(f32)
            qg[:, base + HEAD_DIM : base + 2 * HEAD_DIM] = turn(dk, cos_ref[...], -sin_ref[...]).astype(bf16)
            qg[:, base + 2 * HEAD_DIM : base + 3 * HEAD_DIM] = dv_ref[...].astype(bf16)
            head = qg[:, base : base + 3 * HEAD_DIM]
            small[5:6, base : base + 3 * HEAD_DIM] = jnp.sum(head.astype(f32), 0, keepdims=True)

        pl.run_scoped(
            scoped,
            pltpu.VMEM((SEQ, 3 * HEAD_DIM), bf16),
            pltpu.VMEM((SEQ, HEAD_DIM), bf16),
            pltpu.VMEM((SEQ, HEAD_DIM), f32),
            pltpu.VMEM((SEQ, HEAD_DIM), f32),
        )
        if h + 2 < heads:
            weights["head", h + 2] = head_weights(h + 2)

    quarters = [t_flip(0, 1), t_flip(0), t_flip(1), own]

    def quarter_of(n):
        return pl.ds(pl.multiple_of(quarters[n] * quarter, quarter), quarter)

    def back_tiles(buf, first_hbm, first, second_hbm, second, x_tiles, store):
        step = CHUNK // 2

        def scoped(first_w, second_w, x_w, sems):
            def copies_of(d, slot):
                at = pl.ds(pl.multiple_of(d * step, step), step)
                made = [
                    pltpu.make_async_copy(first_hbm.at[at, :], first_w.at[slot], sems.at[slot, 0]),
                    pltpu.make_async_copy(second_hbm.at[at, :], second_w.at[slot], sems.at[slot, 1]),
                ]
                if x_tiles:
                    made.append(pltpu.make_async_copy(x_hbm.at[:, at], x_w.at[slot], sems.at[slot, 2]))
                return made

            n_steps = width // step
            for copy in copies_of(0, 0):
                copy.start()

            def body(e, _):
                for half in range(2):
                    d = 2 * e + half
                    for copy in copies_of(d, half):
                        copy.wait()

                    @pl.when(d + 1 < n_steps)
                    def _():
                        for copy in copies_of(d + 1, 1 - half):
                            copy.start()

                    columns = pl.ds(half * step, step)
                    sums = [jnp.zeros((1, step), f32) for _ in range(4)]
                    for n in range(4):
                        part = quarter_of(n)
                        a = dot(first[part, :], first_w[half], NT)
                        b = dot(second[part, :], second_w[half], NT)
                        at = pl.ds(pl.multiple_of(e * 2 * quarter + (n % 2) * quarter, quarter), quarter)
                        buf[n // 2, at, columns], terms = store(d, part, a, b, x_w.at[half])
                        sums = [s + t for s, t in zip(sums, terms)]
                    if x_tiles:
                        at = pl.ds(pl.multiple_of(d * step, step), step)
                        small[0:4, at] = jnp.concatenate(sums, 0)
                return 0

            lax.fori_loop(0, n_steps // 2, body, 0)

        pl.run_scoped(
            scoped,
            pltpu.VMEM((2, step, first.shape[1]), bf16),
            pltpu.VMEM((2, step, second.shape[1]), bf16),
            pltpu.VMEM((2, rows if x_tiles else 16, step), bf16),
            pltpu.SemaphoreType.DMA((2, 3)),
        )

    def input_tiles():
        step = CHUNK // 2

        def store(d, part, a, b, x_tile):
            at = pl.ds(pl.multiple_of(d * step, step), step)
            u = (x_tile[part, :].astype(f32) - mean_ref[part, :]) * rstd_ref[part, :]
            terms = [jnp.sum(t, 0, keepdims=True) for t in (a * u, a, b * u, b)]
            return (a * vec[0:1, at] + b * vec[2:3, at]).astype(bf16), terms

        back_tiles(w1buf, wqkv_hbm, qg, fc1_hbm, hg, True, store)

    def output_tiles():
        back_tiles(w2buf, dense_hbm, ctx, fc2_hbm, act, False, lambda d, part, a, b, x_tile: ((a + b).astype(bf16), []))

    e_tiles = width // CHUNK
    buffers = (w1buf, w2buf)
    results = (grad_hbm, out_hbm)

    def sum_start(k):
        (input_tiles, output_tiles)[k]()
        state["sum", k] = send_copy(buffers[k].at[0], core_hbm.at[k], t_partner(0))

    def half_of(k, half, dst):
        return [
            load(core_hbm.at[k, pl.ds(e * 2 * quarter + half * quarter, quarter), :], dst.at[e]) for e in range(e_tiles)
        ]

    def sum_middle(k):
        first = state["sum", k]
        first.wait_recv()
        loaded = half_of(k, 0, ld1)
        slot = s1_slots.take()
        for copy in loaded:
            copy.wait()
        for e in range(e_tiles):
            s1[slot, e] = (buffers[k][1, pl.ds(e * 2 * quarter, quarter), :].astype(f32) + ld1[e].astype(f32)).astype(bf16)
        copy = send_copy(s1.at[slot], y_hbm.at[k], t_partner(1))
        s1_slots.give(slot, copy.wait_send)
        first.wait_send()
        state["sum", k] = copy

    own_rows = pl.ds(pl.multiple_of(own * quarter, quarter), quarter)

    def rows_of(index):
        return pl.ds(pl.multiple_of(index * quarter, quarter), quarter)

    def sum_late(k):
        x_load = load(x_hbm.at[own_rows, :], xrow)
        half_loads = half_of(k, 1, ld1)
        state["sum", k].wait_recv()
        y_load = load(y_hbm.at[k], ldm)
        for copy in half_loads + [x_load, y_load]:
            copy.wait()
        totals = [
            buffers[k][1, pl.ds(e * 2 * quarter + quarter, quarter), :].astype(f32) + ld1[e].astype(f32) + ldm[e].astype(f32)
            for e in range(e_tiles)
        ]
        parts = [(e * CHUNK, (e + 1) * CHUNK) for e in range(e_tiles)]
        if k == 0:
            mean, rstd = mean_ref[own_rows, :], rstd_ref[own_rows, :]
            us = [(xrow[:, a:b].astype(f32) - mean) * rstd for a, b in parts]
            mean_w = sum(jnp.sum(t, -1, keepdims=True) for t in totals) * (1.0 / width)
            mean_wu = sum(jnp.sum(t * u, -1, keepdims=True) for t, u in zip(totals, us)) * (1.0 / width)
            for (a, b), t, u in zip(parts, totals, us):
                piece[k, :, a:b] = (cot[own_rows, a:b].astype(f32) + rstd * (t - mean_w - u * mean_wu)).astype(bf16)
        else:
            for (a, b), t in zip(parts, totals):
                piece[k, :, a:b] = (xrow[:, a:b].astype(f32) + t + vec[5:6, a:b]).astype(bf16)
        result = results[k]
        state["pieces", k] = [
            load(piece.at[k], result.at[own_rows, :]),
            send_copy(piece.at[k], result.at[own_rows, :], t_partner(1)),
            send_copy(piece.at[k], result.at[own_rows, :], t_partner(0)),
        ]

    def sum_gather(k):
        result = results[k]
        state["pieces", k][1].wait_recv()
        at = rows_of(t_flip(1))
        state["pieces", k].append(send_copy(result.at[at, :], result.at[at, :], t_partner(0)))

    def small_round(n):
        if n > 0:
            copy = state["small"]
            copy.wait()
            if n <= 2:
                small[0:4, :] += small_in[n - 1, 0:4, :]
            else:
                small[...] += small_in[n - 1]
        if n < 5:
            partner = t_partner(n) if n < 2 else dp_partner(n - 2)
            state["small"] = send_copy(small, small_in.at[n], partner)
        else:
            state["small"] = load(small, small_out)

    actions = dict(
        m=mlp, h=attention, a=w1, b=w2, c=a3, i=lambda k: sum_start(k), j=sum_middle, k=sum_late, l=sum_gather, s=small_round
    )
    for kind, n in jobs:
        actions[kind](n)

    for c in range(len(orders)):
        state[c].wait_recv()
    for k in range(2):
        local, first, second, third = state["pieces", k]
        local.wait()
        first.wait_send()
        second.wait()
        third.wait()
        state["sum", k]
    for slots in (s1_slots, s2_slots, s3_slots, k2_slots):
        slots.drain()
    state["small"].wait()


ORDER = " ".join(
    [
        "m0 a0 a4 m1",
        "m2 a6 a5 m3",
        "b0 b4 h0 h1",
        "a3 a9 b6 c0",
        "c4 b5 i0 a2",
        "b3 j0 c6 b9",
        "s0 i1 a8 c5",
        "k0 j1 c3 c9",
        "b2 s1 s2 a11",
        "s3 s4 s5 l0",
        "b8 a1 c2 k1",
        "b11 c8 a7 b1",
        "l1 c11 a10 c1",
        "b7 b10 c7 c10",
    ]
).split()
Z_FIRST = (0, 6, 9)


def layer_call(x, c, ln_vectors, biases, fc1, fc2, qkv_weight, dense):
    rows, width = x.shape
    hidden, qkv_columns, context_columns = fc1.shape[1], qkv_weight.shape[1], dense.shape[1]
    heads = qkv_columns // (3 * HEAD_DIM)
    total = 2 * hidden + qkv_columns + context_columns
    chunks = total // CHUNK
    fc1_bias, qkv_bias, dense_bias, fc2_bias = (b.astype(f32) for b in biases)
    pad = jnp.zeros((width - qkv_columns,), f32)
    vectors = jnp.concatenate(
        [*(v.astype(f32) for v in ln_vectors), fc1_bias, dense_bias + fc2_bias, fc1_bias, qkv_bias, pad]
    ).reshape(-1, 128)
    jobs = [(word[0], int(word[1:])) for word in ORDER]
    orders = [(1, 0, 2) if n in Z_FIRST else (0, 1, 2) for n in range(chunks)]
    quarter, nb = rows // 4, width // 8
    anywhere = pl.BlockSpec(memory_space=pl.ANY)
    local = pl.BlockSpec(memory_space=pltpu.VMEM)
    shape = jax.ShapeDtypeStruct
    outs = [
        shape((rows, width), bf16),
        shape((rows, width), bf16),
        shape((nb, total), bf16),
        shape((nb, total), bf16),
        shape((8, width), f32),
        shape((chunks, 4, nb, CHUNK), bf16),
        shape((chunks, 2, nb, CHUNK), bf16),
        shape((2, width // CHUNK * 2 * quarter, CHUNK), bf16),
        shape((2, width // CHUNK, quarter, CHUNK), bf16),
    ]
    vmem = pltpu.VMEM
    scratch = [
        vmem((rows, width), bf16),
        vmem((rows, width), bf16),
        vmem((rows, width), bf16),
        vmem((rows, hidden), bf16),
        vmem((rows, hidden), bf16),
        vmem((rows, qkv_columns), bf16),
        vmem((rows, context_columns), bf16),
        vmem((rows, 1), f32),
        vmem((rows, 1), f32),
        vmem((SEQ, 128), f32),
        vmem((SEQ, 128), f32),
        vmem((VEC_ROWS, width), f32),
        vmem((2, width, CHUNK), bf16),
        vmem((2, width, CHUNK), bf16),
        vmem((4, 4, nb, CHUNK), bf16),
        vmem((3, 2, nb, CHUNK), bf16),
        vmem((3, nb, CHUNK), bf16),
        vmem((6, 2, nb, CHUNK), bf16),
        vmem((4, nb, CHUNK), bf16),
        vmem((4, nb, CHUNK), bf16),
        vmem((2, nb, CHUNK), bf16),
        vmem((2, quarter, width), bf16),
        vmem((quarter, width), bf16),
        vmem((8, width), f32),
        vmem((5, 8, width), f32),
        pltpu.SemaphoreType.DMA((80,)),
        pltpu.SemaphoreType.DMA((1,)),
        pltpu.SemaphoreType.DMA((56,)),
        pltpu.SemaphoreType.DMA((56,)),
        pltpu.SemaphoreType.DMA((chunks,)),
    ]
    flops = 6 * rows * width * (2 * hidden + qkv_columns + context_columns)
    return pl.pallas_call(
        partial(layer_kernel, jobs=jobs, orders=orders, heads=heads),
        in_specs=[anywhere, anywhere, local, local] + [anywhere] * 4,
        out_specs=[anywhere] * len(outs),
        out_shape=outs,
        scratch_shapes=scratch,
        compiler_params=pltpu.CompilerParams(vmem_limit_bytes=VMEM_LIMIT, collective_id=0, has_side_effects=True),
        cost_estimate=pl.CostEstimate(flops=flops, bytes_accessed=1 << 27, transcendentals=2 * rows * hidden),
        name="layer",
    )(x, c, vectors, angle_tables(), fc1, fc2, qkv_weight, dense)


def fused(
    layer_input,
    ln1_gain,
    ln1_bias,
    ln2_gain,
    ln2_bias,
    qkv_weight,
    qkv_bias,
    dense_weight,
    dense_bias,
    fc1_weight,
    fc1_bias,
    fc2_weight,
    fc2_bias,
    cotangent,
):
    output, input_grad, kept, last, small, *_ = layer_call(
        layer_input,
        cotangent,
        (ln1_gain, ln1_bias, ln2_gain, ln2_bias),
        (fc1_bias, qkv_bias, dense_bias, fc2_bias),
        fc1_weight,
        fc2_weight,
        qkv_weight,
        dense_weight,
    )
    hidden, qkv_columns = fc1_weight.shape[1], qkv_weight.shape[1]
    ends = (0, hidden, 2 * hidden, 2 * hidden + qkv_columns, kept.shape[1])
    grad_fc2, grad_fc1, grad_qkv, grad_dense = (
        kept[:, a:b].astype(f32) + last[:, a:b].astype(f32) for a, b in zip(ends[:-1], ends[1:])
    )
    return (
        output,
        input_grad,
        small[0],
        small[1],
        small[2],
        small[3],
        grad_qkv,
        small[5, :qkv_columns],
        grad_dense,
        small[6],
        grad_fc1,
        small[4, :hidden],
        grad_fc2,
        small[6],
    )


def fits(mesh):
    return mesh.shape["dp"] == 8 and mesh.shape["tensor"] == 4


def normalize(x_float, gain_row, shift_row):
    row_mean = jnp.mean(x_float, -1, keepdims=True)
    centred = x_float - row_mean
    spread = jnp.mean(centred * centred, -1, keepdims=True)
    return centred * lax.rsqrt(spread + EPSILON) * gain_row + shift_row


def rotary_tables():
    half_rot = ROT // 2
    freq_index = jnp.arange(half_rot, dtype=jnp.float32)
    frequency = jnp.exp(freq_index * (-2.0 * math.log(10000.0) / ROT))
    angles = jnp.arange(SEQ, dtype=jnp.float32)[:, None] * frequency[None, :]
    return (jnp.cos(angles), jnp.sin(angles))


def rotate(operand, cos_table, sine_table):
    half_rot = ROT // 2
    first_half = operand[..., :half_rot]
    second_half = operand[..., half_rot:ROT]
    cos_part = cos_table[None, :, None, :]
    sine_part = sine_table[None, :, None, :]
    return jnp.concatenate(
        [
            first_half * cos_part - second_half * sine_part,
            second_half * cos_part + first_half * sine_part,
            operand[..., ROT:],
        ],
        -1,
    )


def unrotate(operand, cos_table, sine_table):
    half_rot = ROT // 2
    first_half = operand[..., :half_rot]
    second_half = operand[..., half_rot:ROT]
    cos_part = cos_table[None, :, None, :]
    sine_part = sine_table[None, :, None, :]
    return jnp.concatenate(
        [
            first_half * cos_part + second_half * sine_part,
            second_half * cos_part - first_half * sine_part,
            operand[..., ROT:],
        ],
        -1,
    )


def block_scores(query_block, key_block, start_row, score_scale):
    scores = (
        jnp.einsum("sqhd,skhd->shqk", query_block, key_block, preferred_element_type=jnp.float32)
        * score_scale
    )
    row_ids = start_row + jnp.arange(query_block.shape[1])[:, None]
    col_ids = jnp.arange(key_block.shape[1])[None, :]
    return jnp.where(col_ids <= row_ids, scores, -1e30)


def rounded(values_in):
    return lax.optimization_barrier(values_in.astype(jnp.bfloat16)).astype(jnp.float32)


def on_device(
    layer_input,
    ln1_gain,
    ln1_bias,
    ln2_gain,
    ln2_bias,
    qkv_weight,
    qkv_bias,
    dense_weight,
    dense_bias,
    fc1_weight,
    fc1_bias,
    fc2_weight,
    fc2_bias,
    cotangent,
):
    tok_rows, model_width = layer_input.shape
    local_heads = HEADS // lax.axis_size("tensor")
    seq_count = tok_rows // SEQ
    block_rows = 512
    score_scale = HEAD_DIM ** (-0.5)
    x_float = layer_input.astype(jnp.float32)
    gain_one = ln1_gain.astype(jnp.float32)
    shift_one = ln1_bias.astype(jnp.float32)
    gain_two = ln2_gain.astype(jnp.float32)
    shift_two = ln2_bias.astype(jnp.float32)
    attn_in = normalize(x_float, gain_one, shift_one).astype(jnp.bfloat16)
    mlp_in = normalize(x_float, gain_two, shift_two).astype(jnp.bfloat16)
    qkv_all = jnp.dot(attn_in, qkv_weight, preferred_element_type=jnp.float32) + qkv_bias.astype(
        jnp.float32
    )
    qkv_all = qkv_all.reshape(seq_count, SEQ, local_heads, 3, HEAD_DIM)
    cos_table, sine_table = rotary_tables()
    queries = rotate(qkv_all[..., 0, :], cos_table, sine_table).astype(jnp.bfloat16)
    keys_rot = rotate(qkv_all[..., 1, :], cos_table, sine_table).astype(jnp.bfloat16)
    values = qkv_all[..., 2, :].astype(jnp.bfloat16)
    context_blocks = []
    log_sums = []
    for start_row in range(0, SEQ, block_rows):
        key_end = start_row + block_rows
        masked = block_scores(
            queries[:, start_row:key_end], keys_rot[:, :key_end], start_row, score_scale
        )
        row_peak = jnp.max(masked, -1, keepdims=True)
        weights = jnp.exp(masked - row_peak)
        row_total = jnp.sum(weights, -1, keepdims=True)
        probabilities = (weights / row_total).astype(jnp.bfloat16)
        log_sums.append(row_peak + jnp.log(row_total))
        context_blocks.append(
            jnp.einsum(
                "shqk,skhd->sqhd",
                probabilities,
                values[:, :key_end],
                preferred_element_type=jnp.float32,
            )
        )
    context = jnp.concatenate(context_blocks, 1).astype(jnp.bfloat16)
    context_flat = context.reshape(tok_rows, local_heads * HEAD_DIM)
    attn_part = jnp.einsum(
        "td,ed->te", context_flat, dense_weight, preferred_element_type=jnp.float32
    )
    hidden = jnp.dot(mlp_in, fc1_weight, preferred_element_type=jnp.float32) + fc1_bias.astype(
        jnp.float32
    )
    exact_gelu = partial(jax.nn.gelu, approximate=False)
    activated = exact_gelu(hidden).astype(jnp.bfloat16)
    mlp_part = jnp.einsum("tf,ef->te", activated, fc2_weight, preferred_element_type=jnp.float32)
    partial_out = attn_part + mlp_part
    bias_total = dense_bias.astype(jnp.float32) + fc2_bias.astype(jnp.float32)
    full_sum = lax.psum(partial_out, "tensor")
    output = (x_float + full_sum + bias_total).astype(jnp.bfloat16)
    out_grad = cotangent.astype(jnp.float32)
    grad_fc2 = jnp.einsum("te,tf->ef", cotangent, activated, preferred_element_type=jnp.float32)
    grad_dense = jnp.einsum(
        "te,td->ed", cotangent, context_flat, preferred_element_type=jnp.float32
    )
    out_bias_grad = jnp.sum(out_grad, 0)
    activated_grad = jnp.einsum(
        "te,ef->tf", cotangent, fc2_weight, preferred_element_type=jnp.float32
    )
    gelu_pull = jax.vjp(exact_gelu, hidden)[1]
    hidden_grad = gelu_pull(activated_grad)[0].astype(jnp.bfloat16)
    grad_fc1 = jnp.einsum("td,tf->df", mlp_in, hidden_grad, preferred_element_type=jnp.float32)
    fc1_bias_grad = jnp.sum(hidden_grad.astype(jnp.float32), 0)
    mlp_in_grad = jnp.einsum(
        "tf,df->td", hidden_grad, fc1_weight, preferred_element_type=jnp.float32
    )
    context_grad = jnp.einsum(
        "te,ed->td", cotangent, dense_weight, preferred_element_type=jnp.float32
    ).astype(jnp.bfloat16)
    context_grad = context_grad.reshape(seq_count, SEQ, local_heads, HEAD_DIM)
    key_grad = jnp.zeros((seq_count, SEQ, local_heads, HEAD_DIM), jnp.float32)
    value_grad = jnp.zeros((seq_count, SEQ, local_heads, HEAD_DIM), jnp.float32)
    query_grads = []
    for block_number, start_row in enumerate(range(0, SEQ, block_rows)):
        key_end = start_row + block_rows
        query_block = queries[:, start_row:key_end]
        masked = block_scores(query_block, keys_rot[:, :key_end], start_row, score_scale)
        probabilities = jnp.exp(masked - log_sums[block_number])
        grad_block = context_grad[:, start_row:key_end]
        value_grad = value_grad.at[:, :key_end].add(
            jnp.einsum(
                "shqk,sqhd->skhd",
                probabilities.astype(jnp.bfloat16),
                grad_block,
                preferred_element_type=jnp.float32,
            )
        )
        prob_grad = jnp.einsum(
            "sqhd,skhd->shqk", grad_block, values[:, :key_end], preferred_element_type=jnp.float32
        )
        row_delta = jnp.sum(probabilities * prob_grad, -1, keepdims=True)
        score_grad = (probabilities * (prob_grad - row_delta)).astype(jnp.bfloat16)
        query_grads.append(
            jnp.einsum(
                "shqk,skhd->sqhd",
                score_grad,
                keys_rot[:, :key_end],
                preferred_element_type=jnp.float32,
            )
            * score_scale
        )
        key_grad = key_grad.at[:, :key_end].add(
            jnp.einsum(
                "shqk,sqhd->skhd", score_grad, query_block, preferred_element_type=jnp.float32
            )
            * score_scale
        )
    query_grad = jnp.concatenate(query_grads, 1)
    query_pre = unrotate(rounded(query_grad), cos_table, sine_table).astype(jnp.bfloat16)
    key_pre = unrotate(rounded(key_grad), cos_table, sine_table).astype(jnp.bfloat16)
    value_pre = value_grad.astype(jnp.bfloat16)
    qkv_grad = jnp.stack([query_pre, key_pre, value_pre], 3).reshape(
        tok_rows, local_heads * 3 * HEAD_DIM
    )
    grad_qkv = jnp.einsum("td,tc->dc", attn_in, qkv_grad, preferred_element_type=jnp.float32)
    qkv_bias_grad = jnp.sum(qkv_grad.astype(jnp.float32), 0)
    attn_in_grad = jnp.einsum("tc,dc->td", qkv_grad, qkv_weight, preferred_element_type=jnp.float32)
    norm_one_pull = jax.vjp(normalize, x_float, gain_one, shift_one)[1]
    input_one, gain_grad_one, shift_grad_one = norm_one_pull(attn_in_grad)
    norm_two_pull = jax.vjp(normalize, x_float, gain_two, shift_two)[1]
    input_two, gain_grad_two, shift_grad_two = norm_two_pull(mlp_in_grad)
    input_part = input_one + input_two
    input_total = lax.psum(input_part, "tensor")
    input_grad = (out_grad + input_total).astype(jnp.bfloat16)
    qkv_bias_grad, fc1_bias_grad, out_bias_grad = lax.psum(
        (qkv_bias_grad, fc1_bias_grad, out_bias_grad), "dp"
    )
    gain_grad_one, shift_grad_one, gain_grad_two, shift_grad_two = lax.psum(
        (gain_grad_one, shift_grad_one, gain_grad_two, shift_grad_two), ("dp", "tensor")
    )
    grad_qkv, grad_dense, grad_fc1, grad_fc2 = (
        lax.psum_scatter(
            grad_qkv.astype(jnp.bfloat16), "dp", scatter_dimension=0, tiled=True
        ).astype(jnp.float32),
        lax.psum_scatter(
            grad_dense.astype(jnp.bfloat16), "dp", scatter_dimension=0, tiled=True
        ).astype(jnp.float32),
        lax.psum_scatter(
            grad_fc1.astype(jnp.bfloat16), "dp", scatter_dimension=0, tiled=True
        ).astype(jnp.float32),
        lax.psum_scatter(
            grad_fc2.astype(jnp.bfloat16), "dp", scatter_dimension=0, tiled=True
        ).astype(jnp.float32),
    )
    return (
        output,
        input_grad,
        gain_grad_one,
        shift_grad_one,
        gain_grad_two,
        shift_grad_two,
        grad_qkv,
        qkv_bias_grad,
        grad_dense,
        out_bias_grad,
        grad_fc1,
        fc1_bias_grad,
        grad_fc2,
        out_bias_grad,
    )


def solution(mesh):
    in_specs = (
        P("dp", None),
        P(),
        P(),
        P(),
        P(),
        P(None, "tensor"),
        P("tensor"),
        P(None, "tensor"),
        P(),
        P(None, "tensor"),
        P("tensor"),
        P(None, "tensor"),
        P(),
        P("dp", None),
    )
    out_specs = (
        P("dp", None),
        P("dp", None),
        P(),
        P(),
        P(),
        P(),
        P("dp", "tensor"),
        P("tensor"),
        P("dp", "tensor"),
        P(),
        P("dp", "tensor"),
        P("tensor"),
        P("dp", "tensor"),
        P(),
    )
    return jax.shard_map(
        fused if fits(mesh) else on_device, mesh=mesh, in_specs=in_specs, out_specs=out_specs, check_vma=False
    )
```

```python
import itertools
import math
from functools import partial

import jax
import jax.numpy as jnp
from jax import lax
from jax.experimental import pallas as pl
from jax.experimental.pallas import tpu as pltpu
from jax.sharding import PartitionSpec as P

HEADS = 8
SEQ = 1024
HEAD_DIM = 256
ROT = 64
EPSILON = 1e-05
VMEM_LIMIT = 63 * 1024 * 1024

f32 = jnp.float32
bf16 = jnp.bfloat16
NN = (((1,), (0,)), ((), ()))
NT = (((1,), (1,)), ((), ()))
TN = (((0,), (0,)), ((), ()))


def dot(a, b, dims=NN):
    return lax.dot_general(a, b, dims, preferred_element_type=f32)


def turn(block, cos_table, sine_table):
    half_rot = ROT // 2
    head = block[:, :128]
    lane = lax.broadcasted_iota(jnp.int32, head.shape, 1)
    other = jnp.where(lane < half_rot, pltpu.roll(head, 128 - half_rot, 1), pltpu.roll(head, half_rot, 1))
    return jnp.concatenate([head * cos_table + other * sine_table, block[:, 128:]], 1)


def angle_tables():
    half_rot = ROT // 2
    lane = jnp.arange(128)
    frequency = jnp.exp((lane % half_rot).astype(f32) * (-2.0 * math.log(10000.0) / ROT))
    frequency = jnp.where(lane < ROT, frequency, 0.0)
    step = jnp.arange(32, dtype=f32)
    angles = jnp.concatenate([step, 32.0 * step])[:, None] * frequency[None, :]
    cos, sin = jnp.cos(angles), jnp.sin(angles)
    sign = jnp.where(lane < half_rot, -1.0, 1.0)[None, :]
    return jnp.concatenate([cos[:32], sin[:32], cos[32:], sin[32:], jnp.broadcast_to(sign, (8, 128))], 0)


CHUNK = 512
MESH = pl.DeviceIdType.MESH
VEC_ROWS = 8
VECTORS = 8


class Slots:
    def __init__(self, count):
        self.free = [(n, []) for n in range(count)]

    def take(self):
        slot, waits = self.free.pop(0)
        for wait in waits:
            wait()
        return slot

    def give(self, slot, *waits):
        self.free.append((slot, list(waits)))

    def drain(self):
        for _, waits in self.free:
            for wait in waits:
                wait()


def layer_kernel(
    x_hbm, c_hbm, table_in, fc1_hbm, fc2_hbm, wqkv_hbm, dense_hbm, *refs,
    jobs, orders, heads, block=256,
):
    vec_hbm, refs = refs[:VECTORS], refs[VECTORS:]
    (
        out_hbm, grad_hbm, keep_hbm, last_hbm, small_out, r1_hbm, r2_hbm, core_hbm, y_hbm,
        attn_in, mlp_in, cot, act, hg, qg, ctx, mean_ref, rstd_ref, cos_ref, sin_ref, vec, raw, w1buf, w2buf,
        s1, s2, s3, k2, ld1, ldm, ld2, piece, xrow, small, small_in,
        load_sem, send_sem, recv_sem, keep_sem,
    ) = refs
    rows, width = cot.shape
    hidden = act.shape[1]
    nb = width // 8
    quarter = rows // 4
    me, own = lax.axis_index("dp"), lax.axis_index("tensor")
    dp_bits = [lax.rem(lax.div(me, 1 << k), 2) for k in range(3)]
    t_bits = [lax.rem(lax.div(own, 1 << k), 2) for k in range(2)]

    def dp_flip(*bits):
        return me + sum((1 - 2 * dp_bits[k]) * (1 << k) for k in bits)

    def t_flip(*bits):
        return own + sum((1 - 2 * t_bits[k]) * (1 << k) for k in bits)

    def dp_partner(bit):
        return (dp_flip(bit), own)

    def t_partner(bit):
        return (me, t_flip(bit))

    partners = [dp_partner(k) for k in range(3)] + [t_partner(k) for k in range(2)]
    barrier = pltpu.get_barrier_semaphore()
    for partner in partners:
        pl.semaphore_signal(barrier, inc=1, device_id=partner, device_id_type=MESH)

    copies = itertools.count()

    def send_copy(src, dst, partner):
        n = next(copies)
        copy = pltpu.make_async_remote_copy(
            src_ref=src, dst_ref=dst, send_sem=send_sem.at[n], recv_sem=recv_sem.at[n], device_id=partner, device_id_type=MESH
        )
        copy.start()
        return copy

    loads = itertools.count()

    def load(src, dst):
        copy = pltpu.make_async_copy(src, dst, load_sem.at[next(loads)])
        copy.start()
        return copy

    load_x = load(x_hbm, act)
    load_v = [load(v, raw.at[n, pl.ds(0, v.shape[0])]) for n, v in enumerate(vec_hbm)]

    def mlp_weights(j):
        slot = j % 2
        at = pl.ds(j * CHUNK, CHUNK)
        return [load(fc1_hbm.at[:, at], w1buf.at[slot]), load(fc2_hbm.at[:, at], w2buf.at[slot])]

    def head_weights(h):
        slot = h % 2
        base = 3 * h * HEAD_DIM
        return [
            load(wqkv_hbm.at[:, pl.ds(base, 2 * HEAD_DIM)], w1buf.at[slot]),
            load(wqkv_hbm.at[:, pl.ds(base + 2 * HEAD_DIM, HEAD_DIM)], w2buf.at[slot, :, pl.ds(0, HEAD_DIM)]),
            load(dense_hbm.at[:, pl.ds(h * HEAD_DIM, HEAD_DIM)], w2buf.at[slot, :, pl.ds(HEAD_DIM, HEAD_DIM)]),
        ]

    weights = {("mlp", 0): mlp_weights(0)}
    load_c = load(c_hbm, cot)
    weights["mlp", 1] = mlp_weights(1)
    tiles = hidden // CHUNK

    small[...] = jnp.zeros_like(small)
    for copy in load_v:
        copy.wait()
    for n in range(VECTORS):
        packed = raw[n].astype(f32)
        if n == 6:
            packed = packed + raw[5].astype(f32)
        for i in range(vec_hbm[n].shape[0]):
            vec[n : n + 1, i * 128 : (i + 1) * 128] = packed[i : i + 1, :]
    low_cos, low_sin = table_in[0:32, :], table_in[32:64, :]
    sign = table_in[128:129, :]
    for n in range(SEQ // 32):
        high_cos, high_sin = table_in[64 + n : 65 + n, :], table_in[96 + n : 97 + n, :]
        cos_ref[n * 32 : (n + 1) * 32, :] = high_cos * low_cos - high_sin * low_sin
        sin_ref[n * 32 : (n + 1) * 32, :] = sign * (high_sin * low_cos + high_cos * low_sin)

    load_x.wait()

    def norm_rows(i, _):
        part = pl.ds(pl.multiple_of(i * 128, 128), 128)
        x = act[part, :].astype(f32)
        mean = jnp.mean(x, -1, keepdims=True)
        centred = x - mean
        rstd = lax.rsqrt(jnp.mean(centred * centred, -1, keepdims=True) + EPSILON)
        u = centred * rstd
        attn_in[part, :] = (u * vec[0:1, :] + vec[1:2, :]).astype(bf16)
        mlp_in[part, :] = (u * vec[2:3, :] + vec[3:4, :]).astype(bf16)
        mean_ref[part, :] = mean
        rstd_ref[part, :] = rstd
        return 0

    lax.fori_loop(0, rows // 128, norm_rows, 0)
    load_c.wait()
    pl.semaphore_wait(barrier, len(partners))

    s1_slots, s2_slots, s3_slots, k2_slots = Slots(s1.shape[0]), Slots(s2.shape[0]), Slots(s3.shape[0]), Slots(k2.shape[0])
    state = {}

    def operands(c):
        n_fc = hidden // CHUNK
        n_qkv = qg.shape[1] // CHUNK
        if c < n_fc:
            return cot, act, c
        if c < 2 * n_fc:
            return mlp_in, hg, c - n_fc
        if c < 2 * n_fc + n_qkv:
            return attn_in, qg, c - 2 * n_fc
        return cot, ctx, c - 2 * n_fc - n_qkv

    def block_of(lhs, index):
        return lhs[:, pl.ds(pl.multiple_of(index * nb, nb), nb)]

    def w1(c):
        lhs, rhs, j = operands(c)
        one, two, three = orders[c]
        slot = s1_slots.take()
        base = dp_flip(one, two, three)

        def body(n, _):
            second, third = n // 2, lax.rem(n, 2)
            index = base - second * (1 - 2 * dp_bits[two]) * (1 << two) - third * (1 - 2 * dp_bits[three]) * (1 << three)
            s1[slot, n] = dot(block_of(lhs, index), rhs[:, j * CHUNK : (j + 1) * CHUNK], TN).astype(bf16)
            return 0

        lax.fori_loop(0, 4, body, 0)
        copy = send_copy(s1.at[slot], r1_hbm.at[c], dp_partner(one))
        s1_slots.give(slot, copy.wait_send)
        state[c] = copy

    def w2(c):
        lhs, rhs, j = operands(c)
        one, two, three = orders[c]
        state[c].wait_recv()
        loaded = load(r1_hbm.at[c], ld1)
        slot, kept = s2_slots.take(), k2_slots.take()
        loaded.wait()

        def part(base, n, out):
            def body(i, _):
                index = base - i * (1 - 2 * dp_bits[three]) * (1 << three)
                out[i] = (dot(block_of(lhs, index), rhs[:, j * CHUNK : (j + 1) * CHUNK], TN) + ld1[n + i].astype(f32)).astype(bf16)
                return 0

            lax.fori_loop(0, 2, body, 0)

        part(dp_flip(two, three), 0, s2.at[slot])
        copy = send_copy(s2.at[slot], r2_hbm.at[c], dp_partner(two))
        s2_slots.give(slot, copy.wait_send)
        part(dp_flip(three), 2, k2.at[kept])
        state[c] = (copy, kept)

    def a3(c):
        copy, kept = state[c]
        three = orders[c][2]
        copy.wait_recv()
        loaded = load(r2_hbm.at[c], ld2)
        slot = s3_slots.take()
        loaded.wait()
        s3[slot] = (k2[kept, 0].astype(f32) + ld2[0].astype(f32)).astype(bf16)
        columns = pl.ds(c * CHUNK, CHUNK)
        copy = send_copy(s3.at[slot], last_hbm.at[:, columns], dp_partner(three))
        s3_slots.give(slot, copy.wait_send)
        k2[kept, 1] = (k2[kept, 1].astype(f32) + ld2[1].astype(f32)).astype(bf16)
        keep = pltpu.make_async_copy(k2.at[kept, 1], keep_hbm.at[:, columns], keep_sem.at[c])
        keep.start()
        k2_slots.give(kept, keep.wait)
        state[c] = copy

    def mlp(j):
        slot = j % 2
        for copy in weights.pop(("mlp", j)):
            copy.wait()
        at = j * CHUNK
        bias = vec[4:5, at : at + CHUNK]

        def body(i, sums):
            part = pl.ds(pl.multiple_of(i * block, block), block)
            h = dot(mlp_in[part, :], w1buf[slot]) + bias
            above = dot(cot[part, :], w2buf[slot])
            cdf = 0.5 + 0.5 * lax.erf(h * (2.0**-0.5))
            density = jnp.exp(h * h * -0.5) * ((2.0 * math.pi) ** -0.5)
            act[part, at : at + CHUNK] = (h * cdf).astype(bf16)
            low = (above * (cdf + h * density)).astype(bf16)
            hg[part, at : at + CHUNK] = low
            above_sum = jnp.sum(cot[part, at : at + CHUNK].astype(f32), 0, keepdims=True)
            return sums[0] + jnp.sum(low.astype(f32), 0, keepdims=True), sums[1] + above_sum

        zero = jnp.zeros((1, CHUNK), f32)
        bias_sum, above_sum = lax.fori_loop(0, rows // block, body, (zero, zero))
        small[4:5, at : at + CHUNK] = bias_sum
        small[6:7, at : at + CHUNK] = above_sum
        if j + 2 < tiles:
            weights["mlp", j + 2] = mlp_weights(j + 2)
        else:
            h = j + 2 - tiles
            weights["head", h] = head_weights(h)

    def attention(h):
        slot = h % 2
        for copy in weights.pop(("head", h)):
            copy.wait()
        base = 3 * h * HEAD_DIM
        scale = HEAD_DIM ** (-0.5)

        def scoped(qkv_ref, g_ref, dk_ref, dv_ref):
            def project(i, _):
                part = pl.ds(pl.multiple_of(i * block, block), block)
                acc = dot(attn_in[part, :], w1buf[slot]) + vec[7:8, base : base + 2 * HEAD_DIM]
                cos, sin = cos_ref[part, :], sin_ref[part, :]
                for n in range(2):
                    at = n * HEAD_DIM
                    qkv_ref[part, at : at + HEAD_DIM] = turn(acc[:, at : at + HEAD_DIM], cos, sin).astype(bf16)
                acc = dot(attn_in[part, :], w2buf[slot, :, 0:HEAD_DIM]) + vec[7:8, base + 2 * HEAD_DIM : base + 3 * HEAD_DIM]
                qkv_ref[part, 2 * HEAD_DIM :] = acc.astype(bf16)
                g_ref[part, :] = dot(cot[part, :], w2buf[slot, :, HEAD_DIM : 2 * HEAD_DIM]).astype(bf16)
                return 0

            lax.fori_loop(0, rows // block, project, 0)
            for i in reversed(range(SEQ // block)):
                part = pl.ds(i * block, block)
                key_end = (i + 1) * block
                keys = pl.ds(0, key_end)
                q, g = qkv_ref[part, 0:HEAD_DIM], g_ref[part, :]
                k, v = qkv_ref[keys, HEAD_DIM : 2 * HEAD_DIM], qkv_ref[keys, 2 * HEAD_DIM :]
                scores = dot(q, k, NT) * scale
                row_id = i * block + lax.broadcasted_iota(jnp.int32, scores.shape, 0)
                col_id = lax.broadcasted_iota(jnp.int32, scores.shape, 1)
                scores = jnp.where(col_id <= row_id, scores, -1e30)
                e = jnp.exp(scores - jnp.max(scores, -1, keepdims=True))
                probs = e / jnp.sum(e, -1, keepdims=True)
                low = probs.astype(bf16)
                ctx[part, h * HEAD_DIM : (h + 1) * HEAD_DIM] = dot(low, v).astype(bf16)
                prob_grad = dot(g, v, NT)
                delta = jnp.sum(probs * prob_grad, -1, keepdims=True)
                score_grad = (probs * (prob_grad - delta)).astype(bf16)
                dv = dot(low, g, TN)
                dk = dot(score_grad, q, TN)
                if i == SEQ // block - 1:
                    dv_ref[...] = dv
                    dk_ref[...] = dk
                else:
                    dv_ref[keys, :] += dv
                    dk_ref[keys, :] += dk
                dq = (dot(score_grad, k) * scale).astype(bf16).astype(f32)
                qg[part, base : base + HEAD_DIM] = turn(dq, cos_ref[part, :], -sin_ref[part, :]).astype(bf16)
            dk = (dk_ref[...] * scale).astype(bf16).astype(f32)
            qg[:, base + HEAD_DIM : base + 2 * HEAD_DIM] = turn(dk, cos_ref[...], -sin_ref[...]).astype(bf16)
            qg[:, base + 2 * HEAD_DIM : base + 3 * HEAD_DIM] = dv_ref[...].astype(bf16)
            head = qg[:, base : base + 3 * HEAD_DIM]
            small[5:6, base : base + 3 * HEAD_DIM] = jnp.sum(head.astype(f32), 0, keepdims=True)

        pl.run_scoped(
            scoped,
            pltpu.VMEM((SEQ, 3 * HEAD_DIM), bf16),
            pltpu.VMEM((SEQ, HEAD_DIM), bf16),
            pltpu.VMEM((SEQ, HEAD_DIM), f32),
            pltpu.VMEM((SEQ, HEAD_DIM), f32),
        )
        if h + 2 < heads:
            weights["head", h + 2] = head_weights(h + 2)

    quarters = [t_flip(0, 1), t_flip(0), t_flip(1), own]

    def quarter_of(n):
        return pl.ds(pl.multiple_of(quarters[n] * quarter, quarter), quarter)

    def back_tiles(buf, first_hbm, first, second_hbm, second, x_tiles, store):
        step = CHUNK // 2

        def scoped(first_w, second_w, x_w, sems):
            def copies_of(d, slot):
                at = pl.ds(pl.multiple_of(d * step, step), step)
                made = [
                    pltpu.make_async_copy(first_hbm.at[at, :], first_w.at[slot], sems.at[slot, 0]),
                    pltpu.make_async_copy(second_hbm.at[at, :], second_w.at[slot], sems.at[slot, 1]),
                ]
                if x_tiles:
                    made.append(pltpu.make_async_copy(x_hbm.at[:, at], x_w.at[slot], sems.at[slot, 2]))
                return made

            n_steps = width // step
            for copy in copies_of(0, 0):
                copy.start()

            def body(e, _):
                for half in range(2):
                    d = 2 * e + half
                    for copy in copies_of(d, half):
                        copy.wait()

                    @pl.when(d + 1 < n_steps)
                    def _():
                        for copy in copies_of(d + 1, 1 - half):
                            copy.start()

                    columns = pl.ds(half * step, step)
                    sums = [jnp.zeros((1, step), f32) for _ in range(4)]
                    for n in range(4):
                        part = quarter_of(n)
                        a = dot(first[part, :], first_w[half], NT)
                        b = dot(second[part, :], second_w[half], NT)
                        at = pl.ds(pl.multiple_of(e * 2 * quarter + (n % 2) * quarter, quarter), quarter)
                        buf[n // 2, at, columns], terms = store(d, part, a, b, x_w.at[half])
                        sums = [s + t for s, t in zip(sums, terms)]
                    if x_tiles:
                        at = pl.ds(pl.multiple_of(d * step, step), step)
                        small[0:4, at] = jnp.concatenate(sums, 0)
                return 0

            lax.fori_loop(0, n_steps // 2, body, 0)

        pl.run_scoped(
            scoped,
            pltpu.VMEM((2, step, first.shape[1]), bf16),
            pltpu.VMEM((2, step, second.shape[1]), bf16),
            pltpu.VMEM((2, rows if x_tiles else 16, step), bf16),
            pltpu.SemaphoreType.DMA((2, 3)),
        )

    def input_tiles():
        step = CHUNK // 2

        def store(d, part, a, b, x_tile):
            at = pl.ds(pl.multiple_of(d * step, step), step)
            u = (x_tile[part, :].astype(f32) - mean_ref[part, :]) * rstd_ref[part, :]
            terms = [jnp.sum(t, 0, keepdims=True) for t in (a * u, a, b * u, b)]
            return (a * vec[0:1, at] + b * vec[2:3, at]).astype(bf16), terms

        back_tiles(w1buf, wqkv_hbm, qg, fc1_hbm, hg, True, store)

    def output_tiles():
        back_tiles(w2buf, dense_hbm, ctx, fc2_hbm, act, False, lambda d, part, a, b, x_tile: ((a + b).astype(bf16), []))

    e_tiles = width // CHUNK
    buffers = (w1buf, w2buf)
    results = (grad_hbm, out_hbm)

    def sum_start(k):
        (input_tiles, output_tiles)[k]()
        state["sum", k] = send_copy(buffers[k].at[0], core_hbm.at[k], t_partner(0))

    def half_of(k, half, dst):
        return [
            load(core_hbm.at[k, pl.ds(e * 2 * quarter + half * quarter, quarter), :], dst.at[e]) for e in range(e_tiles)
        ]

    def sum_middle(k):
        first = state["sum", k]
        first.wait_recv()
        loaded = half_of(k, 0, ld1)
        slot = s1_slots.take()
        for copy in loaded:
            copy.wait()
        for e in range(e_tiles):
            s1[slot, e] = (buffers[k][1, pl.ds(e * 2 * quarter, quarter), :].astype(f32) + ld1[e].astype(f32)).astype(bf16)
        copy = send_copy(s1.at[slot], y_hbm.at[k], t_partner(1))
        s1_slots.give(slot, copy.wait_send)
        first.wait_send()
        state["sum", k] = copy

    own_rows = pl.ds(pl.multiple_of(own * quarter, quarter), quarter)

    def rows_of(index):
        return pl.ds(pl.multiple_of(index * quarter, quarter), quarter)

    def sum_late(k):
        x_load = load(x_hbm.at[own_rows, :], xrow)
        half_loads = half_of(k, 1, ld1)
        state["sum", k].wait_recv()
        y_load = load(y_hbm.at[k], ldm)
        for copy in half_loads + [x_load, y_load]:
            copy.wait()
        totals = [
            buffers[k][1, pl.ds(e * 2 * quarter + quarter, quarter), :].astype(f32) + ld1[e].astype(f32) + ldm[e].astype(f32)
            for e in range(e_tiles)
        ]
        parts = [(e * CHUNK, (e + 1) * CHUNK) for e in range(e_tiles)]
        if k == 0:
            mean, rstd = mean_ref[own_rows, :], rstd_ref[own_rows, :]
            us = [(xrow[:, a:b].astype(f32) - mean) * rstd for a, b in parts]
            mean_w = sum(jnp.sum(t, -1, keepdims=True) for t in totals) * (1.0 / width)
            mean_wu = sum(jnp.sum(t * u, -1, keepdims=True) for t, u in zip(totals, us)) * (1.0 / width)
            for (a, b), t, u in zip(parts, totals, us):
                piece[k, :, a:b] = (cot[own_rows, a:b].astype(f32) + rstd * (t - mean_w - u * mean_wu)).astype(bf16)
        else:
            for (a, b), t in zip(parts, totals):
                piece[k, :, a:b] = (xrow[:, a:b].astype(f32) + t + vec[6:7, a:b]).astype(bf16)
        result = results[k]
        state["pieces", k] = [
            load(piece.at[k], result.at[own_rows, :]),
            send_copy(piece.at[k], result.at[own_rows, :], t_partner(1)),
            send_copy(piece.at[k], result.at[own_rows, :], t_partner(0)),
        ]

    def sum_gather(k):
        result = results[k]
        state["pieces", k][1].wait_recv()
        at = rows_of(t_flip(1))
        state["pieces", k].append(send_copy(result.at[at, :], result.at[at, :], t_partner(0)))

    def small_round(n):
        if n > 0:
            copy = state["small"]
            copy.wait()
            if n <= 2:
                small[0:4, :] += small_in[n - 1, 0:4, :]
            else:
                small[...] += small_in[n - 1]
        if n < 5:
            partner = t_partner(n) if n < 2 else dp_partner(n - 2)
            state["small"] = send_copy(small, small_in.at[n], partner)
        else:
            state["small"] = load(small, small_out)

    actions = dict(
        m=mlp, h=attention, a=w1, b=w2, c=a3, i=lambda k: sum_start(k), j=sum_middle, k=sum_late, l=sum_gather, s=small_round
    )
    for kind, n in jobs:
        actions[kind](n)

    for c in range(len(orders)):
        state[c].wait_recv()
    for k in range(2):
        local, first, second, third = state["pieces", k]
        local.wait()
        first.wait_send()
        second.wait()
        third.wait()
        state["sum", k]
    for slots in (s1_slots, s2_slots, s3_slots, k2_slots):
        slots.drain()
    state["small"].wait()


ORDER = " ".join(
    [
        "m0 a4 a0 m1",
        "m2 a2 a6 a5",
        "b0 m3 b4 a7",
        "h0 h1 a3 a8",
        "c4 i0 s0 s1",
        "c0 b6 b5 i1",
        "s2 c6 j0 b3",
        "a10 a1 b8 s3",
        "c5 c3 b10 j1",
        "b7 a9 a11 s4",
        "c8 b1 s5 k0",
        "c10 k1 b2 c7",
        "b9 c1 c9 b11",
        "c2 c11 l0 l1",
    ]
).split()
Z_FIRST = (0, 2, 7)


def layer_call(x, c, vectors, fc1, fc2, qkv_weight, dense):
    rows, width = x.shape
    hidden, qkv_columns, context_columns = fc1.shape[1], qkv_weight.shape[1], dense.shape[1]
    heads = qkv_columns // (3 * HEAD_DIM)
    total = 2 * hidden + qkv_columns + context_columns
    chunks = total // CHUNK
    vectors = [v.reshape(-1, 128) for v in vectors]
    jobs = [(word[0], int(word[1:])) for word in ORDER]
    orders = [(1, 0, 2) if n in Z_FIRST else (0, 1, 2) for n in range(chunks)]
    quarter, nb = rows // 4, width // 8
    anywhere = pl.BlockSpec(memory_space=pl.ANY)
    local = pl.BlockSpec(memory_space=pltpu.VMEM)
    shape = jax.ShapeDtypeStruct
    outs = [
        shape((rows, width), bf16),
        shape((rows, width), bf16),
        shape((nb, total), bf16),
        shape((nb, total), bf16),
        shape((8, width), f32),
        shape((chunks, 4, nb, CHUNK), bf16),
        shape((chunks, 2, nb, CHUNK), bf16),
        shape((2, width // CHUNK * 2 * quarter, CHUNK), bf16),
        shape((2, width // CHUNK, quarter, CHUNK), bf16),
    ]
    vmem = pltpu.VMEM
    scratch = [
        vmem((rows, width), bf16),
        vmem((rows, width), bf16),
        vmem((rows, width), bf16),
        vmem((rows, hidden), bf16),
        vmem((rows, hidden), bf16),
        vmem((rows, qkv_columns), bf16),
        vmem((rows, context_columns), bf16),
        vmem((rows, 1), f32),
        vmem((rows, 1), f32),
        vmem((SEQ, 128), f32),
        vmem((SEQ, 128), f32),
        vmem((VEC_ROWS, width), f32),
        vmem((VECTORS, width // 128, 128), bf16),
        vmem((2, width, CHUNK), bf16),
        vmem((2, width, CHUNK), bf16),
        vmem((5, 4, nb, CHUNK), bf16),
        vmem((6, 2, nb, CHUNK), bf16),
        vmem((6, nb, CHUNK), bf16),
        vmem((6, 2, nb, CHUNK), bf16),
        vmem((4, nb, CHUNK), bf16),
        vmem((4, nb, CHUNK), bf16),
        vmem((2, nb, CHUNK), bf16),
        vmem((2, quarter, width), bf16),
        vmem((quarter, width), bf16),
        vmem((8, width), f32),
        vmem((5, 8, width), f32),
        pltpu.SemaphoreType.DMA((88,)),
        pltpu.SemaphoreType.DMA((56,)),
        pltpu.SemaphoreType.DMA((56,)),
        pltpu.SemaphoreType.DMA((chunks,)),
    ]
    flops = 6 * rows * width * (2 * hidden + qkv_columns + context_columns)
    return pl.pallas_call(
        partial(layer_kernel, jobs=jobs, orders=orders, heads=heads),
        in_specs=[anywhere, anywhere, local] + [anywhere] * (4 + VECTORS),
        out_specs=[anywhere] * len(outs),
        out_shape=outs,
        scratch_shapes=scratch,
        compiler_params=pltpu.CompilerParams(vmem_limit_bytes=VMEM_LIMIT, collective_id=0, has_side_effects=True),
        cost_estimate=pl.CostEstimate(flops=flops, bytes_accessed=1 << 27, transcendentals=2 * rows * hidden),
        name="layer",
    )(x, c, angle_tables(), fc1, fc2, qkv_weight, dense, *vectors)


def finish_kernel(kept_ref, last_ref, out_ref, grad_ref, *refs):
    at = 0
    for ref in refs[:-2]:
        columns = slice(at, at + ref.shape[1])
        ref[...] = kept_ref[:, columns].astype(f32) + last_ref[:, columns].astype(f32)
        at += ref.shape[1]
    refs[-2][...] = out_ref[...]
    refs[-1][...] = grad_ref[...]


def finish_call(kept, last, output, input_grad, sizes, steps=4):
    nb, total = kept.shape
    rows, width = output.shape

    def tiles(count, columns):
        return pl.BlockSpec((count // steps, columns), lambda i: (i, 0))

    ins = [tiles(nb, total), tiles(nb, total), tiles(rows, width), tiles(rows, width)]
    outs = [tiles(nb, n) for n in sizes] + [tiles(rows, width)] * 2
    return pl.pallas_call(
        finish_kernel,
        grid=(steps,),
        in_specs=ins,
        out_specs=outs,
        out_shape=[jax.ShapeDtypeStruct((nb, n), f32) for n in sizes] + [jax.ShapeDtypeStruct((rows, width), bf16)] * 2,
        cost_estimate=pl.CostEstimate(flops=nb * total, bytes_accessed=8 * (nb * total + rows * width), transcendentals=0),
        name="finish",
    )(kept, last, output, input_grad)


def fused(
    layer_input,
    ln1_gain,
    ln1_bias,
    ln2_gain,
    ln2_bias,
    qkv_weight,
    qkv_bias,
    dense_weight,
    dense_bias,
    fc1_weight,
    fc1_bias,
    fc2_weight,
    fc2_bias,
    cotangent,
):
    whole_out, whole_grad, kept, last, small, *_ = layer_call(
        layer_input,
        cotangent,
        (ln1_gain, ln1_bias, ln2_gain, ln2_bias, fc1_bias, dense_bias, fc2_bias, qkv_bias),
        fc1_weight,
        fc2_weight,
        qkv_weight,
        dense_weight,
    )
    hidden, qkv_columns = fc1_weight.shape[1], qkv_weight.shape[1]
    grad_fc2, grad_fc1, grad_qkv, grad_dense, output, input_grad = finish_call(
        kept, last, whole_out, whole_grad, (hidden, hidden, qkv_columns, dense_weight.shape[1])
    )
    return (
        output,
        input_grad,
        small[0],
        small[1],
        small[2],
        small[3],
        grad_qkv,
        small[5, :qkv_columns],
        grad_dense,
        small[6],
        grad_fc1,
        small[4, :hidden],
        grad_fc2,
        small[6],
    )


def fits(mesh):
    return mesh.shape["dp"] == 8 and mesh.shape["tensor"] == 4


def normalize(x_float, gain_row, shift_row):
    row_mean = jnp.mean(x_float, -1, keepdims=True)
    centred = x_float - row_mean
    spread = jnp.mean(centred * centred, -1, keepdims=True)
    return centred * lax.rsqrt(spread + EPSILON) * gain_row + shift_row


def rotary_tables():
    half_rot = ROT // 2
    freq_index = jnp.arange(half_rot, dtype=jnp.float32)
    frequency = jnp.exp(freq_index * (-2.0 * math.log(10000.0) / ROT))
    angles = jnp.arange(SEQ, dtype=jnp.float32)[:, None] * frequency[None, :]
    return (jnp.cos(angles), jnp.sin(angles))


def rotate(operand, cos_table, sine_table):
    half_rot = ROT // 2
    first_half = operand[..., :half_rot]
    second_half = operand[..., half_rot:ROT]
    cos_part = cos_table[None, :, None, :]
    sine_part = sine_table[None, :, None, :]
    return jnp.concatenate(
        [
            first_half * cos_part - second_half * sine_part,
            second_half * cos_part + first_half * sine_part,
            operand[..., ROT:],
        ],
        -1,
    )


def unrotate(operand, cos_table, sine_table):
    half_rot = ROT // 2
    first_half = operand[..., :half_rot]
    second_half = operand[..., half_rot:ROT]
    cos_part = cos_table[None, :, None, :]
    sine_part = sine_table[None, :, None, :]
    return jnp.concatenate(
        [
            first_half * cos_part + second_half * sine_part,
            second_half * cos_part - first_half * sine_part,
            operand[..., ROT:],
        ],
        -1,
    )


def block_scores(query_block, key_block, start_row, score_scale):
    scores = (
        jnp.einsum("sqhd,skhd->shqk", query_block, key_block, preferred_element_type=jnp.float32)
        * score_scale
    )
    row_ids = start_row + jnp.arange(query_block.shape[1])[:, None]
    col_ids = jnp.arange(key_block.shape[1])[None, :]
    return jnp.where(col_ids <= row_ids, scores, -1e30)


def rounded(values_in):
    return lax.optimization_barrier(values_in.astype(jnp.bfloat16)).astype(jnp.float32)


def on_device(
    layer_input,
    ln1_gain,
    ln1_bias,
    ln2_gain,
    ln2_bias,
    qkv_weight,
    qkv_bias,
    dense_weight,
    dense_bias,
    fc1_weight,
    fc1_bias,
    fc2_weight,
    fc2_bias,
    cotangent,
):
    tok_rows, model_width = layer_input.shape
    local_heads = HEADS // lax.axis_size("tensor")
    seq_count = tok_rows // SEQ
    block_rows = 512
    score_scale = HEAD_DIM ** (-0.5)
    x_float = layer_input.astype(jnp.float32)
    gain_one = ln1_gain.astype(jnp.float32)
    shift_one = ln1_bias.astype(jnp.float32)
    gain_two = ln2_gain.astype(jnp.float32)
    shift_two = ln2_bias.astype(jnp.float32)
    attn_in = normalize(x_float, gain_one, shift_one).astype(jnp.bfloat16)
    mlp_in = normalize(x_float, gain_two, shift_two).astype(jnp.bfloat16)
    qkv_all = jnp.dot(attn_in, qkv_weight, preferred_element_type=jnp.float32) + qkv_bias.astype(
        jnp.float32
    )
    qkv_all = qkv_all.reshape(seq_count, SEQ, local_heads, 3, HEAD_DIM)
    cos_table, sine_table = rotary_tables()
    queries = rotate(qkv_all[..., 0, :], cos_table, sine_table).astype(jnp.bfloat16)
    keys_rot = rotate(qkv_all[..., 1, :], cos_table, sine_table).astype(jnp.bfloat16)
    values = qkv_all[..., 2, :].astype(jnp.bfloat16)
    context_blocks = []
    log_sums = []
    for start_row in range(0, SEQ, block_rows):
        key_end = start_row + block_rows
        masked = block_scores(
            queries[:, start_row:key_end], keys_rot[:, :key_end], start_row, score_scale
        )
        row_peak = jnp.max(masked, -1, keepdims=True)
        weights = jnp.exp(masked - row_peak)
        row_total = jnp.sum(weights, -1, keepdims=True)
        probabilities = (weights / row_total).astype(jnp.bfloat16)
        log_sums.append(row_peak + jnp.log(row_total))
        context_blocks.append(
            jnp.einsum(
                "shqk,skhd->sqhd",
                probabilities,
                values[:, :key_end],
                preferred_element_type=jnp.float32,
            )
        )
    context = jnp.concatenate(context_blocks, 1).astype(jnp.bfloat16)
    context_flat = context.reshape(tok_rows, local_heads * HEAD_DIM)
    attn_part = jnp.einsum(
        "td,ed->te", context_flat, dense_weight, preferred_element_type=jnp.float32
    )
    hidden = jnp.dot(mlp_in, fc1_weight, preferred_element_type=jnp.float32) + fc1_bias.astype(
        jnp.float32
    )
    exact_gelu = partial(jax.nn.gelu, approximate=False)
    activated = exact_gelu(hidden).astype(jnp.bfloat16)
    mlp_part = jnp.einsum("tf,ef->te", activated, fc2_weight, preferred_element_type=jnp.float32)
    partial_out = attn_part + mlp_part
    bias_total = dense_bias.astype(jnp.float32) + fc2_bias.astype(jnp.float32)
    full_sum = lax.psum(partial_out, "tensor")
    output = (x_float + full_sum + bias_total).astype(jnp.bfloat16)
    out_grad = cotangent.astype(jnp.float32)
    grad_fc2 = jnp.einsum("te,tf->ef", cotangent, activated, preferred_element_type=jnp.float32)
    grad_dense = jnp.einsum(
        "te,td->ed", cotangent, context_flat, preferred_element_type=jnp.float32
    )
    out_bias_grad = jnp.sum(out_grad, 0)
    activated_grad = jnp.einsum(
        "te,ef->tf", cotangent, fc2_weight, preferred_element_type=jnp.float32
    )
    gelu_pull = jax.vjp(exact_gelu, hidden)[1]
    hidden_grad = gelu_pull(activated_grad)[0].astype(jnp.bfloat16)
    grad_fc1 = jnp.einsum("td,tf->df", mlp_in, hidden_grad, preferred_element_type=jnp.float32)
    fc1_bias_grad = jnp.sum(hidden_grad.astype(jnp.float32), 0)
    mlp_in_grad = jnp.einsum(
        "tf,df->td", hidden_grad, fc1_weight, preferred_element_type=jnp.float32
    )
    context_grad = jnp.einsum(
        "te,ed->td", cotangent, dense_weight, preferred_element_type=jnp.float32
    ).astype(jnp.bfloat16)
    context_grad = context_grad.reshape(seq_count, SEQ, local_heads, HEAD_DIM)
    key_grad = jnp.zeros((seq_count, SEQ, local_heads, HEAD_DIM), jnp.float32)
    value_grad = jnp.zeros((seq_count, SEQ, local_heads, HEAD_DIM), jnp.float32)
    query_grads = []
    for block_number, start_row in enumerate(range(0, SEQ, block_rows)):
        key_end = start_row + block_rows
        query_block = queries[:, start_row:key_end]
        masked = block_scores(query_block, keys_rot[:, :key_end], start_row, score_scale)
        probabilities = jnp.exp(masked - log_sums[block_number])
        grad_block = context_grad[:, start_row:key_end]
        value_grad = value_grad.at[:, :key_end].add(
            jnp.einsum(
                "shqk,sqhd->skhd",
                probabilities.astype(jnp.bfloat16),
                grad_block,
                preferred_element_type=jnp.float32,
            )
        )
        prob_grad = jnp.einsum(
            "sqhd,skhd->shqk", grad_block, values[:, :key_end], preferred_element_type=jnp.float32
        )
        row_delta = jnp.sum(probabilities * prob_grad, -1, keepdims=True)
        score_grad = (probabilities * (prob_grad - row_delta)).astype(jnp.bfloat16)
        query_grads.append(
            jnp.einsum(
                "shqk,skhd->sqhd",
                score_grad,
                keys_rot[:, :key_end],
                preferred_element_type=jnp.float32,
            )
            * score_scale
        )
        key_grad = key_grad.at[:, :key_end].add(
            jnp.einsum(
                "shqk,sqhd->skhd", score_grad, query_block, preferred_element_type=jnp.float32
            )
            * score_scale
        )
    query_grad = jnp.concatenate(query_grads, 1)
    query_pre = unrotate(rounded(query_grad), cos_table, sine_table).astype(jnp.bfloat16)
    key_pre = unrotate(rounded(key_grad), cos_table, sine_table).astype(jnp.bfloat16)
    value_pre = value_grad.astype(jnp.bfloat16)
    qkv_grad = jnp.stack([query_pre, key_pre, value_pre], 3).reshape(
        tok_rows, local_heads * 3 * HEAD_DIM
    )
    grad_qkv = jnp.einsum("td,tc->dc", attn_in, qkv_grad, preferred_element_type=jnp.float32)
    qkv_bias_grad = jnp.sum(qkv_grad.astype(jnp.float32), 0)
    attn_in_grad = jnp.einsum("tc,dc->td", qkv_grad, qkv_weight, preferred_element_type=jnp.float32)
    norm_one_pull = jax.vjp(normalize, x_float, gain_one, shift_one)[1]
    input_one, gain_grad_one, shift_grad_one = norm_one_pull(attn_in_grad)
    norm_two_pull = jax.vjp(normalize, x_float, gain_two, shift_two)[1]
    input_two, gain_grad_two, shift_grad_two = norm_two_pull(mlp_in_grad)
    input_part = input_one + input_two
    input_total = lax.psum(input_part, "tensor")
    input_grad = (out_grad + input_total).astype(jnp.bfloat16)
    qkv_bias_grad, fc1_bias_grad, out_bias_grad = lax.psum(
        (qkv_bias_grad, fc1_bias_grad, out_bias_grad), "dp"
    )
    gain_grad_one, shift_grad_one, gain_grad_two, shift_grad_two = lax.psum(
        (gain_grad_one, shift_grad_one, gain_grad_two, shift_grad_two), ("dp", "tensor")
    )
    grad_qkv, grad_dense, grad_fc1, grad_fc2 = (
        lax.psum_scatter(
            grad_qkv.astype(jnp.bfloat16), "dp", scatter_dimension=0, tiled=True
        ).astype(jnp.float32),
        lax.psum_scatter(
            grad_dense.astype(jnp.bfloat16), "dp", scatter_dimension=0, tiled=True
        ).astype(jnp.float32),
        lax.psum_scatter(
            grad_fc1.astype(jnp.bfloat16), "dp", scatter_dimension=0, tiled=True
        ).astype(jnp.float32),
        lax.psum_scatter(
            grad_fc2.astype(jnp.bfloat16), "dp", scatter_dimension=0, tiled=True
        ).astype(jnp.float32),
    )
    return (
        output,
        input_grad,
        gain_grad_one,
        shift_grad_one,
        gain_grad_two,
        shift_grad_two,
        grad_qkv,
        qkv_bias_grad,
        grad_dense,
        out_bias_grad,
        grad_fc1,
        fc1_bias_grad,
        grad_fc2,
        out_bias_grad,
    )


def solution(mesh):
    in_specs = (
        P("dp", None),
        P(),
        P(),
        P(),
        P(),
        P(None, "tensor"),
        P("tensor"),
        P(None, "tensor"),
        P(),
        P(None, "tensor"),
        P("tensor"),
        P(None, "tensor"),
        P(),
        P("dp", None),
    )
    out_specs = (
        P("dp", None),
        P("dp", None),
        P(),
        P(),
        P(),
        P(),
        P("dp", "tensor"),
        P("tensor"),
        P("dp", "tensor"),
        P(),
        P("dp", "tensor"),
        P("tensor"),
        P("dp", "tensor"),
        P(),
    )
    return jax.shard_map(
        fused if fits(mesh) else on_device, mesh=mesh, in_specs=in_specs, out_specs=out_specs, check_vma=False
    )
```

```python
import itertools
import math
from functools import partial

import jax
import jax.numpy as jnp
from jax import lax
from jax.experimental import pallas as pl
from jax.experimental.pallas import tpu as pltpu
from jax.sharding import PartitionSpec as P

HEADS = 8
SEQ = 1024
HEAD_DIM = 256
ROT = 64
EPSILON = 1e-05
VMEM_LIMIT = 63 * 1024 * 1024

f32 = jnp.float32
bf16 = jnp.bfloat16
NN = (((1,), (0,)), ((), ()))
NT = (((1,), (1,)), ((), ()))
TN = (((0,), (0,)), ((), ()))


def dot(a, b, dims=NN):
    return lax.dot_general(a, b, dims, preferred_element_type=f32)


def turn(block, cos_table, sine_table):
    half_rot = ROT // 2
    head = block[:, :128]
    lane = lax.broadcasted_iota(jnp.int32, head.shape, 1)
    other = jnp.where(lane < half_rot, pltpu.roll(head, 128 - half_rot, 1), pltpu.roll(head, half_rot, 1))
    return jnp.concatenate([head * cos_table + other * sine_table, block[:, 128:]], 1)


def angle_tables():
    half_rot = ROT // 2
    lane = jnp.arange(128)
    frequency = jnp.exp((lane % half_rot).astype(f32) * (-2.0 * math.log(10000.0) / ROT))
    frequency = jnp.where(lane < ROT, frequency, 0.0)
    step = jnp.arange(32, dtype=f32)
    angles = jnp.concatenate([step, 32.0 * step])[:, None] * frequency[None, :]
    cos, sin = jnp.cos(angles), jnp.sin(angles)
    sign = jnp.where(lane < half_rot, -1.0, 1.0)[None, :]
    return jnp.concatenate([cos[:32], sin[:32], cos[32:], sin[32:], jnp.broadcast_to(sign, (8, 128))], 0)


CHUNK = 512
MESH = pl.DeviceIdType.MESH
VEC_ROWS = 8
VECTORS = 8
NORM_ROWS = 128


class Slots:
    def __init__(self, count):
        self.free = [(n, []) for n in range(count)]

    def take(self):
        slot, waits = self.free.pop(0)
        for wait in waits:
            wait()
        return slot

    def give(self, slot, *waits):
        self.free.append((slot, list(waits)))

    def drain(self):
        for _, waits in self.free:
            for wait in waits:
                wait()


def layer_kernel(
    x_hbm, c_hbm, table_in, fc1_hbm, fc2_hbm, wqkv_hbm, dense_hbm, *refs,
    jobs, orders, heads, block=256,
):
    vec_hbm, refs = refs[:VECTORS], refs[VECTORS:]
    (
        out_hbm, grad_hbm, keep_hbm, last_hbm, small_out, r1_hbm, r2_hbm, core_hbm, y_hbm,
        attn_in, mlp_in, cot, act, hg, qg, ctx, mean_ref, rstd_ref, cos_ref, sin_ref, vec, raw, w1buf, w2buf,
        s1, s2, s3, k2, ld1, ldm, ld2, piece, xrow, small, small_in,
        load_sem, send_sem, recv_sem, keep_sem,
    ) = refs
    rows, width = cot.shape
    hidden = act.shape[1]
    nb = width // 8
    quarter = rows // 4
    me, own = lax.axis_index("dp"), lax.axis_index("tensor")
    dp_bits = [lax.rem(lax.div(me, 1 << k), 2) for k in range(3)]
    t_bits = [lax.rem(lax.div(own, 1 << k), 2) for k in range(2)]

    def dp_flip(*bits):
        return me + sum((1 - 2 * dp_bits[k]) * (1 << k) for k in bits)

    def t_flip(*bits):
        return own + sum((1 - 2 * t_bits[k]) * (1 << k) for k in bits)

    def dp_partner(bit):
        return (dp_flip(bit), own)

    def t_partner(bit):
        return (me, t_flip(bit))

    partners = [dp_partner(k) for k in range(3)] + [t_partner(k) for k in range(2)]
    barrier = pltpu.get_barrier_semaphore()
    for partner in partners:
        pl.semaphore_signal(barrier, inc=1, device_id=partner, device_id_type=MESH)

    copies = itertools.count()

    def send_copy(src, dst, partner):
        n = next(copies)
        copy = pltpu.make_async_remote_copy(
            src_ref=src, dst_ref=dst, send_sem=send_sem.at[n], recv_sem=recv_sem.at[n], device_id=partner, device_id_type=MESH
        )
        copy.start()
        return copy

    loads = itertools.count()

    def load(src, dst):
        copy = pltpu.make_async_copy(src, dst, load_sem.at[next(loads)])
        copy.start()
        return copy

    load_x = load(x_hbm, act)
    load_v = [load(v, raw.at[n, pl.ds(0, v.shape[0])]) for n, v in enumerate(vec_hbm)]

    def mlp_weights(j):
        slot = j % 2
        at = pl.ds(j * CHUNK, CHUNK)
        return [load(fc1_hbm.at[:, at], w1buf.at[slot]), load(fc2_hbm.at[:, at], w2buf.at[slot])]

    def head_weights(h):
        slot = h % 2
        base = 3 * h * HEAD_DIM
        return [
            load(wqkv_hbm.at[:, pl.ds(base, 2 * HEAD_DIM)], w1buf.at[slot]),
            load(wqkv_hbm.at[:, pl.ds(base + 2 * HEAD_DIM, HEAD_DIM)], w2buf.at[slot, :, pl.ds(0, HEAD_DIM)]),
            load(dense_hbm.at[:, pl.ds(h * HEAD_DIM, HEAD_DIM)], w2buf.at[slot, :, pl.ds(HEAD_DIM, HEAD_DIM)]),
        ]

    weights = {("mlp", 0): mlp_weights(0)}
    load_c = load(c_hbm, cot)
    weights["mlp", 1] = mlp_weights(1)
    tiles = hidden // CHUNK

    small[...] = jnp.zeros_like(small)
    for copy in load_v:
        copy.wait()
    for n in range(VECTORS):
        packed = raw[n].astype(f32)
        if n == 6:
            packed = packed + raw[5].astype(f32)
        for i in range(vec_hbm[n].shape[0]):
            vec[n : n + 1, i * 128 : (i + 1) * 128] = packed[i : i + 1, :]
    low_cos, low_sin = table_in[0:32, :], table_in[32:64, :]
    sign = table_in[128:129, :]
    for n in range(SEQ // 32):
        high_cos, high_sin = table_in[64 + n : 65 + n, :], table_in[96 + n : 97 + n, :]
        cos_ref[n * 32 : (n + 1) * 32, :] = high_cos * low_cos - high_sin * low_sin
        sin_ref[n * 32 : (n + 1) * 32, :] = sign * (high_sin * low_cos + high_cos * low_sin)

    load_x.wait()

    def norm_rows(i, _):
        part = pl.ds(pl.multiple_of(i * NORM_ROWS, NORM_ROWS), NORM_ROWS)
        x = act[part, :].astype(f32)
        mean = jnp.mean(x, -1, keepdims=True)
        centred = x - mean
        rstd = lax.rsqrt(jnp.mean(centred * centred, -1, keepdims=True) + EPSILON)
        u = centred * rstd
        attn_in[part, :] = (u * vec[0:1, :] + vec[1:2, :]).astype(bf16)
        mlp_in[part, :] = (u * vec[2:3, :] + vec[3:4, :]).astype(bf16)
        mean_ref[part, :] = mean
        rstd_ref[part, :] = rstd
        return 0

    lax.fori_loop(0, rows // NORM_ROWS, norm_rows, 0)
    load_c.wait()
    pl.semaphore_wait(barrier, len(partners))

    s1_slots, s2_slots, s3_slots, k2_slots = Slots(s1.shape[0]), Slots(s2.shape[0]), Slots(s3.shape[0]), Slots(k2.shape[0])
    state = {}

    def operands(c):
        n_fc = hidden // CHUNK
        n_qkv = qg.shape[1] // CHUNK
        if c < n_fc:
            return cot, act, c
        if c < 2 * n_fc:
            return mlp_in, hg, c - n_fc
        if c < 2 * n_fc + n_qkv:
            return attn_in, qg, c - 2 * n_fc
        return cot, ctx, c - 2 * n_fc - n_qkv

    def block_of(lhs, index):
        return lhs[:, pl.ds(pl.multiple_of(index * nb, nb), nb)]

    def w1(c):
        lhs, rhs, j = operands(c)
        one, two, three = orders[c]
        slot = s1_slots.take()
        base = dp_flip(one, two, three)

        def body(n, _):
            second, third = n // 2, lax.rem(n, 2)
            index = base - second * (1 - 2 * dp_bits[two]) * (1 << two) - third * (1 - 2 * dp_bits[three]) * (1 << three)
            s1[slot, n] = dot(block_of(lhs, index), rhs[:, j * CHUNK : (j + 1) * CHUNK], TN).astype(bf16)
            return 0

        lax.fori_loop(0, 4, body, 0)
        copy = send_copy(s1.at[slot], r1_hbm.at[c], dp_partner(one))
        s1_slots.give(slot, copy.wait_send)
        state[c] = copy

    def w2(c):
        lhs, rhs, j = operands(c)
        one, two, three = orders[c]
        state[c].wait_recv()
        loaded = load(r1_hbm.at[c], ld1)
        slot, kept = s2_slots.take(), k2_slots.take()
        loaded.wait()

        def part(base, n, out):
            def body(i, _):
                index = base - i * (1 - 2 * dp_bits[three]) * (1 << three)
                out[i] = (dot(block_of(lhs, index), rhs[:, j * CHUNK : (j + 1) * CHUNK], TN) + ld1[n + i].astype(f32)).astype(bf16)
                return 0

            lax.fori_loop(0, 2, body, 0)

        part(dp_flip(two, three), 0, s2.at[slot])
        copy = send_copy(s2.at[slot], r2_hbm.at[c], dp_partner(two))
        s2_slots.give(slot, copy.wait_send)
        part(dp_flip(three), 2, k2.at[kept])
        state[c] = (copy, kept)

    def a3(c):
        copy, kept = state[c]
        three = orders[c][2]
        copy.wait_recv()
        loaded = load(r2_hbm.at[c], ld2)
        slot = s3_slots.take()
        loaded.wait()
        s3[slot] = (k2[kept, 0].astype(f32) + ld2[0].astype(f32)).astype(bf16)
        columns = pl.ds(c * CHUNK, CHUNK)
        copy = send_copy(s3.at[slot], last_hbm.at[:, columns], dp_partner(three))
        s3_slots.give(slot, copy.wait_send)
        k2[kept, 1] = (k2[kept, 1].astype(f32) + ld2[1].astype(f32)).astype(bf16)
        keep = pltpu.make_async_copy(k2.at[kept, 1], keep_hbm.at[:, columns], keep_sem.at[c])
        keep.start()
        k2_slots.give(kept, keep.wait)
        state[c] = copy

    def mlp(j):
        slot = j % 2
        for copy in weights.pop(("mlp", j)):
            copy.wait()
        at = j * CHUNK
        bias = vec[4:5, at : at + CHUNK]

        def body(i, sums):
            part = pl.ds(pl.multiple_of(i * block, block), block)
            h = dot(mlp_in[part, :], w1buf[slot]) + bias
            above = dot(cot[part, :], w2buf[slot])
            cdf = 0.5 + 0.5 * lax.erf(h * (2.0**-0.5))
            density = jnp.exp(h * h * -0.5) * ((2.0 * math.pi) ** -0.5)
            act[part, at : at + CHUNK] = (h * cdf).astype(bf16)
            low = (above * (cdf + h * density)).astype(bf16)
            hg[part, at : at + CHUNK] = low
            above_sum = jnp.sum(cot[part, at : at + CHUNK].astype(f32), 0, keepdims=True)
            return sums[0] + jnp.sum(low.astype(f32), 0, keepdims=True), sums[1] + above_sum

        zero = jnp.zeros((1, CHUNK), f32)
        bias_sum, above_sum = lax.fori_loop(0, rows // block, body, (zero, zero))
        small[4:5, at : at + CHUNK] = bias_sum
        small[6:7, at : at + CHUNK] = above_sum
        if j + 2 < tiles:
            weights["mlp", j + 2] = mlp_weights(j + 2)
        else:
            h = j + 2 - tiles
            weights["head", h] = head_weights(h)

    def attention(n):
        if n > 0:
            return
        for h in range(heads):
            for copy in weights.pop(("head", h)):
                copy.wait()
        lax.fori_loop(0, heads, one_head, 0)

    def one_head(slot, _):
        base = pl.multiple_of(3 * HEAD_DIM * slot, HEAD_DIM)
        scale = HEAD_DIM ** (-0.5)

        def third(n):
            return pl.ds(pl.multiple_of(base + n * HEAD_DIM, HEAD_DIM), HEAD_DIM)

        mine = pl.ds(pl.multiple_of(slot * HEAD_DIM, HEAD_DIM), HEAD_DIM)

        def scoped(qkv_ref, g_ref, dk_ref, dv_ref):
            def project(i, _):
                part = pl.ds(pl.multiple_of(i * block, block), block)
                acc = dot(attn_in[part, :], w1buf[slot]) + vec[7:8, pl.ds(base, 2 * HEAD_DIM)]
                cos, sin = cos_ref[part, :], sin_ref[part, :]
                for n in range(2):
                    at = n * HEAD_DIM
                    qkv_ref[part, at : at + HEAD_DIM] = turn(acc[:, at : at + HEAD_DIM], cos, sin).astype(bf16)
                acc = dot(attn_in[part, :], w2buf[slot, :, 0:HEAD_DIM]) + vec[7:8, third(2)]
                qkv_ref[part, 2 * HEAD_DIM :] = acc.astype(bf16)
                g_ref[part, :] = dot(cot[part, :], w2buf[slot, :, HEAD_DIM : 2 * HEAD_DIM]).astype(bf16)
                return 0

            lax.fori_loop(0, rows // block, project, 0)
            for i in reversed(range(SEQ // block)):
                part = pl.ds(i * block, block)
                key_end = (i + 1) * block
                keys = pl.ds(0, key_end)
                q, g = qkv_ref[part, 0:HEAD_DIM], g_ref[part, :]
                k, v = qkv_ref[keys, HEAD_DIM : 2 * HEAD_DIM], qkv_ref[keys, 2 * HEAD_DIM :]
                scores = dot(q, k, NT) * scale
                row_id = i * block + lax.broadcasted_iota(jnp.int32, scores.shape, 0)
                col_id = lax.broadcasted_iota(jnp.int32, scores.shape, 1)
                scores = jnp.where(col_id <= row_id, scores, -1e30)
                e = jnp.exp(scores - jnp.max(scores, -1, keepdims=True))
                probs = e / jnp.sum(e, -1, keepdims=True)
                low = probs.astype(bf16)
                ctx[part, mine] = dot(low, v).astype(bf16)
                prob_grad = dot(g, v, NT)
                delta = jnp.sum(probs * prob_grad, -1, keepdims=True)
                score_grad = (probs * (prob_grad - delta)).astype(bf16)
                dv = dot(low, g, TN)
                dk = dot(score_grad, q, TN)
                if i == SEQ // block - 1:
                    dv_ref[...] = dv
                    dk_ref[...] = dk
                else:
                    dv_ref[keys, :] += dv
                    dk_ref[keys, :] += dk
                dq = (dot(score_grad, k) * scale).astype(bf16).astype(f32)
                qg[part, third(0)] = turn(dq, cos_ref[part, :], -sin_ref[part, :]).astype(bf16)
            dk = (dk_ref[...] * scale).astype(bf16).astype(f32)
            qg[:, third(1)] = turn(dk, cos_ref[...], -sin_ref[...]).astype(bf16)
            qg[:, third(2)] = dv_ref[...].astype(bf16)
            for n in range(3):
                small[5:6, third(n)] = jnp.sum(qg[:, third(n)].astype(f32), 0, keepdims=True)

        pl.run_scoped(
            scoped,
            pltpu.VMEM((SEQ, 3 * HEAD_DIM), bf16),
            pltpu.VMEM((SEQ, HEAD_DIM), bf16),
            pltpu.VMEM((SEQ, HEAD_DIM), f32),
            pltpu.VMEM((SEQ, HEAD_DIM), f32),
        )
        return 0

    def quarter_of(n):
        index = own + (1 - n // 2) * (1 - 2 * t_bits[0]) + (1 - lax.rem(n, 2)) * (1 - 2 * t_bits[1]) * 2
        return pl.ds(pl.multiple_of(index * quarter, quarter), quarter)

    def back_tiles(buf, first_hbm, first, second_hbm, second, x_tiles, store):
        step = CHUNK // 2

        def scoped(first_w, second_w, x_w, sems):
            def copies_of(d, slot):
                at = pl.ds(pl.multiple_of(d * step, step), step)
                made = [
                    pltpu.make_async_copy(first_hbm.at[at, :], first_w.at[slot], sems.at[slot, 0]),
                    pltpu.make_async_copy(second_hbm.at[at, :], second_w.at[slot], sems.at[slot, 1]),
                ]
                if x_tiles:
                    made.append(pltpu.make_async_copy(x_hbm.at[:, at], x_w.at[slot], sems.at[slot, 2]))
                return made

            n_steps = width // step
            for copy in copies_of(0, 0):
                copy.start()

            def body(e, _):
                for half in range(2):
                    d = 2 * e + half
                    for copy in copies_of(d, half):
                        copy.wait()

                    @pl.when(d + 1 < n_steps)
                    def _():
                        for copy in copies_of(d + 1, 1 - half):
                            copy.start()

                    columns = pl.ds(half * step, step)

                    def one(m, sums):
                        for n in (2 * m, 2 * m + 1):
                            part = quarter_of(n)
                            a = dot(first[part, :], first_w[half], NT)
                            b = dot(second[part, :], second_w[half], NT)
                            at = pl.ds(pl.multiple_of(e * 2 * quarter + lax.rem(n, 2) * quarter, quarter), quarter)
                            buf[m, at, columns], terms = store(d, part, a, b, x_w.at[half])
                            sums = tuple(s + t for s, t in zip(sums, terms))
                        return sums

                    count = 4 if x_tiles else 0
                    sums = lax.fori_loop(0, 2, one, tuple(jnp.zeros((1, step), f32) for _ in range(count)))
                    if x_tiles:
                        at = pl.ds(pl.multiple_of(d * step, step), step)
                        small[0:4, at] = jnp.concatenate(sums, 0)
                return 0

            lax.fori_loop(0, n_steps // 2, body, 0)

        pl.run_scoped(
            scoped,
            pltpu.VMEM((2, step, first.shape[1]), bf16),
            pltpu.VMEM((2, step, second.shape[1]), bf16),
            pltpu.VMEM((2, rows if x_tiles else 16, step), bf16),
            pltpu.SemaphoreType.DMA((2, 3)),
        )

    def input_tiles():
        step = CHUNK // 2

        def store(d, part, a, b, x_tile):
            at = pl.ds(pl.multiple_of(d * step, step), step)
            u = (x_tile[part, :].astype(f32) - mean_ref[part, :]) * rstd_ref[part, :]
            terms = [jnp.sum(t, 0, keepdims=True) for t in (a * u, a, b * u, b)]
            return (a * vec[0:1, at] + b * vec[2:3, at]).astype(bf16), terms

        back_tiles(w1buf, wqkv_hbm, qg, fc1_hbm, hg, True, store)

    def output_tiles():
        back_tiles(w2buf, dense_hbm, ctx, fc2_hbm, act, False, lambda d, part, a, b, x_tile: ((a + b).astype(bf16), []))

    e_tiles = width // CHUNK
    buffers = (w1buf, w2buf)
    results = (grad_hbm, out_hbm)

    def sum_start(k):
        (input_tiles, output_tiles)[k]()
        state["sum", k] = send_copy(buffers[k].at[0], core_hbm.at[k], t_partner(0))

    def half_of(k, half, dst):
        return [
            load(core_hbm.at[k, pl.ds(e * 2 * quarter + half * quarter, quarter), :], dst.at[e]) for e in range(e_tiles)
        ]

    def sum_middle(k):
        first = state["sum", k]
        first.wait_recv()
        loaded = half_of(k, 0, ld1)
        slot = s1_slots.take()
        for copy in loaded:
            copy.wait()
        for e in range(e_tiles):
            s1[slot, e] = (buffers[k][1, pl.ds(e * 2 * quarter, quarter), :].astype(f32) + ld1[e].astype(f32)).astype(bf16)
        copy = send_copy(s1.at[slot], y_hbm.at[k], t_partner(1))
        s1_slots.give(slot, copy.wait_send)
        first.wait_send()
        state["sum", k] = copy

    own_rows = pl.ds(pl.multiple_of(own * quarter, quarter), quarter)

    def rows_of(index):
        return pl.ds(pl.multiple_of(index * quarter, quarter), quarter)

    def sum_late(k):
        x_load = load(x_hbm.at[own_rows, :], xrow)
        half_loads = half_of(k, 1, ld1)
        state["sum", k].wait_recv()
        y_load = load(y_hbm.at[k], ldm)
        for copy in half_loads + [x_load, y_load]:
            copy.wait()
        totals = [
            buffers[k][1, pl.ds(e * 2 * quarter + quarter, quarter), :].astype(f32) + ld1[e].astype(f32) + ldm[e].astype(f32)
            for e in range(e_tiles)
        ]
        parts = [(e * CHUNK, (e + 1) * CHUNK) for e in range(e_tiles)]
        if k == 0:
            mean, rstd = mean_ref[own_rows, :], rstd_ref[own_rows, :]
            us = [(xrow[:, a:b].astype(f32) - mean) * rstd for a, b in parts]
            mean_w = sum(jnp.sum(t, -1, keepdims=True) for t in totals) * (1.0 / width)
            mean_wu = sum(jnp.sum(t * u, -1, keepdims=True) for t, u in zip(totals, us)) * (1.0 / width)
            for (a, b), t, u in zip(parts, totals, us):
                piece[k, :, a:b] = (cot[own_rows, a:b].astype(f32) + rstd * (t - mean_w - u * mean_wu)).astype(bf16)
        else:
            for (a, b), t in zip(parts, totals):
                piece[k, :, a:b] = (xrow[:, a:b].astype(f32) + t + vec[6:7, a:b]).astype(bf16)
        result = results[k]
        state["pieces", k] = [
            load(piece.at[k], result.at[own_rows, :]),
            send_copy(piece.at[k], result.at[own_rows, :], t_partner(1)),
            send_copy(piece.at[k], result.at[own_rows, :], t_partner(0)),
        ]

    def sum_gather(k):
        result = results[k]
        state["pieces", k][1].wait_recv()
        at = rows_of(t_flip(1))
        state["pieces", k].append(send_copy(result.at[at, :], result.at[at, :], t_partner(0)))

    def small_round(n):
        if n > 0:
            copy = state["small"]
            copy.wait()
            if n <= 2:
                small[0:4, :] += small_in[n - 1, 0:4, :]
            else:
                small[...] += small_in[n - 1]
        if n < 5:
            partner = t_partner(n) if n < 2 else dp_partner(n - 2)
            state["small"] = send_copy(small, small_in.at[n], partner)
        else:
            state["small"] = load(small, small_out)

    actions = dict(
        m=mlp, h=attention, a=w1, b=w2, c=a3, i=lambda k: sum_start(k), j=sum_middle, k=sum_late, l=sum_gather, s=small_round
    )
    for kind, n in jobs:
        actions[kind](n)

    for c in range(len(orders)):
        state[c].wait_recv()
    for k in range(2):
        local, first, second, third = state["pieces", k]
        local.wait()
        first.wait_send()
        second.wait()
        third.wait()
        state["sum", k]
    for slots in (s1_slots, s2_slots, s3_slots, k2_slots):
        slots.drain()
    state["small"].wait()


ORDER = " ".join(
    [
        "m0 a4 a0 m1",
        "m2 a5 m3 a7",
        "a2 h0 b4 h1",
        "b7 a1 a10 b5",
        "c4 i0 c7 a11",
        "s0 s1 b2 j0",
        "a8 c5 b1 s2",
        "i1 c2 j1 a3",
        "b11 a6 b10 c1",
        "b8 k1 c11 b3",
        "c8 c3 s3 b6",
        "a9 c10 l1 s4",
        "b0 s5 k0 c6",
        "b9 c0 c9 l0",
    ]
).split()
Z_FIRST = (0, 5, 10)


def layer_call(x, c, vectors, fc1, fc2, qkv_weight, dense):
    rows, width = x.shape
    hidden, qkv_columns, context_columns = fc1.shape[1], qkv_weight.shape[1], dense.shape[1]
    heads = qkv_columns // (3 * HEAD_DIM)
    total = 2 * hidden + qkv_columns + context_columns
    chunks = total // CHUNK
    vectors = [v.reshape(-1, 128) for v in vectors]
    jobs = [(word[0], int(word[1:])) for word in ORDER]
    orders = [(1, 0, 2) if n in Z_FIRST else (0, 1, 2) for n in range(chunks)]
    quarter, nb = rows // 4, width // 8
    anywhere = pl.BlockSpec(memory_space=pl.ANY)
    local = pl.BlockSpec(memory_space=pltpu.VMEM)
    shape = jax.ShapeDtypeStruct
    outs = [
        shape((rows, width), bf16),
        shape((rows, width), bf16),
        shape((nb, total), bf16),
        shape((nb, total), bf16),
        shape((8, width), f32),
        shape((chunks, 4, nb, CHUNK), bf16),
        shape((chunks, 2, nb, CHUNK), bf16),
        shape((2, width // CHUNK * 2 * quarter, CHUNK), bf16),
        shape((2, width // CHUNK, quarter, CHUNK), bf16),
    ]
    vmem = pltpu.VMEM
    scratch = [
        vmem((rows, width), bf16),
        vmem((rows, width), bf16),
        vmem((rows, width), bf16),
        vmem((rows, hidden), bf16),
        vmem((rows, hidden), bf16),
        vmem((rows, qkv_columns), bf16),
        vmem((rows, context_columns), bf16),
        vmem((rows, 1), f32),
        vmem((rows, 1), f32),
        vmem((SEQ, 128), f32),
        vmem((SEQ, 128), f32),
        vmem((VEC_ROWS, width), f32),
        vmem((VECTORS, width // 128, 128), bf16),
        vmem((2, width, CHUNK), bf16),
        vmem((2, width, CHUNK), bf16),
        vmem((5, 4, nb, CHUNK), bf16),
        vmem((6, 2, nb, CHUNK), bf16),
        vmem((6, nb, CHUNK), bf16),
        vmem((6, 2, nb, CHUNK), bf16),
        vmem((4, nb, CHUNK), bf16),
        vmem((4, nb, CHUNK), bf16),
        vmem((2, nb, CHUNK), bf16),
        vmem((2, quarter, width), bf16),
        vmem((quarter, width), bf16),
        vmem((8, width), f32),
        vmem((5, 8, width), f32),
        pltpu.SemaphoreType.DMA((88,)),
        pltpu.SemaphoreType.DMA((56,)),
        pltpu.SemaphoreType.DMA((56,)),
        pltpu.SemaphoreType.DMA((chunks,)),
    ]
    flops = 6 * rows * width * (2 * hidden + qkv_columns + context_columns)
    return pl.pallas_call(
        partial(layer_kernel, jobs=jobs, orders=orders, heads=heads),
        in_specs=[anywhere, anywhere, local] + [anywhere] * (4 + VECTORS),
        out_specs=[anywhere] * len(outs),
        out_shape=outs,
        scratch_shapes=scratch,
        compiler_params=pltpu.CompilerParams(vmem_limit_bytes=VMEM_LIMIT, collective_id=0, has_side_effects=True),
        cost_estimate=pl.CostEstimate(flops=flops, bytes_accessed=1 << 27, transcendentals=2 * rows * hidden),
        name="layer",
    )(x, c, angle_tables(), fc1, fc2, qkv_weight, dense, *vectors)


def finish_kernel(kept_ref, last_ref, out_ref, grad_ref, *refs):
    at = 0
    for ref in refs[:-2]:
        columns = slice(at, at + ref.shape[1])
        ref[...] = kept_ref[:, columns].astype(f32) + last_ref[:, columns].astype(f32)
        at += ref.shape[1]
    refs[-2][...] = out_ref[...]
    refs[-1][...] = grad_ref[...]


def finish_call(kept, last, output, input_grad, sizes, steps=4):
    nb, total = kept.shape
    rows, width = output.shape

    def tiles(count, columns):
        return pl.BlockSpec((count // steps, columns), lambda i: (i, 0))

    ins = [tiles(nb, total), tiles(nb, total), tiles(rows, width), tiles(rows, width)]
    outs = [tiles(nb, n) for n in sizes] + [tiles(rows, width)] * 2
    return pl.pallas_call(
        finish_kernel,
        grid=(steps,),
        in_specs=ins,
        out_specs=outs,
        out_shape=[jax.ShapeDtypeStruct((nb, n), f32) for n in sizes] + [jax.ShapeDtypeStruct((rows, width), bf16)] * 2,
        cost_estimate=pl.CostEstimate(flops=nb * total, bytes_accessed=8 * (nb * total + rows * width), transcendentals=0),
        name="finish",
    )(kept, last, output, input_grad)


def fused(
    layer_input,
    ln1_gain,
    ln1_bias,
    ln2_gain,
    ln2_bias,
    qkv_weight,
    qkv_bias,
    dense_weight,
    dense_bias,
    fc1_weight,
    fc1_bias,
    fc2_weight,
    fc2_bias,
    cotangent,
):
    whole_out, whole_grad, kept, last, small, *_ = layer_call(
        layer_input,
        cotangent,
        (ln1_gain, ln1_bias, ln2_gain, ln2_bias, fc1_bias, dense_bias, fc2_bias, qkv_bias),
        fc1_weight,
        fc2_weight,
        qkv_weight,
        dense_weight,
    )
    hidden, qkv_columns = fc1_weight.shape[1], qkv_weight.shape[1]
    grad_fc2, grad_fc1, grad_qkv, grad_dense, output, input_grad = finish_call(
        kept, last, whole_out, whole_grad, (hidden, hidden, qkv_columns, dense_weight.shape[1])
    )
    return (
        output,
        input_grad,
        small[0],
        small[1],
        small[2],
        small[3],
        grad_qkv,
        small[5, :qkv_columns],
        grad_dense,
        small[6],
        grad_fc1,
        small[4, :hidden],
        grad_fc2,
        small[6],
    )


def fits(mesh):
    return mesh.shape["dp"] == 8 and mesh.shape["tensor"] == 4


def normalize(x_float, gain_row, shift_row):
    row_mean = jnp.mean(x_float, -1, keepdims=True)
    centred = x_float - row_mean
    spread = jnp.mean(centred * centred, -1, keepdims=True)
    return centred * lax.rsqrt(spread + EPSILON) * gain_row + shift_row


def rotary_tables():
    half_rot = ROT // 2
    freq_index = jnp.arange(half_rot, dtype=jnp.float32)
    frequency = jnp.exp(freq_index * (-2.0 * math.log(10000.0) / ROT))
    angles = jnp.arange(SEQ, dtype=jnp.float32)[:, None] * frequency[None, :]
    return (jnp.cos(angles), jnp.sin(angles))


def rotate(operand, cos_table, sine_table):
    half_rot = ROT // 2
    first_half = operand[..., :half_rot]
    second_half = operand[..., half_rot:ROT]
    cos_part = cos_table[None, :, None, :]
    sine_part = sine_table[None, :, None, :]
    return jnp.concatenate(
        [
            first_half * cos_part - second_half * sine_part,
            second_half * cos_part + first_half * sine_part,
            operand[..., ROT:],
        ],
        -1,
    )


def unrotate(operand, cos_table, sine_table):
    half_rot = ROT // 2
    first_half = operand[..., :half_rot]
    second_half = operand[..., half_rot:ROT]
    cos_part = cos_table[None, :, None, :]
    sine_part = sine_table[None, :, None, :]
    return jnp.concatenate(
        [
            first_half * cos_part + second_half * sine_part,
            second_half * cos_part - first_half * sine_part,
            operand[..., ROT:],
        ],
        -1,
    )


def block_scores(query_block, key_block, start_row, score_scale):
    scores = (
        jnp.einsum("sqhd,skhd->shqk", query_block, key_block, preferred_element_type=jnp.float32)
        * score_scale
    )
    row_ids = start_row + jnp.arange(query_block.shape[1])[:, None]
    col_ids = jnp.arange(key_block.shape[1])[None, :]
    return jnp.where(col_ids <= row_ids, scores, -1e30)


def rounded(values_in):
    return lax.optimization_barrier(values_in.astype(jnp.bfloat16)).astype(jnp.float32)


def on_device(
    layer_input,
    ln1_gain,
    ln1_bias,
    ln2_gain,
    ln2_bias,
    qkv_weight,
    qkv_bias,
    dense_weight,
    dense_bias,
    fc1_weight,
    fc1_bias,
    fc2_weight,
    fc2_bias,
    cotangent,
):
    tok_rows, model_width = layer_input.shape
    local_heads = HEADS // lax.axis_size("tensor")
    seq_count = tok_rows // SEQ
    block_rows = 512
    score_scale = HEAD_DIM ** (-0.5)
    x_float = layer_input.astype(jnp.float32)
    gain_one = ln1_gain.astype(jnp.float32)
    shift_one = ln1_bias.astype(jnp.float32)
    gain_two = ln2_gain.astype(jnp.float32)
    shift_two = ln2_bias.astype(jnp.float32)
    attn_in = normalize(x_float, gain_one, shift_one).astype(jnp.bfloat16)
    mlp_in = normalize(x_float, gain_two, shift_two).astype(jnp.bfloat16)
    qkv_all = jnp.dot(attn_in, qkv_weight, preferred_element_type=jnp.float32) + qkv_bias.astype(
        jnp.float32
    )
    qkv_all = qkv_all.reshape(seq_count, SEQ, local_heads, 3, HEAD_DIM)
    cos_table, sine_table = rotary_tables()
    queries = rotate(qkv_all[..., 0, :], cos_table, sine_table).astype(jnp.bfloat16)
    keys_rot = rotate(qkv_all[..., 1, :], cos_table, sine_table).astype(jnp.bfloat16)
    values = qkv_all[..., 2, :].astype(jnp.bfloat16)
    context_blocks = []
    log_sums = []
    for start_row in range(0, SEQ, block_rows):
        key_end = start_row + block_rows
        masked = block_scores(
            queries[:, start_row:key_end], keys_rot[:, :key_end], start_row, score_scale
        )
        row_peak = jnp.max(masked, -1, keepdims=True)
        weights = jnp.exp(masked - row_peak)
        row_total = jnp.sum(weights, -1, keepdims=True)
        probabilities = (weights / row_total).astype(jnp.bfloat16)
        log_sums.append(row_peak + jnp.log(row_total))
        context_blocks.append(
            jnp.einsum(
                "shqk,skhd->sqhd",
                probabilities,
                values[:, :key_end],
                preferred_element_type=jnp.float32,
            )
        )
    context = jnp.concatenate(context_blocks, 1).astype(jnp.bfloat16)
    context_flat = context.reshape(tok_rows, local_heads * HEAD_DIM)
    attn_part = jnp.einsum(
        "td,ed->te", context_flat, dense_weight, preferred_element_type=jnp.float32
    )
    hidden = jnp.dot(mlp_in, fc1_weight, preferred_element_type=jnp.float32) + fc1_bias.astype(
        jnp.float32
    )
    exact_gelu = partial(jax.nn.gelu, approximate=False)
    activated = exact_gelu(hidden).astype(jnp.bfloat16)
    mlp_part = jnp.einsum("tf,ef->te", activated, fc2_weight, preferred_element_type=jnp.float32)
    partial_out = attn_part + mlp_part
    bias_total = dense_bias.astype(jnp.float32) + fc2_bias.astype(jnp.float32)
    full_sum = lax.psum(partial_out, "tensor")
    output = (x_float + full_sum + bias_total).astype(jnp.bfloat16)
    out_grad = cotangent.astype(jnp.float32)
    grad_fc2 = jnp.einsum("te,tf->ef", cotangent, activated, preferred_element_type=jnp.float32)
    grad_dense = jnp.einsum(
        "te,td->ed", cotangent, context_flat, preferred_element_type=jnp.float32
    )
    out_bias_grad = jnp.sum(out_grad, 0)
    activated_grad = jnp.einsum(
        "te,ef->tf", cotangent, fc2_weight, preferred_element_type=jnp.float32
    )
    gelu_pull = jax.vjp(exact_gelu, hidden)[1]
    hidden_grad = gelu_pull(activated_grad)[0].astype(jnp.bfloat16)
    grad_fc1 = jnp.einsum("td,tf->df", mlp_in, hidden_grad, preferred_element_type=jnp.float32)
    fc1_bias_grad = jnp.sum(hidden_grad.astype(jnp.float32), 0)
    mlp_in_grad = jnp.einsum(
        "tf,df->td", hidden_grad, fc1_weight, preferred_element_type=jnp.float32
    )
    context_grad = jnp.einsum(
        "te,ed->td", cotangent, dense_weight, preferred_element_type=jnp.float32
    ).astype(jnp.bfloat16)
    context_grad = context_grad.reshape(seq_count, SEQ, local_heads, HEAD_DIM)
    key_grad = jnp.zeros((seq_count, SEQ, local_heads, HEAD_DIM), jnp.float32)
    value_grad = jnp.zeros((seq_count, SEQ, local_heads, HEAD_DIM), jnp.float32)
    query_grads = []
    for block_number, start_row in enumerate(range(0, SEQ, block_rows)):
        key_end = start_row + block_rows
        query_block = queries[:, start_row:key_end]
        masked = block_scores(query_block, keys_rot[:, :key_end], start_row, score_scale)
        probabilities = jnp.exp(masked - log_sums[block_number])
        grad_block = context_grad[:, start_row:key_end]
        value_grad = value_grad.at[:, :key_end].add(
            jnp.einsum(
                "shqk,sqhd->skhd",
                probabilities.astype(jnp.bfloat16),
                grad_block,
                preferred_element_type=jnp.float32,
            )
        )
        prob_grad = jnp.einsum(
            "sqhd,skhd->shqk", grad_block, values[:, :key_end], preferred_element_type=jnp.float32
        )
        row_delta = jnp.sum(probabilities * prob_grad, -1, keepdims=True)
        score_grad = (probabilities * (prob_grad - row_delta)).astype(jnp.bfloat16)
        query_grads.append(
            jnp.einsum(
                "shqk,skhd->sqhd",
                score_grad,
                keys_rot[:, :key_end],
                preferred_element_type=jnp.float32,
            )
            * score_scale
        )
        key_grad = key_grad.at[:, :key_end].add(
            jnp.einsum(
                "shqk,sqhd->skhd", score_grad, query_block, preferred_element_type=jnp.float32
            )
            * score_scale
        )
    query_grad = jnp.concatenate(query_grads, 1)
    query_pre = unrotate(rounded(query_grad), cos_table, sine_table).astype(jnp.bfloat16)
    key_pre = unrotate(rounded(key_grad), cos_table, sine_table).astype(jnp.bfloat16)
    value_pre = value_grad.astype(jnp.bfloat16)
    qkv_grad = jnp.stack([query_pre, key_pre, value_pre], 3).reshape(
        tok_rows, local_heads * 3 * HEAD_DIM
    )
    grad_qkv = jnp.einsum("td,tc->dc", attn_in, qkv_grad, preferred_element_type=jnp.float32)
    qkv_bias_grad = jnp.sum(qkv_grad.astype(jnp.float32), 0)
    attn_in_grad = jnp.einsum("tc,dc->td", qkv_grad, qkv_weight, preferred_element_type=jnp.float32)
    norm_one_pull = jax.vjp(normalize, x_float, gain_one, shift_one)[1]
    input_one, gain_grad_one, shift_grad_one = norm_one_pull(attn_in_grad)
    norm_two_pull = jax.vjp(normalize, x_float, gain_two, shift_two)[1]
    input_two, gain_grad_two, shift_grad_two = norm_two_pull(mlp_in_grad)
    input_part = input_one + input_two
    input_total = lax.psum(input_part, "tensor")
    input_grad = (out_grad + input_total).astype(jnp.bfloat16)
    qkv_bias_grad, fc1_bias_grad, out_bias_grad = lax.psum(
        (qkv_bias_grad, fc1_bias_grad, out_bias_grad), "dp"
    )
    gain_grad_one, shift_grad_one, gain_grad_two, shift_grad_two = lax.psum(
        (gain_grad_one, shift_grad_one, gain_grad_two, shift_grad_two), ("dp", "tensor")
    )
    grad_qkv, grad_dense, grad_fc1, grad_fc2 = (
        lax.psum_scatter(
            grad_qkv.astype(jnp.bfloat16), "dp", scatter_dimension=0, tiled=True
        ).astype(jnp.float32),
        lax.psum_scatter(
            grad_dense.astype(jnp.bfloat16), "dp", scatter_dimension=0, tiled=True
        ).astype(jnp.float32),
        lax.psum_scatter(
            grad_fc1.astype(jnp.bfloat16), "dp", scatter_dimension=0, tiled=True
        ).astype(jnp.float32),
        lax.psum_scatter(
            grad_fc2.astype(jnp.bfloat16), "dp", scatter_dimension=0, tiled=True
        ).astype(jnp.float32),
    )
    return (
        output,
        input_grad,
        gain_grad_one,
        shift_grad_one,
        gain_grad_two,
        shift_grad_two,
        grad_qkv,
        qkv_bias_grad,
        grad_dense,
        out_bias_grad,
        grad_fc1,
        fc1_bias_grad,
        grad_fc2,
        out_bias_grad,
    )


def solution(mesh):
    in_specs = (
        P("dp", None),
        P(),
        P(),
        P(),
        P(),
        P(None, "tensor"),
        P("tensor"),
        P(None, "tensor"),
        P(),
        P(None, "tensor"),
        P("tensor"),
        P(None, "tensor"),
        P(),
        P("dp", None),
    )
    out_specs = (
        P("dp", None),
        P("dp", None),
        P(),
        P(),
        P(),
        P(),
        P("dp", "tensor"),
        P("tensor"),
        P("dp", "tensor"),
        P(),
        P("dp", "tensor"),
        P("tensor"),
        P("dp", "tensor"),
        P(),
    )
    return jax.shard_map(
        fused if fits(mesh) else on_device, mesh=mesh, in_specs=in_specs, out_specs=out_specs, check_vma=False
    )
```

```python
import itertools
import math
from functools import partial

import jax
import jax.numpy as jnp
from jax import lax
from jax.experimental import pallas as pl
from jax.experimental.pallas import tpu as pltpu
from jax.sharding import PartitionSpec as P

HEADS = 8
SEQ = 1024
HEAD_DIM = 256
ROT = 64
EPSILON = 1e-05
VMEM_LIMIT = 63 * 1024 * 1024

f32 = jnp.float32
bf16 = jnp.bfloat16
NN = (((1,), (0,)), ((), ()))
NT = (((1,), (1,)), ((), ()))
TN = (((0,), (0,)), ((), ()))


def dot(a, b, dims=NN):
    return lax.dot_general(a, b, dims, preferred_element_type=f32)


def turn(block, cos_table, sine_table):
    half_rot = ROT // 2
    head = block[:, :128]
    lane = lax.broadcasted_iota(jnp.int32, head.shape, 1)
    other = jnp.where(lane < half_rot, pltpu.roll(head, 128 - half_rot, 1), pltpu.roll(head, half_rot, 1))
    return jnp.concatenate([head * cos_table + other * sine_table, block[:, 128:]], 1)


def angle_tables():
    half_rot = ROT // 2
    lane = jnp.arange(128)
    frequency = jnp.exp((lane % half_rot).astype(f32) * (-2.0 * math.log(10000.0) / ROT))
    frequency = jnp.where(lane < ROT, frequency, 0.0)
    step = jnp.arange(32, dtype=f32)
    angles = jnp.concatenate([step, 32.0 * step])[:, None] * frequency[None, :]
    cos, sin = jnp.cos(angles), jnp.sin(angles)
    sign = jnp.where(lane < half_rot, -1.0, 1.0)[None, :]
    return jnp.concatenate([cos[:32], sin[:32], cos[32:], sin[32:], jnp.broadcast_to(sign, (8, 128))], 0)


CHUNK = 512
MESH = pl.DeviceIdType.MESH
VEC_ROWS = 8
VECTORS = 8
NORM_ROWS = 128


class Slots:
    def __init__(self, count):
        self.free = [(n, []) for n in range(count)]

    def take(self):
        slot, waits = self.free.pop(0)
        for wait in waits:
            wait()
        return slot

    def give(self, slot, *waits):
        self.free.append((slot, list(waits)))

    def drain(self):
        for _, waits in self.free:
            for wait in waits:
                wait()


def layer_kernel(
    x_hbm, c_hbm, table_in, fc1_hbm, fc2_hbm, wqkv_hbm, dense_hbm, *refs,
    jobs, orders, chunks, heads, block=256,
):
    vec_hbm, refs = refs[:VECTORS], refs[VECTORS:]
    (
        out_hbm, grad_hbm, keep_hbm, last_hbm, small_out, r1_hbm, r2_hbm, relay_hbm, core_hbm, y_hbm,
        attn_in, mlp_in, cot, act, hg, qg, ctx, mean_ref, rstd_ref, cos_ref, sin_ref, vec, raw, w1buf, w2buf,
        s1, s2, s3, k2, ld1, ldm, ld2, piece, xrow, small, small_in,
        load_sem, send_sem, recv_sem, keep_sem, relay_sem,
    ) = refs
    rows, width = cot.shape
    hidden = act.shape[1]
    nb = width // 8
    quarter = rows // 4
    me, own = lax.axis_index("dp"), lax.axis_index("tensor")
    dp_bits = [lax.rem(lax.div(me, 1 << k), 2) for k in range(3)]
    t_bits = [lax.rem(lax.div(own, 1 << k), 2) for k in range(2)]

    def dp_flip(*bits):
        return me + sum((1 - 2 * dp_bits[k]) * (1 << k) for k in bits)

    def t_flip(*bits):
        return own + sum((1 - 2 * t_bits[k]) * (1 << k) for k in bits)

    def dp_partner(bit):
        return (dp_flip(bit), own)

    def t_partner(bit):
        return (me, t_flip(bit))

    partners = [dp_partner(k) for k in range(3)] + [t_partner(k) for k in range(2)] + [(dp_flip(1, 2), own)]
    barrier = pltpu.get_barrier_semaphore()
    for partner in partners:
        pl.semaphore_signal(barrier, inc=1, device_id=partner, device_id_type=MESH)

    copies = itertools.count()

    def send_copy(src, dst, partner):
        n = next(copies)
        copy = pltpu.make_async_remote_copy(
            src_ref=src, dst_ref=dst, send_sem=send_sem.at[n], recv_sem=recv_sem.at[n], device_id=partner, device_id_type=MESH
        )
        copy.start()
        return copy

    loads = itertools.count()

    def load(src, dst):
        copy = pltpu.make_async_copy(src, dst, load_sem.at[next(loads)])
        copy.start()
        return copy

    load_x = load(x_hbm, act)
    load_v = [load(v, raw.at[n, pl.ds(0, v.shape[0])]) for n, v in enumerate(vec_hbm)]

    def mlp_weights(j):
        slot = j % 2
        at = pl.ds(j * CHUNK, CHUNK)
        return [load(fc1_hbm.at[:, at], w1buf.at[slot]), load(fc2_hbm.at[:, at], w2buf.at[slot])]

    def head_weights(h):
        slot = h % 2
        base = 3 * h * HEAD_DIM
        return [
            load(wqkv_hbm.at[:, pl.ds(base, 2 * HEAD_DIM)], w1buf.at[slot]),
            load(wqkv_hbm.at[:, pl.ds(base + 2 * HEAD_DIM, HEAD_DIM)], w2buf.at[slot, :, pl.ds(0, HEAD_DIM)]),
            load(dense_hbm.at[:, pl.ds(h * HEAD_DIM, HEAD_DIM)], w2buf.at[slot, :, pl.ds(HEAD_DIM, HEAD_DIM)]),
        ]

    weights = {("mlp", 0): mlp_weights(0)}
    load_c = load(c_hbm, cot)
    weights["mlp", 1] = mlp_weights(1)
    tiles = hidden // CHUNK

    small[...] = jnp.zeros_like(small)
    for copy in load_v:
        copy.wait()
    for n in range(VECTORS):
        packed = raw[n].astype(f32)
        if n == 6:
            packed = packed + raw[5].astype(f32)
        for i in range(vec_hbm[n].shape[0]):
            vec[n : n + 1, i * 128 : (i + 1) * 128] = packed[i : i + 1, :]
    low_cos, low_sin = table_in[0:32, :], table_in[32:64, :]
    sign = table_in[128:129, :]
    for n in range(SEQ // 32):
        high_cos, high_sin = table_in[64 + n : 65 + n, :], table_in[96 + n : 97 + n, :]
        cos_ref[n * 32 : (n + 1) * 32, :] = high_cos * low_cos - high_sin * low_sin
        sin_ref[n * 32 : (n + 1) * 32, :] = sign * (high_sin * low_cos + high_cos * low_sin)

    load_x.wait()

    def norm_rows(i, _):
        part = pl.ds(pl.multiple_of(i * NORM_ROWS, NORM_ROWS), NORM_ROWS)
        x = act[part, :].astype(f32)
        mean = jnp.mean(x, -1, keepdims=True)
        centred = x - mean
        rstd = lax.rsqrt(jnp.mean(centred * centred, -1, keepdims=True) + EPSILON)
        u = centred * rstd
        attn_in[part, :] = (u * vec[0:1, :] + vec[1:2, :]).astype(bf16)
        mlp_in[part, :] = (u * vec[2:3, :] + vec[3:4, :]).astype(bf16)
        mean_ref[part, :] = mean
        rstd_ref[part, :] = rstd
        return 0

    lax.fori_loop(0, rows // NORM_ROWS, norm_rows, 0)
    load_c.wait()
    pl.semaphore_wait(barrier, len(partners))

    s1_slots, s2_slots, s3_slots, k2_slots = Slots(s1.shape[0]), Slots(s2.shape[0]), Slots(s3.shape[0]), Slots(k2.shape[0])
    state = {}

    parts_of = {"fc2": (cot, act), "fc1": (mlp_in, hg), "qkv": (attn_in, qg), "dense": (cot, ctx)}
    starts = list(itertools.accumulate([c[2] for c in chunks], initial=0))

    def operands(c):
        kind, first, columns = chunks[c]
        lhs, rhs = parts_of[kind]
        return lhs, rhs.at[:, pl.ds(first, columns)], columns

    def cut(ref, columns):
        return ref if columns == CHUNK else ref.at[..., pl.ds(0, columns)]

    inner = dp_bits[1] + dp_bits[2] - 2 * dp_bits[1] * dp_bits[2]
    relayed = any(kind == "r" for kind, _ in jobs)

    def block_of(lhs, index):
        return lhs[:, pl.ds(pl.multiple_of(index * nb, nb), nb)]

    def w1(c):
        lhs, rhs, columns = operands(c)
        one, two, three = orders[c]
        slot = s1_slots.take()
        base = dp_flip(one, two, three)
        out = cut(s1.at[slot], columns)

        def body(n, _):
            second, third = n // 2, lax.rem(n, 2)
            index = base - second * (1 - 2 * dp_bits[two]) * (1 << two) - third * (1 - 2 * dp_bits[three]) * (1 << three)
            out[n] = dot(block_of(lhs, index), rhs[...], TN).astype(bf16)
            return 0

        lax.fori_loop(0, 4, body, 0)
        copy = send_copy(out, cut(r1_hbm.at[c], columns), dp_partner(one))
        s1_slots.give(slot, copy.wait_send)
        state[c] = copy

    def w2(c):
        lhs, rhs, columns = operands(c)
        one, two, three = orders[c]
        state[c].wait_recv()
        held = cut(ld1, columns)
        loaded = load(cut(r1_hbm.at[c], columns), held)
        slot, kept = s2_slots.take(), k2_slots.take()
        loaded.wait()

        def part(base, n, out):
            def body(i, _):
                index = base - i * (1 - 2 * dp_bits[three]) * (1 << three)
                out[i] = (dot(block_of(lhs, index), rhs[...], TN) + held[n + i].astype(f32)).astype(bf16)
                return 0

            lax.fori_loop(0, 2, body, 0)

        sent = cut(s2.at[slot], columns)
        part(dp_flip(two, three), 0, sent)
        copy = send_copy(sent, cut(r2_hbm.at[c], columns), dp_partner(two))
        s2_slots.give(slot, copy.wait_send)
        part(dp_flip(three), 2, cut(k2.at[kept], columns))
        state[c] = (copy, kept)

    def a3(c):
        columns = chunks[c][2]
        copy, kept = state[c]
        copy.wait_recv()
        held, mine = cut(ld2, columns), cut(k2.at[kept], columns)
        loaded = load(cut(r2_hbm.at[c], columns), held)
        slot = s3_slots.take()
        sent = cut(s3.at[slot], columns)
        loaded.wait()
        sent[...] = (mine[0].astype(f32) + held[0].astype(f32)).astype(bf16)
        place = pl.ds(starts[c], columns)
        n = next(copies)
        to_end, to_inner = (
            pltpu.make_async_remote_copy(
                src_ref=sent,
                dst_ref=dst,
                send_sem=send_sem.at[n],
                recv_sem=sem,
                device_id=partner,
                device_id_type=MESH,
            )
            for dst, sem, partner in (
                (last_hbm.at[:, place], recv_sem.at[n], dp_partner(2)),
                (relay_hbm.at[:, place], relay_sem.at[c], dp_partner(1)),
            )
        )

        if relayed:

            @pl.when(inner == 1)
            def _():
                to_end.start()

            @pl.when(inner == 0)
            def _():
                to_inner.start()

        else:
            to_end.start()

        s3_slots.give(slot, to_end.wait_send)
        mine[1] = (mine[1].astype(f32) + held[1].astype(f32)).astype(bf16)
        keep = pltpu.make_async_copy(mine.at[1], keep_hbm.at[:, place], keep_sem.at[c])
        keep.start()
        k2_slots.give(kept, keep.wait)
        passed = pltpu.make_async_remote_copy(
            src_ref=relay_hbm.at[:, place],
            dst_ref=last_hbm.at[:, place],
            send_sem=send_sem.at[next(copies)],
            recv_sem=recv_sem.at[n],
            device_id=(dp_flip(1, 2), own),
            device_id_type=MESH,
        )
        state[c] = (to_end, to_inner, passed)

    def relay(c):
        _, arriving, passed = state[c]

        @pl.when(inner == 1)
        def _():
            arriving.wait_recv()
            passed.start()

    def mlp(j):
        slot = j % 2
        for copy in weights.pop(("mlp", j)):
            copy.wait()
        at = j * CHUNK
        bias = vec[4:5, at : at + CHUNK]

        def body(i, sums):
            part = pl.ds(pl.multiple_of(i * block, block), block)
            h = dot(mlp_in[part, :], w1buf[slot]) + bias
            above = dot(cot[part, :], w2buf[slot])
            cdf = 0.5 + 0.5 * lax.erf(h * (2.0**-0.5))
            density = jnp.exp(h * h * -0.5) * ((2.0 * math.pi) ** -0.5)
            act[part, at : at + CHUNK] = (h * cdf).astype(bf16)
            low = (above * (cdf + h * density)).astype(bf16)
            hg[part, at : at + CHUNK] = low
            above_sum = jnp.sum(cot[part, at : at + CHUNK].astype(f32), 0, keepdims=True)
            return sums[0] + jnp.sum(low.astype(f32), 0, keepdims=True), sums[1] + above_sum

        zero = jnp.zeros((1, CHUNK), f32)
        bias_sum, above_sum = lax.fori_loop(0, rows // block, body, (zero, zero))
        small[4:5, at : at + CHUNK] = bias_sum
        small[6:7, at : at + CHUNK] = above_sum
        if j + 2 < tiles:
            weights["mlp", j + 2] = mlp_weights(j + 2)
        else:
            h = j + 2 - tiles
            weights["head", h] = head_weights(h)

    def attention(n):
        if n > 0:
            return
        for h in range(heads):
            for copy in weights.pop(("head", h)):
                copy.wait()
        lax.fori_loop(0, heads, one_head, 0)

    def one_head(slot, _):
        base = pl.multiple_of(3 * HEAD_DIM * slot, HEAD_DIM)
        scale = HEAD_DIM ** (-0.5)

        def third(n):
            return pl.ds(pl.multiple_of(base + n * HEAD_DIM, HEAD_DIM), HEAD_DIM)

        mine = pl.ds(pl.multiple_of(slot * HEAD_DIM, HEAD_DIM), HEAD_DIM)

        def scoped(qkv_ref, g_ref, dk_ref, dv_ref):
            def project(i, _):
                part = pl.ds(pl.multiple_of(i * block, block), block)
                acc = dot(attn_in[part, :], w1buf[slot]) + vec[7:8, pl.ds(base, 2 * HEAD_DIM)]
                cos, sin = cos_ref[part, :], sin_ref[part, :]
                for n in range(2):
                    at = n * HEAD_DIM
                    qkv_ref[part, at : at + HEAD_DIM] = turn(acc[:, at : at + HEAD_DIM], cos, sin).astype(bf16)
                acc = dot(attn_in[part, :], w2buf[slot, :, 0:HEAD_DIM]) + vec[7:8, third(2)]
                qkv_ref[part, 2 * HEAD_DIM :] = acc.astype(bf16)
                g_ref[part, :] = dot(cot[part, :], w2buf[slot, :, HEAD_DIM : 2 * HEAD_DIM]).astype(bf16)
                return 0

            lax.fori_loop(0, rows // block, project, 0)
            for i in reversed(range(SEQ // block)):
                part = pl.ds(i * block, block)
                key_end = (i + 1) * block
                keys = pl.ds(0, key_end)
                q, g = qkv_ref[part, 0:HEAD_DIM], g_ref[part, :]
                k, v = qkv_ref[keys, HEAD_DIM : 2 * HEAD_DIM], qkv_ref[keys, 2 * HEAD_DIM :]
                scores = dot(q, k, NT) * scale
                row_id = i * block + lax.broadcasted_iota(jnp.int32, scores.shape, 0)
                col_id = lax.broadcasted_iota(jnp.int32, scores.shape, 1)
                scores = jnp.where(col_id <= row_id, scores, -1e30)
                e = jnp.exp(scores - jnp.max(scores, -1, keepdims=True))
                probs = e / jnp.sum(e, -1, keepdims=True)
                low = probs.astype(bf16)
                ctx[part, mine] = dot(low, v).astype(bf16)
                prob_grad = dot(g, v, NT)
                delta = jnp.sum(probs * prob_grad, -1, keepdims=True)
                score_grad = (probs * (prob_grad - delta)).astype(bf16)
                dv = dot(low, g, TN)
                dk = dot(score_grad, q, TN)
                if i == SEQ // block - 1:
                    dv_ref[...] = dv
                    dk_ref[...] = dk
                else:
                    dv_ref[keys, :] += dv
                    dk_ref[keys, :] += dk
                dq = (dot(score_grad, k) * scale).astype(bf16).astype(f32)
                qg[part, third(0)] = turn(dq, cos_ref[part, :], -sin_ref[part, :]).astype(bf16)
            dk = (dk_ref[...] * scale).astype(bf16).astype(f32)
            qg[:, third(1)] = turn(dk, cos_ref[...], -sin_ref[...]).astype(bf16)
            qg[:, third(2)] = dv_ref[...].astype(bf16)
            for n in range(3):
                small[5:6, third(n)] = jnp.sum(qg[:, third(n)].astype(f32), 0, keepdims=True)

        pl.run_scoped(
            scoped,
            pltpu.VMEM((SEQ, 3 * HEAD_DIM), bf16),
            pltpu.VMEM((SEQ, HEAD_DIM), bf16),
            pltpu.VMEM((SEQ, HEAD_DIM), f32),
            pltpu.VMEM((SEQ, HEAD_DIM), f32),
        )
        return 0

    def quarter_of(n):
        index = own + (1 - n // 2) * (1 - 2 * t_bits[0]) + (1 - lax.rem(n, 2)) * (1 - 2 * t_bits[1]) * 2
        return pl.ds(pl.multiple_of(index * quarter, quarter), quarter)

    def back_tiles(buf, first_hbm, first, second_hbm, second, x_tiles, store):
        step = CHUNK // 2

        def scoped(first_w, second_w, x_w, sems):
            def copies_of(d, slot):
                at = pl.ds(pl.multiple_of(d * step, step), step)
                made = [
                    pltpu.make_async_copy(first_hbm.at[at, :], first_w.at[slot], sems.at[slot, 0]),
                    pltpu.make_async_copy(second_hbm.at[at, :], second_w.at[slot], sems.at[slot, 1]),
                ]
                if x_tiles:
                    made.append(pltpu.make_async_copy(x_hbm.at[:, at], x_w.at[slot], sems.at[slot, 2]))
                return made

            n_steps = width // step
            for copy in copies_of(0, 0):
                copy.start()

            def body(e, _):
                for half in range(2):
                    d = 2 * e + half
                    for copy in copies_of(d, half):
                        copy.wait()

                    @pl.when(d + 1 < n_steps)
                    def _():
                        for copy in copies_of(d + 1, 1 - half):
                            copy.start()

                    columns = pl.ds(half * step, step)

                    def one(m, sums):
                        for n in (2 * m, 2 * m + 1):
                            part = quarter_of(n)
                            a = dot(first[part, :], first_w[half], NT)
                            b = dot(second[part, :], second_w[half], NT)
                            at = pl.ds(pl.multiple_of(e * 2 * quarter + lax.rem(n, 2) * quarter, quarter), quarter)
                            buf[m, at, columns], terms = store(d, part, a, b, x_w.at[half])
                            sums = tuple(s + t for s, t in zip(sums, terms))
                        return sums

                    count = 4 if x_tiles else 0
                    sums = lax.fori_loop(0, 2, one, tuple(jnp.zeros((1, step), f32) for _ in range(count)))
                    if x_tiles:
                        at = pl.ds(pl.multiple_of(d * step, step), step)
                        small[0:4, at] = jnp.concatenate(sums, 0)
                return 0

            lax.fori_loop(0, n_steps // 2, body, 0)

        pl.run_scoped(
            scoped,
            pltpu.VMEM((2, step, first.shape[1]), bf16),
            pltpu.VMEM((2, step, second.shape[1]), bf16),
            pltpu.VMEM((2, rows if x_tiles else 16, step), bf16),
            pltpu.SemaphoreType.DMA((2, 3)),
        )

    def input_tiles():
        step = CHUNK // 2

        def store(d, part, a, b, x_tile):
            at = pl.ds(pl.multiple_of(d * step, step), step)
            u = (x_tile[part, :].astype(f32) - mean_ref[part, :]) * rstd_ref[part, :]
            terms = [jnp.sum(t, 0, keepdims=True) for t in (a * u, a, b * u, b)]
            return (a * vec[0:1, at] + b * vec[2:3, at]).astype(bf16), terms

        back_tiles(w1buf, wqkv_hbm, qg, fc1_hbm, hg, True, store)

    def output_tiles():
        back_tiles(w2buf, dense_hbm, ctx, fc2_hbm, act, False, lambda d, part, a, b, x_tile: ((a + b).astype(bf16), []))

    e_tiles = width // CHUNK
    buffers = (w1buf, w2buf)
    results = (grad_hbm, out_hbm)

    def sum_start(k):
        (input_tiles, output_tiles)[k]()
        state["sum", k] = send_copy(buffers[k].at[0], core_hbm.at[k], t_partner(0))

    def half_of(k, half, dst):
        return [
            load(core_hbm.at[k, pl.ds(e * 2 * quarter + half * quarter, quarter), :], dst.at[e]) for e in range(e_tiles)
        ]

    def sum_middle(k):
        first = state["sum", k]
        first.wait_recv()
        loaded = half_of(k, 0, ld1)
        slot = s1_slots.take()
        for copy in loaded:
            copy.wait()
        for e in range(e_tiles):
            s1[slot, e] = (buffers[k][1, pl.ds(e * 2 * quarter, quarter), :].astype(f32) + ld1[e].astype(f32)).astype(bf16)
        copy = send_copy(s1.at[slot], y_hbm.at[k], t_partner(1))
        s1_slots.give(slot, copy.wait_send)
        first.wait_send()
        state["sum", k] = copy

    own_rows = pl.ds(pl.multiple_of(own * quarter, quarter), quarter)

    def rows_of(index):
        return pl.ds(pl.multiple_of(index * quarter, quarter), quarter)

    def sum_late(k):
        x_load = load(x_hbm.at[own_rows, :], xrow)
        half_loads = half_of(k, 1, ld1)
        state["sum", k].wait_recv()
        y_load = load(y_hbm.at[k], ldm)
        for copy in half_loads + [x_load, y_load]:
            copy.wait()
        totals = [
            buffers[k][1, pl.ds(e * 2 * quarter + quarter, quarter), :].astype(f32) + ld1[e].astype(f32) + ldm[e].astype(f32)
            for e in range(e_tiles)
        ]
        parts = [(e * CHUNK, (e + 1) * CHUNK) for e in range(e_tiles)]
        if k == 0:
            mean, rstd = mean_ref[own_rows, :], rstd_ref[own_rows, :]
            us = [(xrow[:, a:b].astype(f32) - mean) * rstd for a, b in parts]
            mean_w = sum(jnp.sum(t, -1, keepdims=True) for t in totals) * (1.0 / width)
            mean_wu = sum(jnp.sum(t * u, -1, keepdims=True) for t, u in zip(totals, us)) * (1.0 / width)
            for (a, b), t, u in zip(parts, totals, us):
                piece[k, :, a:b] = (cot[own_rows, a:b].astype(f32) + rstd * (t - mean_w - u * mean_wu)).astype(bf16)
        else:
            for (a, b), t in zip(parts, totals):
                piece[k, :, a:b] = (xrow[:, a:b].astype(f32) + t + vec[6:7, a:b]).astype(bf16)
        result = results[k]
        state["pieces", k] = [
            load(piece.at[k], result.at[own_rows, :]),
            send_copy(piece.at[k], result.at[own_rows, :], t_partner(1)),
            send_copy(piece.at[k], result.at[own_rows, :], t_partner(0)),
        ]

    def sum_gather(k):
        result = results[k]
        state["pieces", k][1].wait_recv()
        at = rows_of(t_flip(1))
        state["pieces", k].append(send_copy(result.at[at, :], result.at[at, :], t_partner(0)))

    def small_round(n):
        if n > 0:
            copy = state["small"]
            copy.wait()
            if n <= 2:
                small[0:4, :] += small_in[n - 1, 0:4, :]
            else:
                small[...] += small_in[n - 1]
        if n < 5:
            partner = t_partner(n) if n < 2 else dp_partner(n - 2)
            state["small"] = send_copy(small, small_in.at[n], partner)
        else:
            state["small"] = load(small, small_out)

    actions = dict(
        m=mlp, h=attention, a=w1, b=w2, c=a3, i=lambda k: sum_start(k), j=sum_middle, k=sum_late, l=sum_gather, r=relay, s=small_round
    )
    for kind, n in jobs:
        actions[kind](n)

    for c in range(len(orders)):
        state[c][0].wait_recv()

    if relayed:

        @pl.when(inner == 1)
        def _():
            for c in range(len(orders)):
                state[c][2].wait_send()

    for k in range(2):
        local, first, second, third = state["pieces", k]
        local.wait()
        first.wait_send()
        second.wait()
        third.wait()
        state["sum", k]
    for slots in (s1_slots, s2_slots, s3_slots, k2_slots):
        slots.drain()
    state["small"].wait()


ORDER = " ".join(
    [
        "m0 a4 a0 m1",
        "m2 m3 a6 a7",
        "h0 b0 h1 a3",
        "a10 a8 b7 a1",
        "b4 c0 a5 i0",
        "s0 c7 b8 i1",
        "j0 c4 s1 a13",
        "b5 c8 a9 s2",
        "a2 b3 a12 j1",
        "c5 b13 b9 c3",
        "b1 s3 c13 b2",
        "s4 c9 b6 k1",
        "a11 b10 c2 b12",
        "k0 c6 c1 b11",
        "l0 s5 l1 c10",
        "c12 c11",
    ]
).split()
Z_FIRST = (1, 4, 6, 10)


def layer_call(x, c, vectors, fc1, fc2, qkv_weight, dense):
    rows, width = x.shape
    hidden, qkv_columns, context_columns = fc1.shape[1], qkv_weight.shape[1], dense.shape[1]
    heads = qkv_columns // (3 * HEAD_DIM)
    total = 2 * hidden + qkv_columns + context_columns
    chunks = []
    for kind, columns, widths in (
        ("fc2", hidden, ()),
        ("fc1", hidden, ()),
        ("qkv", qkv_columns, (CHUNK // 2, CHUNK // 2)),
        ("dense", context_columns, (CHUNK // 2, CHUNK // 2)),
    ):
        at = 0
        for size in [CHUNK] * ((columns - sum(widths)) // CHUNK) + list(widths):
            chunks.append((kind, at, size))
            at += size
    vectors = [v.reshape(-1, 128) for v in vectors]
    jobs = [(word[0], int(word[1:])) for word in ORDER]
    orders = [(1, 0, 2) if n in Z_FIRST else (0, 1, 2) for n in range(len(chunks))]
    quarter, nb = rows // 4, width // 8
    anywhere = pl.BlockSpec(memory_space=pl.ANY)
    local = pl.BlockSpec(memory_space=pltpu.VMEM)
    shape = jax.ShapeDtypeStruct
    outs = [
        shape((rows, width), bf16),
        shape((rows, width), bf16),
        shape((nb, total), bf16),
        shape((nb, total), bf16),
        shape((8, width), f32),
        shape((len(chunks), 4, nb, CHUNK), bf16),
        shape((len(chunks), 2, nb, CHUNK), bf16),
        shape((nb, total), bf16),
        shape((2, width // CHUNK * 2 * quarter, CHUNK), bf16),
        shape((2, width // CHUNK, quarter, CHUNK), bf16),
    ]
    vmem = pltpu.VMEM
    scratch = [
        vmem((rows, width), bf16),
        vmem((rows, width), bf16),
        vmem((rows, width), bf16),
        vmem((rows, hidden), bf16),
        vmem((rows, hidden), bf16),
        vmem((rows, qkv_columns), bf16),
        vmem((rows, context_columns), bf16),
        vmem((rows, 1), f32),
        vmem((rows, 1), f32),
        vmem((SEQ, 128), f32),
        vmem((SEQ, 128), f32),
        vmem((VEC_ROWS, width), f32),
        vmem((VECTORS, width // 128, 128), bf16),
        vmem((2, width, CHUNK), bf16),
        vmem((2, width, CHUNK), bf16),
        vmem((5, 4, nb, CHUNK), bf16),
        vmem((6, 2, nb, CHUNK), bf16),
        vmem((6, nb, CHUNK), bf16),
        vmem((6, 2, nb, CHUNK), bf16),
        vmem((4, nb, CHUNK), bf16),
        vmem((4, nb, CHUNK), bf16),
        vmem((2, nb, CHUNK), bf16),
        vmem((2, quarter, width), bf16),
        vmem((quarter, width), bf16),
        vmem((8, width), f32),
        vmem((5, 8, width), f32),
        pltpu.SemaphoreType.DMA((96,)),
        pltpu.SemaphoreType.DMA((76,)),
        pltpu.SemaphoreType.DMA((76,)),
        pltpu.SemaphoreType.DMA((len(chunks),)),
        pltpu.SemaphoreType.DMA((len(chunks),)),
    ]
    flops = 6 * rows * width * (2 * hidden + qkv_columns + context_columns)
    return pl.pallas_call(
        partial(layer_kernel, jobs=jobs, orders=orders, chunks=chunks, heads=heads),
        in_specs=[anywhere, anywhere, local] + [anywhere] * (4 + VECTORS),
        out_specs=[anywhere] * len(outs),
        out_shape=outs,
        scratch_shapes=scratch,
        compiler_params=pltpu.CompilerParams(vmem_limit_bytes=VMEM_LIMIT, collective_id=0, has_side_effects=True),
        cost_estimate=pl.CostEstimate(flops=flops, bytes_accessed=1 << 27, transcendentals=2 * rows * hidden),
        name="layer",
    )(x, c, angle_tables(), fc1, fc2, qkv_weight, dense, *vectors)


def finish_kernel(kept_ref, last_ref, out_ref, grad_ref, *refs):
    at = 0
    for ref in refs[:-2]:
        columns = slice(at, at + ref.shape[1])
        ref[...] = kept_ref[:, columns].astype(f32) + last_ref[:, columns].astype(f32)
        at += ref.shape[1]
    refs[-2][...] = out_ref[...]
    refs[-1][...] = grad_ref[...]


def finish_call(kept, last, output, input_grad, sizes, steps=2):
    nb, total = kept.shape
    rows, width = output.shape

    def tiles(count, columns):
        return pl.BlockSpec((count // steps, columns), lambda i: (i, 0))

    ins = [tiles(nb, total), tiles(nb, total), tiles(rows, width), tiles(rows, width)]
    outs = [tiles(nb, n) for n in sizes] + [tiles(rows, width)] * 2
    return pl.pallas_call(
        finish_kernel,
        grid=(steps,),
        in_specs=ins,
        out_specs=outs,
        out_shape=[jax.ShapeDtypeStruct((nb, n), f32) for n in sizes] + [jax.ShapeDtypeStruct((rows, width), bf16)] * 2,
        compiler_params=pltpu.CompilerParams(vmem_limit_bytes=VMEM_LIMIT),
        cost_estimate=pl.CostEstimate(flops=nb * total, bytes_accessed=8 * (nb * total + rows * width), transcendentals=0),
        name="finish",
    )(kept, last, output, input_grad)


def fused(
    layer_input,
    ln1_gain,
    ln1_bias,
    ln2_gain,
    ln2_bias,
    qkv_weight,
    qkv_bias,
    dense_weight,
    dense_bias,
    fc1_weight,
    fc1_bias,
    fc2_weight,
    fc2_bias,
    cotangent,
):
    whole_out, whole_grad, kept, last, small, *_ = layer_call(
        layer_input,
        cotangent,
        (ln1_gain, ln1_bias, ln2_gain, ln2_bias, fc1_bias, dense_bias, fc2_bias, qkv_bias),
        fc1_weight,
        fc2_weight,
        qkv_weight,
        dense_weight,
    )
    hidden, qkv_columns = fc1_weight.shape[1], qkv_weight.shape[1]
    grad_fc2, grad_fc1, grad_qkv, grad_dense, output, input_grad = finish_call(
        kept, last, whole_out, whole_grad, (hidden, hidden, qkv_columns, dense_weight.shape[1])
    )
    return (
        output,
        input_grad,
        small[0],
        small[1],
        small[2],
        small[3],
        grad_qkv,
        small[5, :qkv_columns],
        grad_dense,
        small[6],
        grad_fc1,
        small[4, :hidden],
        grad_fc2,
        small[6],
    )


def fits(mesh):
    return mesh.shape["dp"] == 8 and mesh.shape["tensor"] == 4


def normalize(x_float, gain_row, shift_row):
    row_mean = jnp.mean(x_float, -1, keepdims=True)
    centred = x_float - row_mean
    spread = jnp.mean(centred * centred, -1, keepdims=True)
    return centred * lax.rsqrt(spread + EPSILON) * gain_row + shift_row


def rotary_tables():
    half_rot = ROT // 2
    freq_index = jnp.arange(half_rot, dtype=jnp.float32)
    frequency = jnp.exp(freq_index * (-2.0 * math.log(10000.0) / ROT))
    angles = jnp.arange(SEQ, dtype=jnp.float32)[:, None] * frequency[None, :]
    return (jnp.cos(angles), jnp.sin(angles))


def rotate(operand, cos_table, sine_table):
    half_rot = ROT // 2
    first_half = operand[..., :half_rot]
    second_half = operand[..., half_rot:ROT]
    cos_part = cos_table[None, :, None, :]
    sine_part = sine_table[None, :, None, :]
    return jnp.concatenate(
        [
            first_half * cos_part - second_half * sine_part,
            second_half * cos_part + first_half * sine_part,
            operand[..., ROT:],
        ],
        -1,
    )


def unrotate(operand, cos_table, sine_table):
    half_rot = ROT // 2
    first_half = operand[..., :half_rot]
    second_half = operand[..., half_rot:ROT]
    cos_part = cos_table[None, :, None, :]
    sine_part = sine_table[None, :, None, :]
    return jnp.concatenate(
        [
            first_half * cos_part + second_half * sine_part,
            second_half * cos_part - first_half * sine_part,
            operand[..., ROT:],
        ],
        -1,
    )


def block_scores(query_block, key_block, start_row, score_scale):
    scores = (
        jnp.einsum("sqhd,skhd->shqk", query_block, key_block, preferred_element_type=jnp.float32)
        * score_scale
    )
    row_ids = start_row + jnp.arange(query_block.shape[1])[:, None]
    col_ids = jnp.arange(key_block.shape[1])[None, :]
    return jnp.where(col_ids <= row_ids, scores, -1e30)


def rounded(values_in):
    return lax.optimization_barrier(values_in.astype(jnp.bfloat16)).astype(jnp.float32)


def on_device(
    layer_input,
    ln1_gain,
    ln1_bias,
    ln2_gain,
    ln2_bias,
    qkv_weight,
    qkv_bias,
    dense_weight,
    dense_bias,
    fc1_weight,
    fc1_bias,
    fc2_weight,
    fc2_bias,
    cotangent,
):
    tok_rows, model_width = layer_input.shape
    local_heads = HEADS // lax.axis_size("tensor")
    seq_count = tok_rows // SEQ
    block_rows = 512
    score_scale = HEAD_DIM ** (-0.5)
    x_float = layer_input.astype(jnp.float32)
    gain_one = ln1_gain.astype(jnp.float32)
    shift_one = ln1_bias.astype(jnp.float32)
    gain_two = ln2_gain.astype(jnp.float32)
    shift_two = ln2_bias.astype(jnp.float32)
    attn_in = normalize(x_float, gain_one, shift_one).astype(jnp.bfloat16)
    mlp_in = normalize(x_float, gain_two, shift_two).astype(jnp.bfloat16)
    qkv_all = jnp.dot(attn_in, qkv_weight, preferred_element_type=jnp.float32) + qkv_bias.astype(
        jnp.float32
    )
    qkv_all = qkv_all.reshape(seq_count, SEQ, local_heads, 3, HEAD_DIM)
    cos_table, sine_table = rotary_tables()
    queries = rotate(qkv_all[..., 0, :], cos_table, sine_table).astype(jnp.bfloat16)
    keys_rot = rotate(qkv_all[..., 1, :], cos_table, sine_table).astype(jnp.bfloat16)
    values = qkv_all[..., 2, :].astype(jnp.bfloat16)
    context_blocks = []
    log_sums = []
    for start_row in range(0, SEQ, block_rows):
        key_end = start_row + block_rows
        masked = block_scores(
            queries[:, start_row:key_end], keys_rot[:, :key_end], start_row, score_scale
        )
        row_peak = jnp.max(masked, -1, keepdims=True)
        weights = jnp.exp(masked - row_peak)
        row_total = jnp.sum(weights, -1, keepdims=True)
        probabilities = (weights / row_total).astype(jnp.bfloat16)
        log_sums.append(row_peak + jnp.log(row_total))
        context_blocks.append(
            jnp.einsum(
                "shqk,skhd->sqhd",
                probabilities,
                values[:, :key_end],
                preferred_element_type=jnp.float32,
            )
        )
    context = jnp.concatenate(context_blocks, 1).astype(jnp.bfloat16)
    context_flat = context.reshape(tok_rows, local_heads * HEAD_DIM)
    attn_part = jnp.einsum(
        "td,ed->te", context_flat, dense_weight, preferred_element_type=jnp.float32
    )
    hidden = jnp.dot(mlp_in, fc1_weight, preferred_element_type=jnp.float32) + fc1_bias.astype(
        jnp.float32
    )
    exact_gelu = partial(jax.nn.gelu, approximate=False)
    activated = exact_gelu(hidden).astype(jnp.bfloat16)
    mlp_part = jnp.einsum("tf,ef->te", activated, fc2_weight, preferred_element_type=jnp.float32)
    partial_out = attn_part + mlp_part
    bias_total = dense_bias.astype(jnp.float32) + fc2_bias.astype(jnp.float32)
    full_sum = lax.psum(partial_out, "tensor")
    output = (x_float + full_sum + bias_total).astype(jnp.bfloat16)
    out_grad = cotangent.astype(jnp.float32)
    grad_fc2 = jnp.einsum("te,tf->ef", cotangent, activated, preferred_element_type=jnp.float32)
    grad_dense = jnp.einsum(
        "te,td->ed", cotangent, context_flat, preferred_element_type=jnp.float32
    )
    out_bias_grad = jnp.sum(out_grad, 0)
    activated_grad = jnp.einsum(
        "te,ef->tf", cotangent, fc2_weight, preferred_element_type=jnp.float32
    )
    gelu_pull = jax.vjp(exact_gelu, hidden)[1]
    hidden_grad = gelu_pull(activated_grad)[0].astype(jnp.bfloat16)
    grad_fc1 = jnp.einsum("td,tf->df", mlp_in, hidden_grad, preferred_element_type=jnp.float32)
    fc1_bias_grad = jnp.sum(hidden_grad.astype(jnp.float32), 0)
    mlp_in_grad = jnp.einsum(
        "tf,df->td", hidden_grad, fc1_weight, preferred_element_type=jnp.float32
    )
    context_grad = jnp.einsum(
        "te,ed->td", cotangent, dense_weight, preferred_element_type=jnp.float32
    ).astype(jnp.bfloat16)
    context_grad = context_grad.reshape(seq_count, SEQ, local_heads, HEAD_DIM)
    key_grad = jnp.zeros((seq_count, SEQ, local_heads, HEAD_DIM), jnp.float32)
    value_grad = jnp.zeros((seq_count, SEQ, local_heads, HEAD_DIM), jnp.float32)
    query_grads = []
    for block_number, start_row in enumerate(range(0, SEQ, block_rows)):
        key_end = start_row + block_rows
        query_block = queries[:, start_row:key_end]
        masked = block_scores(query_block, keys_rot[:, :key_end], start_row, score_scale)
        probabilities = jnp.exp(masked - log_sums[block_number])
        grad_block = context_grad[:, start_row:key_end]
        value_grad = value_grad.at[:, :key_end].add(
            jnp.einsum(
                "shqk,sqhd->skhd",
                probabilities.astype(jnp.bfloat16),
                grad_block,
                preferred_element_type=jnp.float32,
            )
        )
        prob_grad = jnp.einsum(
            "sqhd,skhd->shqk", grad_block, values[:, :key_end], preferred_element_type=jnp.float32
        )
        row_delta = jnp.sum(probabilities * prob_grad, -1, keepdims=True)
        score_grad = (probabilities * (prob_grad - row_delta)).astype(jnp.bfloat16)
        query_grads.append(
            jnp.einsum(
                "shqk,skhd->sqhd",
                score_grad,
                keys_rot[:, :key_end],
                preferred_element_type=jnp.float32,
            )
            * score_scale
        )
        key_grad = key_grad.at[:, :key_end].add(
            jnp.einsum(
                "shqk,sqhd->skhd", score_grad, query_block, preferred_element_type=jnp.float32
            )
            * score_scale
        )
    query_grad = jnp.concatenate(query_grads, 1)
    query_pre = unrotate(rounded(query_grad), cos_table, sine_table).astype(jnp.bfloat16)
    key_pre = unrotate(rounded(key_grad), cos_table, sine_table).astype(jnp.bfloat16)
    value_pre = value_grad.astype(jnp.bfloat16)
    qkv_grad = jnp.stack([query_pre, key_pre, value_pre], 3).reshape(
        tok_rows, local_heads * 3 * HEAD_DIM
    )
    grad_qkv = jnp.einsum("td,tc->dc", attn_in, qkv_grad, preferred_element_type=jnp.float32)
    qkv_bias_grad = jnp.sum(qkv_grad.astype(jnp.float32), 0)
    attn_in_grad = jnp.einsum("tc,dc->td", qkv_grad, qkv_weight, preferred_element_type=jnp.float32)
    norm_one_pull = jax.vjp(normalize, x_float, gain_one, shift_one)[1]
    input_one, gain_grad_one, shift_grad_one = norm_one_pull(attn_in_grad)
    norm_two_pull = jax.vjp(normalize, x_float, gain_two, shift_two)[1]
    input_two, gain_grad_two, shift_grad_two = norm_two_pull(mlp_in_grad)
    input_part = input_one + input_two
    input_total = lax.psum(input_part, "tensor")
    input_grad = (out_grad + input_total).astype(jnp.bfloat16)
    qkv_bias_grad, fc1_bias_grad, out_bias_grad = lax.psum(
        (qkv_bias_grad, fc1_bias_grad, out_bias_grad), "dp"
    )
    gain_grad_one, shift_grad_one, gain_grad_two, shift_grad_two = lax.psum(
        (gain_grad_one, shift_grad_one, gain_grad_two, shift_grad_two), ("dp", "tensor")
    )
    grad_qkv, grad_dense, grad_fc1, grad_fc2 = (
        lax.psum_scatter(
            grad_qkv.astype(jnp.bfloat16), "dp", scatter_dimension=0, tiled=True
        ).astype(jnp.float32),
        lax.psum_scatter(
            grad_dense.astype(jnp.bfloat16), "dp", scatter_dimension=0, tiled=True
        ).astype(jnp.float32),
        lax.psum_scatter(
            grad_fc1.astype(jnp.bfloat16), "dp", scatter_dimension=0, tiled=True
        ).astype(jnp.float32),
        lax.psum_scatter(
            grad_fc2.astype(jnp.bfloat16), "dp", scatter_dimension=0, tiled=True
        ).astype(jnp.float32),
    )
    return (
        output,
        input_grad,
        gain_grad_one,
        shift_grad_one,
        gain_grad_two,
        shift_grad_two,
        grad_qkv,
        qkv_bias_grad,
        grad_dense,
        out_bias_grad,
        grad_fc1,
        fc1_bias_grad,
        grad_fc2,
        out_bias_grad,
    )


def solution(mesh):
    in_specs = (
        P("dp", None),
        P(),
        P(),
        P(),
        P(),
        P(None, "tensor"),
        P("tensor"),
        P(None, "tensor"),
        P(),
        P(None, "tensor"),
        P("tensor"),
        P(None, "tensor"),
        P(),
        P("dp", None),
    )
    out_specs = (
        P("dp", None),
        P("dp", None),
        P(),
        P(),
        P(),
        P(),
        P("dp", "tensor"),
        P("tensor"),
        P("dp", "tensor"),
        P(),
        P("dp", "tensor"),
        P("tensor"),
        P("dp", "tensor"),
        P(),
    )
    return jax.shard_map(
        fused if fits(mesh) else on_device, mesh=mesh, in_specs=in_specs, out_specs=out_specs, check_vma=False
    )
```
